256 devices in a mesh: gx: 16 (over z, core), gy: 8 (over x_hi, y), gz: 2 (over x_lo).
Axes of the slice: x: 4 (x_hi: 2, x_lo: 2; x = x_hi * 2 + x_lo), y: 4, z: 8, core: 2. Of those that a mesh axis runs over, the one named last changes fastest.
Arguments:
- load_current: float32 [1536, 8192], P('gy', 'gx'), may hold values from 0 to 90
- sink_mask: int32 [1536, 8192], P('gy', 'gx'), may hold values 0 or 1
- pad_mask: int32 [1536, 8192], P('gy', 'gx'), may hold values from 0 to 1, as said below
- plane_class: int32 [4, 1536, 8192], P('gz', 'gy', 'gx'), may hold values from 0 to 7
- via_class: int32 [4, 1536, 8192], P('gz', 'gy', 'gx'), may hold values from 0 to 7
- plane_table: float32 [4, 8], P('gz'), may hold values from 0.25 to 4
- via_table: float32 [4, 8], P('gz'), may hold values from 0.25 to 4
Outputs:
- voltage: float32 [4, 1536, 8192], P('gz', 'gy', 'gx')
- residual: float32 [4, 1536, 8192], P('gz', 'gy', 'gx')
The draws below stay inside these ranges and needn't reach their ends.
Inputs may be any that keep to these rules, and one draw needn't show every extreme that they name: `pad_mask`: exactly one pad in each aligned 8 x 8 tile of nodes.
All inputs are finite; a program needn't handle non-finite values. No bound on the sum of `sink_mask` on one device may be relied on, other than what follows from the above.
Results may differ from the reference program's by a relative error of at most 0.00012.
Values sent between devices are 32-bit elements; how exact they have to be, the bound alone decides.
A program may use at most 64 MiB of HBM per device.

```python
import math
import jax
import jax.numpy as jnp

L_DEV = 2
ITERS = 3
NCLASS = 8
LAYERS = 4
NX = 8192
NY = 1536
N_GZ = 2


def draw_pad_mask(key, part):
    pad_key = jax.random.fold_in(key, 11)
    pad_spots = jax.random.randint(pad_key, (NY // 8, NX // 8), 0, 64)
    row_ids = jnp.arange(NY, dtype=jnp.int32)[:, None]
    col_ids = jnp.arange(NX, dtype=jnp.int32)[None, :]
    local_index = row_ids % 8 * 8 + col_ids % 8
    chosen = jnp.repeat(jnp.repeat(pad_spots, 8, axis=0), 8, axis=1)
    return (local_index == chosen).astype(jnp.int32)


def draw_load_current(key, part):
    base_key = jax.random.fold_in(key, 23)
    row_key, col_key, cell_key = jax.random.split(base_key, 3)
    rise_rows = jnp.arange(NY, dtype=jnp.float32) / NY * math.log(3.0)
    rise_cols = jnp.arange(NX, dtype=jnp.float32) / NX * math.log(3.0)
    log_span = math.log(10.0)
    cell_factor = jnp.exp(jax.random.uniform(cell_key, (NY, NX), jnp.float32, math.log(0.2), math.log(2.0)))
    row_scale = jnp.exp(jax.random.uniform(row_key, (NY, 1), jnp.float32) * log_span + rise_rows[:, None])
    col_scale = jnp.exp(jax.random.uniform(col_key, (1, NX), jnp.float32) * log_span + rise_cols[None, :])
    return (0.02 * row_scale * col_scale * cell_factor).astype(jnp.float32)


def touch_ends(values, rng, low, high):
    dims = values.shape
    spot = [jax.random.randint(jax.random.fold_in(rng, axis), (), 0, dims[axis]) for axis in range(len(dims))]
    values = values.at[tuple(spot)].set(low)
    longest = dims.index(max(dims))
    spot[longest] = (spot[longest] + 1) % dims[longest]
    return values.at[tuple(spot)].set(high)


def shard_levels(own_key, dims, cuts, least, largest):
    factor_of = 1.0
    for dim, blocks in cuts:
        heights = jax.random.uniform(jax.random.fold_in(jax.random.fold_in(own_key, 6), dim), (blocks,), jnp.float32, least / len(cuts), largest / len(cuts))
        factor_of = factor_of * jnp.repeat(jnp.exp(heights), dims[dim] // blocks).reshape((-1,) + (1,) * (len(dims) - 1 - dim))
    return factor_of


def setup_inputs(seed: int = 0) -> dict:
    splits = jax.random.split(jax.random.key(seed), 8)
    load_current = draw_load_current(jax.random.fold_in(splits[7], 71), 0)
    sink_mask = touch_ends((jax.random.randint(splits[1], (NY, NX), 0, 2) < 1).astype(jnp.int32), jax.random.fold_in(splits[1], 1), 0, 1)
    pad_mask = draw_pad_mask(jax.random.fold_in(splits[7], 71), 0)
    plane_class = touch_ends(jax.random.randint(splits[3], (LAYERS, NY, NX), 0, NCLASS), jax.random.fold_in(splits[3], 1), 0, NCLASS - 1).astype(jnp.int32)
    via_class = touch_ends(jax.random.randint(splits[4], (LAYERS, NY, NX), 0, NCLASS), jax.random.fold_in(splits[4], 1), 0, NCLASS - 1).astype(jnp.int32)
    plane_table = jnp.clip(jnp.exp(math.log(4.0) - 2.7725887 * jax.random.uniform(splits[5], (LAYERS, NCLASS), jnp.float32) ** shard_levels(splits[5], (LAYERS, NCLASS), ((0, 2),), -0.2, 0.2)), 0.25, 4.0)
    via_table = jnp.clip(jnp.exp(math.log(4.0) - 2.7725887 * jax.random.uniform(splits[6], (LAYERS, NCLASS), jnp.float32) ** shard_levels(splits[6], (LAYERS, NCLASS), ((0, 2),), -0.2, 0.2)), 0.25, 4.0)
    return {"load_current": load_current, "sink_mask": sink_mask, "pad_mask": pad_mask, "plane_class": plane_class, "via_class": via_class, "plane_table": plane_table, "via_table": via_table}


PAD_CONDUCTANCE = 20.0


def lookup(classes, table):
    summed = jnp.zeros(classes.shape, jnp.float32)
    for level in range(table.shape[1]):
        summed = summed + jnp.where(classes == level, table[:, level][:, None, None], jnp.float32(0.0))
    return summed


def harmonic(first, second):
    return 2.0 * first * second / (first + second)


def factor(diagonal, up_edge):
    inverses = []
    factors = []
    for level in range(diagonal.shape[0]):
        pivots = diagonal[level]
        if level > 0:
            pivots = pivots + up_edge[level - 1] * factors[level - 1]
        inverse = 1.0 / pivots
        inverses.append(inverse)
        factors.append(-up_edge[level] * inverse)
    return jnp.stack(inverses), jnp.stack(factors)


def solve_block(inverses, factors, up_edge, source_term):
    forward = []
    for level in range(source_term.shape[0]):
        entries = source_term[level]
        if level > 0:
            entries = entries + up_edge[level - 1] * forward[level - 1]
        forward.append(entries * inverses[level])
    result = [forward[-1]]
    for level in range(source_term.shape[0] - 2, -1, -1):
        result.insert(0, forward[level] - factors[level] * result[0])
    return jnp.stack(result)


def reference(load_current, sink_mask, pad_mask, plane_class, via_class, plane_table, via_table):
    g_plane = lookup(plane_class, plane_table)
    g_via = lookup(via_class, via_table)
    zero_plane = jnp.zeros((1, NY, NX), jnp.float32)
    east_edge = harmonic(g_plane, jnp.roll(g_plane, -1, 2))
    north_edge = harmonic(g_plane, jnp.roll(g_plane, -1, 1))
    up_edge = jnp.concatenate([harmonic(g_via[:-1], g_via[1:]), zero_plane], 0)
    down_edge = jnp.concatenate([zero_plane, up_edge[:-1]], 0)
    west_edge = jnp.roll(east_edge, 1, 2)
    south_edge = jnp.roll(north_edge, 1, 1)
    pad_layer = jnp.concatenate([jnp.zeros((LAYERS - 1, NY, NX), jnp.float32), (PAD_CONDUCTANCE * pad_mask.astype(jnp.float32))[None]], 0)
    diagonal = east_edge + west_edge + north_edge + south_edge + up_edge + down_edge + pad_layer

    def operate(field):
        above_field = jnp.concatenate([field[1:], zero_plane], 0)
        below_field = jnp.concatenate([zero_plane, field[:-1]], 0)
        return (diagonal * field
                - east_edge * jnp.roll(field, -1, 2) - west_edge * jnp.roll(field, 1, 2)
                - north_edge * jnp.roll(field, -1, 1) - south_edge * jnp.roll(field, 1, 1)
                - up_edge * above_field - down_edge * below_field)

    def blocks(array):
        return array.reshape(N_GZ, L_DEV, NY, NX)

    up_blocks = blocks(up_edge)
    inverses, factors = jax.vmap(factor)(blocks(diagonal), up_blocks)

    def precondition(residual):
        return jax.vmap(solve_block)(inverses, factors, up_blocks, blocks(residual)).reshape(LAYERS, NY, NX)

    source = sink_mask.astype(jnp.float32) * load_current
    right_side = jnp.concatenate([source[None], jnp.zeros((LAYERS - 1, NY, NX), jnp.float32)], 0)
    voltage = jnp.zeros((LAYERS, NY, NX), jnp.float32)
    residual = right_side
    precond = precondition(residual)
    direction = precond
    weight_now = jnp.sum(residual * precond)
    for iteration in range(ITERS):
        image_field = operate(direction)
        step_size = weight_now / jnp.sum(direction * image_field)
        voltage = voltage + step_size * direction
        residual = residual - step_size * image_field
        if iteration + 1 < ITERS:
            precond = precondition(residual)
            weight_next = jnp.sum(residual * precond)
            direction = precond + (weight_next / weight_now) * direction
            weight_now = weight_next
    return voltage, residual
```

```python
import jax
import jax.numpy as jnp
from jax import lax
from jax.sharding import Mesh
from jax.sharding import PartitionSpec as P

GX = ("gx_0", "gx_1")
GY = ("gy_0", "gy_1")
GX_GY_GZ = ("gx_0", "gx_1", "gy_0", "gy_1", "gz")


PAD_CONDUCTANCE = 20.0


def padded(array, sides, width):
    edges = {}
    for axis, dim in sides:
        peers, length = (lax.axis_size(axis), array.shape[dim])
        up = [(i, (i + 1) % peers) for i in range(peers)]
        last = lax.slice_in_dim(array, length - width, length, axis=dim)
        leading = lax.slice_in_dim(array, 0, width, axis=dim)
        edges[dim] = (
            lax.ppermute(last, axis, up),
            lax.ppermute(leading, axis, [(b, a) for a, b in up]),
        )
    done = []
    for _, dim in sides:
        low, high = edges[dim]
        around = [(width, width) if d in done else (0, 0) for d in range(array.ndim)]
        array = jnp.concatenate([jnp.pad(low, around), array, jnp.pad(high, around)], axis=dim)
        done.append(dim)
    return array


def padded_2(block, sides, width):
    for axis, dim in sides:
        count = lax.axis_size(axis)
        forward = [(i, i + 1) for i in range(count - 1)]
        backward = [(target, source) for source, target in forward]
        low = lax.ppermute(
            lax.slice_in_dim(block, block.shape[dim] - width, None, axis=dim), axis, forward
        )
        high = lax.ppermute(lax.slice_in_dim(block, 0, width, axis=dim), axis, backward)
        block = jnp.concatenate([low, block, high], axis=dim)
    return block


def lookup(classes, table):
    summed = jnp.zeros(classes.shape, jnp.float32)
    for level in range(table.shape[1]):
        summed = summed + jnp.where(
            classes == level, table[:, level][:, None, None], jnp.float32(0.0)
        )
    return summed


def harmonic(first, second):
    return 2.0 * first * second / (first + second)


def factor(diagonal, up_edge):
    inverses = []
    factors = []
    for level in range(diagonal.shape[0]):
        pivots = diagonal[level]
        if level > 0:
            pivots = pivots + up_edge[level - 1] * factors[level - 1]
        inverse = 1.0 / pivots
        inverses.append(inverse)
        factors.append(-up_edge[level] * inverse)
    return (jnp.stack(inverses), jnp.stack(factors))


def solve_block(inverses, factors, up_edge, source_term):
    forward = []
    for level in range(source_term.shape[0]):
        entries = source_term[level]
        if level > 0:
            entries = entries + up_edge[level - 1] * forward[level - 1]
        forward.append(entries * inverses[level])
    result = [forward[-1]]
    level = 0
    result.insert(0, forward[level] - factors[level] * result[0])
    return jnp.stack(result)


def plane_extend(field):
    return padded(field, ((GX, 2), (GY, 1)), 1)


def layer_extend(field):
    return padded_2(field, (("gz", 0),), 1)


def shards(load_current, sink_mask, pad_mask, plane_class, via_class, plane_table, via_table):
    n_layers, n_rows, n_cols = plane_class.shape
    g_plane = lookup(plane_class, plane_table)
    g_via = lookup(via_class, via_table)
    plane_ext = plane_extend(g_plane)
    middle = plane_ext[:, 1:-1, :]
    across = harmonic(middle[:, :, :-1], middle[:, :, 1:])
    east_edge = across[:, :, 1:]
    west_edge = across[:, :, :-1]
    column = plane_ext[:, :, 1:-1]
    along_rows = harmonic(column[:, :-1], column[:, 1:])
    north_edge = along_rows[:, 1:]
    south_edge = along_rows[:, :-1]
    via_ext = layer_extend(g_via)
    vertical = harmonic(via_ext[:-1], via_ext[1:])
    up_edge = vertical[1:]
    down_edge = vertical[:-1]
    group_index = lax.axis_index("gz")
    is_top = group_index == lax.axis_size("gz") - 1
    is_bottom = group_index == 0
    pad_plane = jnp.where(is_top, PAD_CONDUCTANCE * pad_mask.astype(jnp.float32), jnp.float32(0.0))
    pad_layer = jnp.concatenate(
        [jnp.zeros((n_layers - 1, n_rows, n_cols), jnp.float32), pad_plane[None]], 0
    )
    diagonal = east_edge + west_edge + north_edge + south_edge + up_edge + down_edge + pad_layer
    inverses, factors = factor(diagonal, up_edge)

    def precondition(residual):
        return solve_block(inverses, factors, up_edge, residual)

    def couple(field):
        inner = plane_extend(field)
        layer_ext = layer_extend(field)
        cross = jnp.concatenate(
            [down_edge[:1] * layer_ext[:1]]
            + [jnp.zeros_like(field[:1])] * (n_layers - 2)
            + [up_edge[-1:] * layer_ext[-1:]],
            0,
        )
        return (
            east_edge * inner[:, 1:-1, 2:]
            + west_edge * inner[:, 1:-1, :-2]
            + north_edge * inner[:, 2:, 1:-1]
            + south_edge * inner[:, :-2, 1:-1]
            + cross
        )

    def totals(*pairs):
        return lax.psum(jnp.stack([jnp.sum(a * b) for a, b in pairs]), GX_GY_GZ)

    source = jnp.where(is_bottom, sink_mask.astype(jnp.float32) * load_current, jnp.float32(0.0))
    s0 = jnp.concatenate(
        [source[None], jnp.zeros((n_layers - 1, n_rows, n_cols), jnp.float32)], 0
    )
    z0 = precondition(s0)
    s1 = s0 - couple(z0)
    mu, t00 = totals((z0, s0), (z0, s1))
    step, shift = mu / t00, t00 / mu
    z1 = z0 - step * precondition(s1)
    r1 = s0 - step * s1
    s2 = r1 - couple(z1)
    z2 = precondition(s2) - shift * z1
    s3 = (s2 - shift * r1) - couple(z2)
    sums = totals((z0, s2), (z2, s1), (z1, s2), (z2, s2), (z2, s3), (z1, s0), (z2, s0))
    t01, t02, t11, t12, t22, g1, g2 = sums / mu
    t00 = shift
    l1, l2 = t01 / t00, t02 / t00
    d1, e1 = t11 - l1 * t01, t12 - l1 * t02
    l3 = e1 / d1
    d2 = t22 - l2 * t02 - l3 * e1
    y1 = g1 - l1
    y2 = g2 - l2 - l3 * y1
    c2 = y2 / d2
    c1 = y1 / d1 - l3 * c2
    c0 = 1.0 / t00 - l1 * c1 - l2 * c2
    voltage = c0 * z0 + c1 * z1 + c2 * z2
    residual = s0 - c0 * s1 - c1 * s2 - c2 * s3
    return (voltage, residual)


def solution(mesh):
    split = Mesh(
        mesh.devices.reshape(8, 2, 2, 4, mesh.shape["gz"]), ("gx_0", "gx_1", "gy_0", "gy_1", "gz")
    )
    placed = (
        P(GY, GX),
        P(GY, GX),
        P(GY, GX),
        P("gz", GY, GX),
        P("gz", GY, GX),
        P("gz", None),
        P("gz", None),
    )
    return jax.shard_map(
        shards,
        mesh=split,
        in_specs=placed,
        out_specs=(P("gz", GY, GX), P("gz", GY, GX)),
        check_vma=False,
    )
```

```python
import functools

import jax
import jax.numpy as jnp
from jax import lax
from jax.experimental import pallas as pl
from jax.experimental.pallas import tpu as pltpu
from jax.sharding import PartitionSpec as P

PAD_CONDUCTANCE = 20.0
MESH = pl.DeviceIdType.MESH
HALO = 8
LANES = 128
F32 = jnp.float32


def harmonic(first, second):
    return 2.0 * first * second / (first + second)


def pick(classes, table):
    low = (classes & 1) == 1
    mid = (classes & 2) == 2
    high = (classes & 4) == 4
    pairs = [jnp.where(low, table[2 * k + 1], table[2 * k]) for k in range(4)]
    return jnp.where(
        high, jnp.where(mid, pairs[3], pairs[2]), jnp.where(mid, pairs[1], pairs[0])
    )


def kernel(
    sizes,
    load_ref, sink_ref, pad_ref, plane_ref, via_ref, plane_tab, via_tab,
    volt_ref, resid_ref,
    class_n, class_s, class_e, class_w, via_other, tab_other,
    g_buf, g_e, g_w,
    east, west, north, south, cross, inv0, inv1, mix, src,
    z0, z0_e, z0_w, z0_o, y1, y1_e, y1_w, y1_o, z1, z1_e, z1_w, z1_o, z2, z2_e, z2_w, z2_o,
    s1, s2, q2, s3,
    part, got_x, got_y, got_z, send_sem, recv_sem,
):
    nx, ny, rows, cols = sizes
    strips = rows // 8
    ix, iy, iz = lax.axis_index("gx"), lax.axis_index("gy"), lax.axis_index("gz")
    gx_up, gx_dn = lax.rem(ix + 1, nx), lax.rem(ix + nx - 1, nx)
    gy_up, gy_dn = lax.rem(iy + 1, ny), lax.rem(iy + ny - 1, ny)
    other = 1 - iz
    used = [0]

    def copy(source, target, where_to):
        k = used[0]
        used[0] += 1
        return pltpu.make_async_remote_copy(
            src_ref=source, dst_ref=target, send_sem=send_sem.at[k], recv_sem=recv_sem.at[k],
            device_id=where_to, device_id_type=MESH,
        )

    barrier = pltpu.get_barrier_semaphore()
    peers = [{"gx": lax.rem(ix + k, nx)} for k in range(1, nx)]
    peers += [{"gy": lax.rem(iy + k, ny)} for k in range(1, ny)]
    peers += [{"gz": other}]
    for peer in peers:
        pl.semaphore_signal(barrier, inc=1, device_id=peer, device_id_type=MESH)
    pl.semaphore_wait(barrier, len(peers))

    first = [
        copy(via_ref.at[other], via_other, {"gz": other}),
        copy(via_tab, tab_other, {"gz": other}),
        copy(plane_ref.at[:, pl.ds(rows - 8, 8), :], class_s, {"gy": gy_up}),
        copy(plane_ref.at[:, pl.ds(0, 8), :], class_n, {"gy": gy_dn}),
        copy(plane_ref.at[:, :, pl.ds(cols - LANES, LANES)], class_w, {"gx": gx_up}),
        copy(plane_ref.at[:, :, pl.ds(0, LANES)], class_e, {"gx": gx_dn}),
    ]
    for c in first:
        c.start()

    def own_table(tab, slot):
        line = jnp.where(iz == 0, tab[slot : slot + 1, :], tab[1 - slot : 2 - slot, :])
        return [line[:, k : k + 1] for k in range(8)]

    plane_of = [own_table(plane_tab, slot) for slot in (0, 1)]
    via_of = [own_table(via_tab, slot) for slot in (0, 1)]
    layer = (iz, other)

    def at(i):
        return pl.ds(pl.multiple_of(i * 8, 8), 8)

    def inner(i):
        return pl.ds(pl.multiple_of(i * 8 + HALO, 8), 8)

    def lookup_own(i, _):
        for slot in (0, 1):
            g_buf[slot, inner(i), :] = pick(plane_ref[layer[slot], at(i), :], plane_of[slot])
        return 0

    lax.fori_loop(0, strips, lookup_own, 0)
    for c in first:
        c.wait()
    for slot in (0, 1):
        g_buf[slot, 0:HALO, :] = pick(class_s[layer[slot]], plane_of[slot])
        g_buf[slot, HALO + rows : 2 * HALO + rows, :] = pick(class_n[layer[slot]], plane_of[slot])

    other_line = jnp.where(iz == 0, tab_other[0:1, :], tab_other[1:2, :])
    other_of = [other_line[:, k : k + 1] for k in range(8)]

    def lookup_sides(i, _):
        for slot in (0, 1):
            g_e[slot, at(i), :] = pick(class_e[layer[slot], at(i), :], plane_of[slot])
            g_w[slot, at(i), :] = pick(class_w[layer[slot], at(i), :], plane_of[slot])
        return 0

    lax.fori_loop(0, strips, lookup_sides, 0)

    def around(buf, buf_e, buf_w, slot, i):
        here = buf[slot, inner(i), :]
        below = buf[slot, pl.ds(pl.multiple_of(i * 8, 8), 8), :]
        above = buf[slot, pl.ds(pl.multiple_of(i * 8 + 2 * HALO, 8), 8), :]
        up = jnp.concatenate([here[1:], above[:1]], 0)
        down = jnp.concatenate([below[7:], here[:7]], 0)
        right = pltpu.roll(
            jnp.concatenate([here, buf_e[slot, at(i), :]], 1), cols + LANES - 1, 1
        )[:, :cols]
        left = pltpu.roll(jnp.concatenate([buf_w[slot, at(i), :], here], 1), 1, 1)[:, LANES:]
        return here, right, left, up, down

    is_source = jnp.where(iz == 0, F32(1.0), F32(0.0))
    pad_scale = jnp.where(iz == 0, F32(0.0), F32(PAD_CONDUCTANCE))

    def solve(i, b0, b1):
        i0, i1, m = inv0[at(i), :], inv1[at(i), :], mix[at(i), :]
        x1 = (b1 + m * b0) * i1
        return b0 * i0 + m * x1, x1

    def build(i, _):
        sums = []
        for slot in (0, 1):
            here, right, left, up, down = around(g_buf, g_e, g_w, slot, i)
            edges = [harmonic(here, near) for near in (right, left, up, down)]
            for ref, value in zip((east, west, north, south), edges):
                ref[slot, at(i), :] = value
            sums.append(edges[0] + edges[1] + edges[2] + edges[3])
        via0 = pick(via_ref[layer[0], at(i), :], via_of[0])
        via1 = pick(via_ref[layer[1], at(i), :], via_of[1])
        link = harmonic(via0, via1)
        far = harmonic(via1, pick(via_other[at(i), :], other_of))
        cross[at(i), :] = far
        d0 = sums[0] + link + pad_scale * pad_ref[at(i), :].astype(F32)
        d1 = sums[1] + link + far
        i0 = 1.0 / d0
        m = link * i0
        i1 = 1.0 / (d1 - link * m)
        inv0[at(i), :] = i0
        inv1[at(i), :] = i1
        mix[at(i), :] = m
        b0 = is_source * (sink_ref[at(i), :].astype(F32) * load_ref[at(i), :])
        src[at(i), :] = b0
        x1 = m * b0 * i1
        z0[0, inner(i), :] = b0 * i0 + m * x1
        z0[1, inner(i), :] = x1
        return 0

    lax.fori_loop(0, strips, build, 0)

    def exchange(buf, buf_e, buf_w, buf_o):
        moves = [
            copy(buf.at[1, pl.ds(HALO, rows), :], buf_o, {"gz": other}),
            copy(buf.at[:, pl.ds(rows, 8), :], buf.at[:, pl.ds(0, 8), :], {"gy": gy_up}),
            copy(buf.at[:, pl.ds(HALO, 8), :], buf.at[:, pl.ds(HALO + rows, 8), :], {"gy": gy_dn}),
            copy(buf.at[:, pl.ds(HALO, rows), pl.ds(cols - LANES, LANES)], buf_w, {"gx": gx_up}),
            copy(buf.at[:, pl.ds(HALO, rows), pl.ds(0, LANES)], buf_e, {"gx": gx_dn}),
        ]
        for c in moves:
            c.start()
        return moves

    def couple(buf, buf_e, buf_w, buf_o, i):
        out = []
        for slot in (0, 1):
            here, right, left, up, down = around(buf, buf_e, buf_w, slot, i)
            u = (
                east[slot, at(i), :] * right + west[slot, at(i), :] * left
                + north[slot, at(i), :] * up + south[slot, at(i), :] * down
            )
            if slot == 1:
                u = u + cross[at(i), :] * buf_o[at(i), :]
            out.append((here, u))
        return out

    lane = lax.broadcasted_iota(jnp.int32, (1, LANES), 1)

    def all_sum(which, sums):
        line = jnp.zeros((1, LANES), F32)
        for k, value in enumerate(sums):
            line = jnp.where(lane == k, jnp.sum(value), line)
        for stage, (axis, size, me, got) in enumerate(
            (("gx", nx, ix, got_x), ("gy", ny, iy, got_y), ("gz", 2, iz, got_z))
        ):
            part[which, stage] = line
            got[which, me] = line
            moves = [
                copy(part.at[which, stage], got.at[which, me], {axis: lax.rem(me + k, size)})
                for k in range(1, size)
            ]
            for c in moves:
                c.start()
            for c in moves:
                c.wait()
            line = got[which, 0]
            for k in range(1, size):
                line = line + got[which, k]
        return [
            jnp.sum(jnp.where(lane == k, line, 0.0), axis=1, keepdims=True)
            for k in range(len(sums))
        ]

    zero = jnp.zeros((8, cols), F32)

    for c in exchange(z0, z0_e, z0_w, z0_o):
        c.wait()

    def pass1(i, carry):
        (h0, u0), (h1, u1) = couple(z0, z0_e, z0_w, z0_o, i)
        b0 = src[at(i), :]
        a0, a1 = b0 - u0, -u1
        s1[0, at(i), :] = a0
        s1[1, at(i), :] = a1
        x0, x1 = solve(i, a0, a1)
        y1[0, inner(i), :] = x0
        y1[1, inner(i), :] = x1
        return carry[0] + h0 * b0, carry[1] + (h0 * a0 + h1 * a1)

    sums = lax.fori_loop(0, strips, pass1, (zero, zero))
    moves = exchange(y1, y1_e, y1_w, y1_o)
    mu, t00 = all_sum(0, sums)
    for c in moves:
        c.wait()
    step, shift = mu / t00, t00 / mu

    def blend(i, _):
        for slot in (0, 1):
            for a, b, c in ((z0_e, y1_e, z1_e), (z0_w, y1_w, z1_w)):
                c[slot, at(i), :] = a[slot, at(i), :] - step * b[slot, at(i), :]
            z1[slot, inner(i), :] = z0[slot, inner(i), :] - step * y1[slot, inner(i), :]
        z1_o[at(i), :] = z0_o[at(i), :] - step * y1_o[at(i), :]
        return 0

    lax.fori_loop(0, strips, blend, 0)
    for slot in (0, 1):
        for lo in (0, HALO + rows):
            z1[slot, lo : lo + 8, :] = z0[slot, lo : lo + 8, :] - step * y1[slot, lo : lo + 8, :]

    def pass2(i, carry):
        (h0, u0), (h1, u1) = couple(z1, z1_e, z1_w, z1_o, i)
        b0 = src[at(i), :]
        r0, r1 = b0 - step * s1[0, at(i), :], -step * s1[1, at(i), :]
        a0, a1 = r0 - u0, r1 - u1
        s2[0, at(i), :] = a0
        s2[1, at(i), :] = a1
        q2[0, at(i), :] = a0 - shift * r0
        q2[1, at(i), :] = a1 - shift * r1
        x0, x1 = solve(i, a0, a1)
        z2[0, inner(i), :] = x0 - shift * h0
        z2[1, inner(i), :] = x1 - shift * h1
        f0, f1 = z0[0, inner(i), :], z0[1, inner(i), :]
        return (
            carry[0] + (f0 * a0 + f1 * a1),
            carry[1] + (h0 * a0 + h1 * a1),
            carry[2] + h0 * b0,
        )

    mids = lax.fori_loop(0, strips, pass2, (zero, zero, zero))
    for c in exchange(z2, z2_e, z2_w, z2_o):
        c.wait()

    def pass3(i, carry):
        (h0, u0), (h1, u1) = couple(z2, z2_e, z2_w, z2_o, i)
        a0, a1 = q2[0, at(i), :] - u0, q2[1, at(i), :] - u1
        s3[0, at(i), :] = a0
        s3[1, at(i), :] = a1
        return (
            carry[0] + (h0 * s1[0, at(i), :] + h1 * s1[1, at(i), :]),
            carry[1] + (h0 * s2[0, at(i), :] + h1 * s2[1, at(i), :]),
            carry[2] + (h0 * a0 + h1 * a1),
            carry[3] + h0 * src[at(i), :],
        )

    lasts = lax.fori_loop(0, strips, pass3, (zero, zero, zero, zero))
    totals = all_sum(1, (*mids, *lasts))
    t01, t11, g1, t02, t12, t22, g2 = [t / mu for t in totals]
    l1, l2 = t01 / shift, t02 / shift
    d1, e1 = t11 - l1 * t01, t12 - l1 * t02
    l3 = e1 / d1
    d2 = t22 - l2 * t02 - l3 * e1
    b1 = g1 - l1
    b2 = g2 - l2 - l3 * b1
    c2 = b2 / d2
    c1 = b1 / d1 - l3 * c2
    c0 = step - l1 * c1 - l2 * c2

    def finish(i, _):
        for slot in (0, 1):
            volt_ref[layer[slot], at(i), :] = (
                c0 * z0[slot, inner(i), :] + c1 * z1[slot, inner(i), :] + c2 * z2[slot, inner(i), :]
            )
            tail = (
                c0 * s1[slot, at(i), :] + c1 * s2[slot, at(i), :] + c2 * s3[slot, at(i), :]
            )
            resid_ref[layer[slot], at(i), :] = (src[at(i), :] - tail) if slot == 0 else -tail
        return 0

    lax.fori_loop(0, strips, finish, 0)


def solution(mesh):
    nx, ny = mesh.shape["gx"], mesh.shape["gy"]

    def shards(load_current, sink_mask, pad_mask, plane_class, via_class, plane_table, via_table):
        _, rows, cols = plane_class.shape
        flat = pltpu.VMEM((rows, cols), F32)
        both = pltpu.VMEM((2, rows, cols), F32)
        tall = pltpu.VMEM((2, rows + 2 * HALO, cols), F32)
        side = pltpu.VMEM((2, rows, LANES), F32)
        side_i = pltpu.VMEM((2, rows, LANES), jnp.int32)
        edge_i = pltpu.VMEM((2, 8, cols), jnp.int32)
        field = [tall, side, side, flat]
        copies = 6 + 3 * 5 + 2 * (nx - 1 + ny - 1 + 1)
        scratch = [
            edge_i, edge_i, side_i, side_i, pltpu.VMEM((rows, cols), jnp.int32),
            pltpu.VMEM(via_table.shape, F32),
            tall, side, side,
            both, both, both, both, flat, flat, flat, flat, flat,
            *field, *field, *field, *field,
            both, both, both, both,
            pltpu.VMEM((2, 3, 1, LANES), F32),
            pltpu.VMEM((2, nx, 1, LANES), F32),
            pltpu.VMEM((2, ny, 1, LANES), F32),
            pltpu.VMEM((2, 2, 1, LANES), F32),
            pltpu.SemaphoreType.DMA((copies,)),
            pltpu.SemaphoreType.DMA((copies,)),
        ]
        shape = jax.ShapeDtypeStruct(plane_class.shape, F32)
        vmem = pl.BlockSpec(memory_space=pltpu.VMEM)
        return pl.pallas_call(
            functools.partial(kernel, (nx, ny, rows, cols)),
            out_shape=(shape, shape),
            in_specs=[vmem] * 7,
            out_specs=(vmem, vmem),
            scratch_shapes=scratch,
            compiler_params=pltpu.CompilerParams(
                collective_id=0, has_side_effects=True, vmem_limit_bytes=56 * 1024 * 1024
            ),
        )(load_current, sink_mask, pad_mask, plane_class, via_class, plane_table, via_table)

    layers = P("gz", "gy", "gx")
    plane = P("gy", "gx")
    table = P("gz", None)
    return jax.shard_map(
        shards,
        mesh=mesh,
        in_specs=(plane, plane, plane, layers, layers, table, table),
        out_specs=(layers, layers),
        check_vma=False,
    )
```

```python
import functools

import jax
import jax.numpy as jnp
from jax import lax
from jax.experimental import pallas as pl
from jax.experimental.pallas import tpu as pltpu
from jax.sharding import PartitionSpec as P

PAD_CONDUCTANCE = 20.0
MESH = pl.DeviceIdType.MESH
HALO = 8
LANES = 128
CHUNK = 24
F32 = jnp.float32


def harmonic(first, second):
    return 2.0 * first * second / (first + second)


def pick(classes, table):
    low = (classes & 1) == 1
    mid = (classes & 2) == 2
    high = (classes & 4) == 4
    pairs = [jnp.where(low, table[2 * k + 1], table[2 * k]) for k in range(4)]
    return jnp.where(
        high, jnp.where(mid, pairs[3], pairs[2]), jnp.where(mid, pairs[1], pairs[0])
    )


def fold(value):
    return sum(
        value[:, k : k + LANES] for k in range(LANES, value.shape[1], LANES)
    ) + value[:, :LANES]


def kernel(
    sizes,
    load_h, sink_h, pad_h, plane_h, via_h, plane_tab, via_tab,
    volt_h, resid_h,
    load_ref, sink_ref, pad_ref, plane_ref, via_ref, volt_ref, resid_ref,
    via_mine, via_far,
    g_buf, g_e, g_w,
    east, west, north, south, cross, inv0, inv1, mix, src,
    z0, z0_e, z0_w, z0_o, y1, y1_e, y1_w, y1_o, h2, h2_e, h2_w, h2_o, z2, z2_e, z2_w,
    s1, s2, s3,
    part, got_x, got_y, got_z, first_sum,
    in_sem, out_sem, far_send, far_recv, side_send, side_recv, edge_send, edge_recv,
    sum_send, sum_recv,
):
    nx, ny, rows, cols = sizes
    chunks = rows // CHUNK
    per = CHUNK // 8
    ix, iy, iz = lax.axis_index("gx"), lax.axis_index("gy"), lax.axis_index("gz")
    gx_up, gx_dn = lax.rem(ix + 1, nx), lax.rem(ix + nx - 1, nx)
    gy_up, gy_dn = lax.rem(iy + 1, ny), lax.rem(iy + ny - 1, ny)
    other = 1 - iz
    layer = (iz, other)

    fetch = [
        pltpu.make_async_copy(a, b, in_sem.at[k])
        for k, (a, b) in enumerate(
            (
                (via_h, via_ref), (plane_h, plane_ref), (pad_h, pad_ref),
                (sink_h, sink_ref), (load_h, load_ref),
            )
        )
    ]
    for c in fetch:
        c.start()

    barrier = pltpu.get_barrier_semaphore()
    peers = [{"gx": lax.rem(ix + k, nx)} for k in range(1, nx)]
    peers += [{"gy": lax.rem(iy + k, ny)} for k in range(1, ny)]
    peers += [{"gz": other}]
    for peer in peers:
        pl.semaphore_signal(barrier, inc=1, device_id=peer, device_id_type=MESH)
    pl.semaphore_wait(barrier, len(peers))

    def at(c, j=0, n=8):
        return pl.ds(pl.multiple_of(c * CHUNK + 8 * j, 8), n)

    def inner(c, j=0, n=8):
        return pl.ds(pl.multiple_of(c * CHUNK + (8 * j + HALO), 8), n)

    def remote(source, target, send, recv, where_to):
        return pltpu.make_async_remote_copy(
            src_ref=source, dst_ref=target, send_sem=send, recv_sem=recv,
            device_id=where_to, device_id_type=MESH,
        )

    def far_copy(stage, c):
        buf, out = ((via_mine, via_far), (z0, z0_o), (y1, y1_o), (h2, h2_o))[stage]
        source = buf.at[at(c, 0, CHUNK), :] if stage == 0 else buf.at[1, inner(c, 0, CHUNK), :]
        return remote(
            source, out.at[at(c, 0, CHUNK), :],
            far_send.at[stage, c], far_recv.at[stage, c], {"gz": other},
        )

    fields = ((z0, z0_e, z0_w), (y1, y1_e, y1_w), (h2, h2_e, h2_w), (g_buf, g_e, g_w))

    def side_copies(stage, c):
        buf, buf_e, buf_w = fields[stage]
        span = inner(c, 0, CHUNK)
        return [
            remote(
                buf.at[:, span, pl.ds(cols - LANES, LANES)], buf_w.at[:, at(c, 0, CHUNK), :],
                side_send.at[stage, 0, c], side_recv.at[stage, 0, c], {"gx": gx_up},
            ),
            remote(
                buf.at[:, span, pl.ds(0, LANES)], buf_e.at[:, at(c, 0, CHUNK), :],
                side_send.at[stage, 1, c], side_recv.at[stage, 1, c], {"gx": gx_dn},
            ),
        ]

    def edge_copy(stage, way):
        buf = fields[stage][0]
        if way == 0:
            span, out, where_to = pl.ds(rows, 8), pl.ds(0, 8), gy_up
        else:
            span, out, where_to = pl.ds(HALO, 8), pl.ds(HALO + rows, 8), gy_dn
        return remote(
            buf.at[:, span, :], buf.at[:, out, :],
            edge_send.at[stage, way], edge_recv.at[stage, way], {"gy": where_to},
        )

    def send_chunk(stage, c):
        for move in side_copies(stage, c):
            move.start()

        @pl.when(c == chunks - 1)
        def _():
            edge_copy(stage, 0).start()

        @pl.when(c == 0)
        def _():
            edge_copy(stage, 1).start()

    def await_chunk(stage, c):
        for move in side_copies(stage, c):
            move.wait_recv()

        @pl.when(c == 0)
        def _():
            edge_copy(stage, 0).wait_recv()

        @pl.when(c == chunks - 1)
        def _():
            edge_copy(stage, 1).wait_recv()

    def turn(k, shift):
        return lax.rem(k + shift, chunks)

    plane_of = [[plane_tab[layer[slot], k] for k in range(8)] for slot in (0, 1)]
    via_of = [[via_tab[layer[slot], k] for k in range(8)] for slot in (0, 1)]

    fetch[0].wait()

    def lookup_far(k, _):
        c = turn(k, chunks - 1)
        for j in range(per):
            via_mine[at(c, j), :] = pick(via_ref[other, at(c, j), :], via_of[1])
        far_copy(0, c).start()
        return 0

    lax.fori_loop(0, chunks, lookup_far, 0)
    fetch[1].wait()

    def lookup_own(c, _):
        for slot in (0, 1):
            for j in range(per):
                g_buf[slot, inner(c, j), :] = pick(
                    plane_ref[layer[slot], at(c, j), :], plane_of[slot]
                )
        send_chunk(3, c)
        return 0

    lax.fori_loop(0, chunks, lookup_own, 0)

    @pl.when(iz == 0)
    def _():
        def clear(c, _):
            z0_o[at(c, 0, CHUNK), :] = jnp.zeros((CHUNK, cols), F32)
            return 0

        lax.fori_loop(0, chunks, clear, 0)

    for c in fetch[2:]:
        c.wait()

    def around(field, slot, c, j):
        buf, buf_e, buf_w = field
        here = buf[slot, inner(c, j), :]
        below = buf[slot, at(c, j), :]
        above = buf[slot, at(c, j + 2), :]
        up = jnp.concatenate([here[1:], above[:1]], 0)
        down = jnp.concatenate([below[7:], here[:7]], 0)
        right = pltpu.roll(
            jnp.concatenate([here, buf_e[slot, at(c, j), :]], 1), cols + LANES - 1, 1
        )[:, :cols]
        left = pltpu.roll(
            jnp.concatenate([buf_w[slot, at(c, j), :], here], 1), 1, 1
        )[:, LANES:]
        return here, right, left, up, down

    is_source = jnp.where(iz == 0, F32(1.0), F32(0.0))
    pad_scale = jnp.where(iz == 0, F32(0.0), F32(PAD_CONDUCTANCE))

    def solve(span, b0, b1):
        m = mix[span, :]
        x1 = (b1 + m * b0) * inv1[span, :]
        return b0 * inv0[span, :] + m * x1, x1

    def plane_edges(slot, c):
        sums = []
        below = g_buf[slot, at(c), :]
        here = g_buf[slot, inner(c), :]
        last = harmonic(below, jnp.concatenate([below[1:], here[:1]], 0))
        for j in range(per):
            span = at(c, j)
            here = g_buf[slot, inner(c, j), :]
            above = g_buf[slot, at(c, j + 2), :]
            wide = jnp.concatenate([g_w[slot, span, :], here, g_e[slot, span, :]], 1)
            edge = harmonic(wide, pltpu.roll(wide, cols + 2 * LANES - 1, 1))[:, : cols + LANES]
            e = edge[:, LANES:]
            w = pltpu.roll(edge, 1, 1)[:, LANES:]
            n = harmonic(here, jnp.concatenate([here[1:], above[:1]], 0))
            s = jnp.concatenate([last[7:], n[:7]], 0)
            last = n
            east[slot, span, :] = e
            west[slot, span, :] = w
            north[slot, span, :] = n
            south[slot, span, :] = s
            sums.append(e + w + n + s)
        return sums

    def build(k, _):
        c = turn(k, chunks - 1)
        await_chunk(3, c)
        sums = [plane_edges(slot, c) for slot in (0, 1)]
        far_copy(0, c).wait_recv()
        for j in range(per):
            span = at(c, j)
            via0 = pick(via_ref[iz, span, :], via_of[0])
            via1 = via_mine[span, :]
            link = harmonic(via0, via1)
            far = harmonic(via1, via_far[span, :])
            cross[span, :] = far
            d0 = sums[0][j] + link + pad_scale * pad_ref[span, :].astype(F32)
            d1 = sums[1][j] + link + far
            i0 = 1.0 / d0
            m = link * i0
            i1 = 1.0 / (d1 - link * m)
            inv0[span, :] = i0
            inv1[span, :] = i1
            mix[span, :] = m
            b0 = is_source * (sink_ref[span, :].astype(F32) * load_ref[span, :])
            src[span, :] = b0
            x1 = m * b0 * i1
            z0[0, inner(c, j), :] = b0 * i0 + m * x1
            z0[1, inner(c, j), :] = x1

        @pl.when(iz == 0)
        def _():
            far_copy(1, c).start()

        send_chunk(0, c)
        return 0

    lax.fori_loop(0, chunks, build, 0)

    def couple(field, slot, c, j):
        here, right, left, up, down = around(field, slot, c, j)
        span = at(c, j)
        u = (
            east[slot, span, :] * right + west[slot, span, :] * left
            + north[slot, span, :] * up + south[slot, span, :] * down
        )
        return here, u

    zero = jnp.zeros((8, LANES), F32)

    def pass1(k, carry):
        c = turn(k, 0)
        mu, t00 = carry
        await_chunk(0, c)

        @pl.when(iz == 1)
        def _():
            far_copy(1, c).wait_recv()

        for j in range(per):
            span = at(c, j)
            h0, u0 = couple(fields[0], 0, c, j)
            h1, u1 = couple(fields[0], 1, c, j)
            b0 = src[span, :]
            a0, a1 = b0 - u0, -(u1 + cross[span, :] * z0_o[span, :])
            s1[0, span, :] = a0
            s1[1, span, :] = a1
            x0, x1 = solve(span, a0, a1)
            y1[0, inner(c, j), :] = x0
            y1[1, inner(c, j), :] = x1
            mu = mu + fold(h0 * b0)
            t00 = t00 + fold(h0 * a0 + h1 * a1)
        far_copy(2, c).start()
        send_chunk(1, c)
        return mu, t00

    sums = lax.fori_loop(0, chunks, pass1, (zero, zero))

    lane = lax.broadcasted_iota(jnp.int32, (1, LANES), 1)
    axes = (("gx", nx, ix, got_x), ("gy", ny, iy, got_y), ("gz", 2, iz, got_z))
    offset = (0, nx, nx + ny)

    def line_of(values):
        line = jnp.zeros((1, LANES), F32)
        for k, value in enumerate(values):
            line = jnp.where(lane == k, jnp.sum(value), line)
        return line

    def sum_moves(which, stage):
        axis, size, me, got = axes[stage]
        return [
            remote(
                part.at[which, stage], got.at[which, me],
                sum_send.at[which, offset[stage] + k], sum_recv.at[which, offset[stage] + k],
                {axis: lax.rem(me + k, size)},
            )
            for k in range(1, size)
        ]

    def sum_start(which, stage, line):
        part[which, stage] = line
        axes[stage][3][which, axes[stage][2]] = line
        for c in sum_moves(which, stage):
            c.start()

    def sum_finish(which, stage):
        _, size, _, got = axes[stage]
        for c in sum_moves(which, stage):
            c.wait()
        line = got[which, 0]
        for k in range(1, size):
            line = line + got[which, k]
        return line

    def hand_over():
        return remote(
            part.at[0, 2], first_sum, sum_send.at[0, nx + ny], sum_recv.at[0, nx + ny], {"gz": other}
        )

    first_line = line_of(sums)

    @pl.when(iz == 0)
    def _():
        sum_start(0, 0, first_line)

    def pass2(k, _):
        c = turn(k, 1)
        await_chunk(1, c)
        far_copy(2, c).wait_recv()
        for j in range(per):
            span = at(c, j)
            _, u0 = couple(fields[1], 0, c, j)
            _, u1 = couple(fields[1], 1, c, j)
            a0 = s1[0, span, :] - u0
            a1 = s1[1, span, :] - (u1 + cross[span, :] * y1_o[span, :])
            s2[0, span, :] = a0
            s2[1, span, :] = a1
            x0, x1 = solve(span, a0, a1)
            h2[0, inner(c, j), :] = x0
            h2[1, inner(c, j), :] = x1
        far_copy(3, c).start()
        send_chunk(2, c)

        @pl.when(jnp.logical_and(iz == 0, k == chunks // 2))
        def _():
            sum_start(0, 1, sum_finish(0, 0))

        return 0

    lax.fori_loop(0, chunks, pass2, 0)

    @pl.when(iz == 0)
    def _():
        line = sum_finish(0, 1)
        part[0, 2] = line
        first_sum[...] = line
        hand_over().start()
        hand_over().wait_send()

    @pl.when(iz == 1)
    def _():
        hand_over().wait_recv()

    def take(line, k):
        return jnp.sum(jnp.where(lane == k, line, 0.0), axis=1, keepdims=True)

    line = first_sum[...]
    mu, t00 = take(line, 0), take(line, 1)
    step, shift = mu / t00, t00 / mu

    def third(a, b, c):
        return (b - step * c) - shift * (a - step * b)

    def blend(c, _):
        for slot in (0, 1):
            for j in range(per):
                span = inner(c, j)
                z2[slot, span, :] = third(z0[slot, span, :], y1[slot, span, :], h2[slot, span, :])
        return 0

    lax.fori_loop(0, chunks, blend, 0)

    def pass3(k, carry):
        c = jnp.where(k < chunks - 2, k + 1, jnp.where(k == chunks - 2, 0, chunks - 1))
        await_chunk(2, c)

        @pl.when(c == 0)
        def _():
            for slot in (0, 1):
                z2[slot, 0:8, :] = third(z0[slot, 0:8, :], y1[slot, 0:8, :], h2[slot, 0:8, :])

        @pl.when(c == chunks - 1)
        def _():
            top = pl.ds(HALO + rows, 8)
            for slot in (0, 1):
                z2[slot, top, :] = third(z0[slot, top, :], y1[slot, top, :], h2[slot, top, :])

        t01, t11, g1, t02, t12, t22, g2 = carry
        for j in range(per):
            span = at(c, j)
            b0 = src[span, :]
            for slot in (0, 1):
                z2_e[slot, span, :] = third(z0_e[slot, span, :], y1_e[slot, span, :], h2_e[slot, span, :])
                z2_w[slot, span, :] = third(z0_w[slot, span, :], y1_w[slot, span, :], h2_w[slot, span, :])
                h, u = couple((z2, z2_e, z2_w), slot, c, j)
                first = s1[slot, span, :]
                second = first - step * s2[slot, span, :]
                r1 = (b0 - step * first) if slot == 0 else -step * first
                a = (second - shift * r1) - u
                s2[slot, span, :] = second
                s3[slot, span, :] = a
                p = z0[slot, inner(c, j), :]
                q = p - step * y1[slot, inner(c, j), :]
                t01 = t01 + fold(p * second)
                t11 = t11 + fold(q * second)
                t02 = t02 + fold(h * first)
                t12 = t12 + fold(h * second)
                t22 = t22 + fold(h * a)
                if slot == 0:
                    g1 = g1 + fold(q * b0)
                    g2 = g2 + fold(h * b0)
        return t01, t11, g1, t02, t12, t22, g2

    sums = list(lax.fori_loop(0, chunks, pass3, (zero,) * 7))

    def cross_term(k, carry):
        c = turn(k, 1)
        far_copy(3, c).wait_recv()
        for j in range(per):
            span = at(c, j)
            far = cross[span, :] * third(z0_o[span, :], y1_o[span, :], h2_o[span, :])
            s3[1, span, :] = s3[1, span, :] - far
            carry = carry + fold(z2[1, inner(c, j), :] * far)
        return carry

    def far_part():
        return lax.fori_loop(0, chunks, cross_term, zero)

    sums[5] = sums[5] - 2.0 * lax.cond(iz == 0, far_part, lambda: zero)
    line = line_of(sums)
    for stage in range(3):
        sum_start(1, stage, line)
        line = sum_finish(1, stage)

    @pl.when(iz == 1)
    def _():
        far_part()

    t01, t11, g1, t02, t12, t22, g2 = [take(line, k) / mu for k in range(7)]
    l1, l2 = t01 / shift, t02 / shift
    d1, e1 = t11 - l1 * t01, t12 - l1 * t02
    l3 = e1 / d1
    d2 = t22 - l2 * t02 - l3 * e1
    b1 = g1 - l1
    b2 = g2 - l2 - l3 * b1
    c2 = b2 / d2
    c1 = b1 / d1 - l3 * c2
    c0 = step - l1 * c1 - l2 * c2

    def result_copies(c):
        span = at(c, 0, CHUNK)
        return [
            pltpu.make_async_copy(a.at[:, span, :], b.at[:, span, :], out_sem.at[k, c])
            for k, (a, b) in enumerate(((volt_ref, volt_h), (resid_ref, resid_h)))
        ]

    def finish(c, _):
        for slot in (0, 1):
            for j in range(per):
                span, wide = at(c, j), inner(c, j)
                p = z0[slot, wide, :]
                volt_ref[layer[slot], span, :] = (
                    c0 * p + c1 * (p - step * y1[slot, wide, :]) + c2 * z2[slot, wide, :]
                )
                tail = c0 * s1[slot, span, :] + c1 * s2[slot, span, :] + c2 * s3[slot, span, :]
                resid_ref[layer[slot], span, :] = (src[span, :] - tail) if slot == 0 else -tail
        for move in result_copies(c):
            move.start()
        return 0

    lax.fori_loop(0, chunks, finish, 0)

    def drain(c, _):
        for move in result_copies(c):
            move.wait()
        for stage in range(4):
            if stage == 1:

                @pl.when(iz == 0)
                def _():
                    far_copy(1, c).wait_send()

            else:
                far_copy(stage, c).wait_send()
            for move in side_copies(stage, c):
                move.wait_send()
        return 0

    lax.fori_loop(0, chunks, drain, 0)
    for stage in range(4):
        for way in (0, 1):
            edge_copy(stage, way).wait_send()


def solution(mesh):
    nx, ny = mesh.shape["gx"], mesh.shape["gy"]

    def shards(load_current, sink_mask, pad_mask, plane_class, via_class, plane_table, via_table):
        _, rows, cols = plane_class.shape
        chunks = rows // CHUNK
        flat = pltpu.VMEM((rows, cols), F32)
        flat_i = pltpu.VMEM((rows, cols), jnp.int32)
        both = pltpu.VMEM((2, rows, cols), F32)
        both_i = pltpu.VMEM((2, rows, cols), jnp.int32)
        tall = pltpu.VMEM((2, rows + 2 * HALO, cols), F32)
        side = pltpu.VMEM((2, rows, LANES), F32)
        field = [tall, side, side, flat]
        dma = pltpu.SemaphoreType.DMA
        scratch = [
            flat, flat_i, flat_i, both_i, both_i, both, both,
            flat, flat,
            tall, side, side,
            both, both, both, both, flat, flat, flat, flat, flat,
            *field, *field, *field, tall, side, side,
            both, both, both,
            pltpu.VMEM((2, 3, 1, LANES), F32),
            pltpu.VMEM((2, nx, 1, LANES), F32),
            pltpu.VMEM((2, ny, 1, LANES), F32),
            pltpu.VMEM((2, 2, 1, LANES), F32),
            pltpu.VMEM((1, LANES), F32),
            dma((5,)), dma((2, chunks)),
            dma((4, chunks)), dma((4, chunks)),
            dma((4, 2, chunks)), dma((4, 2, chunks)),
            dma((4, 2)), dma((4, 2)),
            dma((2, nx + ny + 2)), dma((2, nx + ny + 2)),
        ]
        shape = jax.ShapeDtypeStruct(plane_class.shape, F32)
        hbm = pl.BlockSpec(memory_space=pl.ANY)
        smem = pl.BlockSpec(memory_space=pltpu.SMEM)
        return pl.pallas_call(
            functools.partial(kernel, (nx, ny, rows, cols)),
            out_shape=(shape, shape),
            in_specs=[hbm] * 5 + [smem] * 2,
            out_specs=(hbm, hbm),
            scratch_shapes=scratch,
            compiler_params=pltpu.CompilerParams(
                collective_id=0, has_side_effects=True, vmem_limit_bytes=48 * 1024 * 1024
            ),
        )(load_current, sink_mask, pad_mask, plane_class, via_class, plane_table, via_table)

    layers = P("gz", "gy", "gx")
    plane = P("gy", "gx")
    table = P("gz", None)
    return jax.shard_map(
        shards,
        mesh=mesh,
        in_specs=(plane, plane, plane, layers, layers, table, table),
        out_specs=(layers, layers),
        check_vma=False,
    )
```

```python
import functools

import jax
import jax.numpy as jnp
from jax import lax
from jax.experimental import pallas as pl
from jax.experimental.pallas import tpu as pltpu
from jax.sharding import PartitionSpec as P

PAD_CONDUCTANCE = 20.0
MESH = pl.DeviceIdType.MESH
HALO = 8
LANES = 128
CHUNK = 24
DEPTH = 2
AHEAD = 3
F32 = jnp.float32


def harmonic(first, second):
    return 2.0 * first * second / (first + second)


def pick(classes, table):
    low = (classes & 1) == 1
    mid = (classes & 2) == 2
    high = (classes & 4) == 4
    pairs = [jnp.where(low, table[2 * k + 1], table[2 * k]) for k in range(4)]
    return jnp.where(
        high, jnp.where(mid, pairs[3], pairs[2]), jnp.where(mid, pairs[1], pairs[0])
    )


def fold(value):
    return sum(
        value[:, k : k + LANES] for k in range(LANES, value.shape[1], LANES)
    ) + value[:, :LANES]


def kernel(
    sizes,
    load_h, sink_h, pad_h, plane_h, via_h, plane_tab_h, via_tab_h,
    volt_h, resid_h,
    load_ref, sink_ref, pad_ref, plane_ref, via_ref, plane_tab, via_tab, volt_ref, resid_ref,
    via_mine, via_far,
    g_buf, g_e, g_w,
    east, west, north, south, cross, inv0, inv1, mix, src,
    z0, z0_e, z0_w, z0_o, y1, y1_e, y1_w, y1_o, h2, h2_e, h2_w, h2_o, z2, z2_e, z2_w,
    s1, s2, s3,
    part, got_x, got_y, got_z, first_sum,
    in_sem, out_sem, far_send, far_recv, side_send, side_recv, edge_send, edge_recv,
    sum_send, sum_recv,
):
    nx, ny, rows, cols = sizes
    chunks = rows // CHUNK
    per = CHUNK // 8
    ix, iy, iz = lax.axis_index("gx"), lax.axis_index("gy"), lax.axis_index("gz")
    gx_up, gx_dn = lax.rem(ix + 1, nx), lax.rem(ix + nx - 1, nx)
    gy_up, gy_dn = lax.rem(iy + 1, ny), lax.rem(iy + ny - 1, ny)
    other = 1 - iz
    layer = (iz, other)

    fetch = [
        pltpu.make_async_copy(a, b, in_sem.at[k])
        for k, (a, b) in enumerate(
            (
                (plane_tab_h, plane_tab), (via_tab_h, via_tab), (plane_h, plane_ref),
                (via_h, via_ref), (pad_h, pad_ref), (sink_h, sink_ref), (load_h, load_ref),
            )
        )
    ]
    for c in fetch:
        c.start()

    barrier = pltpu.get_barrier_semaphore()
    peers = [{"gx": lax.rem(ix + k, nx)} for k in range(1, nx)]
    peers += [{"gy": lax.rem(iy + k, ny)} for k in range(1, ny)]
    peers += [{"gz": other}]
    for peer in peers:
        pl.semaphore_signal(barrier, inc=1, device_id=peer, device_id_type=MESH)
    pl.semaphore_wait(barrier, len(peers))

    def at(c, j=0, n=8):
        return pl.ds(pl.multiple_of(c * CHUNK + 8 * j, 8), n)

    def inner(c, j=0, n=8):
        return pl.ds(pl.multiple_of(c * CHUNK + (8 * j + HALO), 8), n)

    def remote(source, target, send, recv, where_to):
        return pltpu.make_async_remote_copy(
            src_ref=source, dst_ref=target, send_sem=send, recv_sem=recv,
            device_id=where_to, device_id_type=MESH,
        )

    def far_copy(stage, c):
        buf, out = ((via_mine, via_far), (z0, z0_o), (y1, y1_o), (h2, h2_o))[stage]
        source = buf.at[at(c, 0, CHUNK), :] if stage == 0 else buf.at[1, inner(c, 0, CHUNK), :]
        return remote(
            source, out.at[at(c, 0, CHUNK), :],
            far_send.at[stage, c], far_recv.at[stage, c], {"gz": other},
        )

    fields = ((z0, z0_e, z0_w), (y1, y1_e, y1_w), (h2, h2_e, h2_w), (g_buf, g_e, g_w))

    def side_copies(stage, c):
        buf, buf_e, buf_w = fields[stage]
        span = inner(c, 0, CHUNK)
        return [
            remote(
                buf.at[:, span, pl.ds(cols - LANES, LANES)], buf_w.at[:, at(c, 0, CHUNK), :],
                side_send.at[stage, 0, c], side_recv.at[stage, 0, c], {"gx": gx_up},
            ),
            remote(
                buf.at[:, span, pl.ds(0, LANES)], buf_e.at[:, at(c, 0, CHUNK), :],
                side_send.at[stage, 1, c], side_recv.at[stage, 1, c], {"gx": gx_dn},
            ),
        ]

    def edge_copy(stage, way):
        buf = fields[stage][0]
        if way == 0:
            span, out, where_to = pl.ds(rows, 8), pl.ds(0, 8), gy_up
        else:
            span, out, where_to = pl.ds(HALO, 8), pl.ds(HALO + rows, 8), gy_dn
        return remote(
            buf.at[:, span, :], buf.at[:, out, :],
            edge_send.at[stage, way], edge_recv.at[stage, way], {"gy": where_to},
        )

    def send_chunk(stage, c):
        for move in side_copies(stage, c):
            move.start()

        @pl.when(c == chunks - 1)
        def _():
            edge_copy(stage, 0).start()

        @pl.when(c == 0)
        def _():
            edge_copy(stage, 1).start()

    def await_chunk(stage, c):
        for move in side_copies(stage, c):
            move.wait_recv()

        @pl.when(c == 0)
        def _():
            edge_copy(stage, 0).wait_recv()

        @pl.when(c == chunks - 1)
        def _():
            edge_copy(stage, 1).wait_recv()

    def place(k):
        late = jnp.where(k == 3, chunks - 1, jnp.where(k == 4, 0, k - 1))
        return jnp.where(k < 3, k + 1, late)

    for c in fetch[:3]:
        c.wait()
    plane_of = [[plane_tab[layer[slot], k] for k in range(8)] for slot in (0, 1)]
    via_of = [[via_tab[layer[slot], k] for k in range(8)] for slot in (0, 1)]

    def lookup_own(k, _):
        c = place(k)
        for slot in (0, 1):
            for j in range(per):
                g_buf[slot, inner(c, j), :] = pick(
                    plane_ref[layer[slot], at(c, j), :], plane_of[slot]
                )
        send_chunk(3, c)
        return 0

    lax.fori_loop(0, chunks, lookup_own, 0)
    fetch[3].wait()

    def lookup_far(k, _):
        c = place(k)
        for j in range(per):
            via_mine[at(c, j), :] = pick(via_ref[other, at(c, j), :], via_of[1])
        far_copy(0, c).start()
        return 0

    lax.fori_loop(0, chunks, lookup_far, 0)

    def far_step(stage, k):
        return far_copy(stage, place(k))

    def far_send_next(stage, k):
        @pl.when(k >= DEPTH)
        def _():
            far_step(stage, k - DEPTH).wait_send()

        if stage > 1:

            @pl.when(k < DEPTH)
            def _():
                far_step(stage - 1, k + chunks - DEPTH).wait_send()

        far_step(stage, k).start()

    @pl.when(iz == 0)
    def _():
        def clear(c, _):
            z0_o[at(c, 0, CHUNK), :] = jnp.zeros((CHUNK, cols), F32)
            return 0

        lax.fori_loop(0, chunks, clear, 0)

    for c in fetch[4:]:
        c.wait()

    def around(field, slot, c, j):
        buf, buf_e, buf_w = field
        here = buf[slot, inner(c, j), :]
        below = buf[slot, at(c, j), :]
        above = buf[slot, at(c, j + 2), :]
        up = jnp.concatenate([here[1:], above[:1]], 0)
        down = jnp.concatenate([below[7:], here[:7]], 0)
        right = pltpu.roll(
            jnp.concatenate([here, buf_e[slot, at(c, j), :]], 1), cols + LANES - 1, 1
        )[:, :cols]
        left = pltpu.roll(
            jnp.concatenate([buf_w[slot, at(c, j), :], here], 1), 1, 1
        )[:, LANES:]
        return here, right, left, up, down

    is_source = jnp.where(iz == 0, F32(1.0), F32(0.0))
    pad_scale = jnp.where(iz == 0, F32(0.0), F32(PAD_CONDUCTANCE))

    def solve(span, b0, b1):
        m = mix[span, :]
        x1 = (b1 + m * b0) * inv1[span, :]
        return b0 * inv0[span, :] + m * x1, x1

    def plane_edges(slot, c):
        sums = []
        below = g_buf[slot, at(c), :]
        here = g_buf[slot, inner(c), :]
        last = harmonic(below, jnp.concatenate([below[1:], here[:1]], 0))
        for j in range(per):
            span = at(c, j)
            here = g_buf[slot, inner(c, j), :]
            above = g_buf[slot, at(c, j + 2), :]
            wide = jnp.concatenate([g_w[slot, span, :], here, g_e[slot, span, :]], 1)
            edge = harmonic(wide, pltpu.roll(wide, cols + 2 * LANES - 1, 1))[:, : cols + LANES]
            e = edge[:, LANES:]
            w = pltpu.roll(edge, 1, 1)[:, LANES:]
            n = harmonic(here, jnp.concatenate([here[1:], above[:1]], 0))
            s = jnp.concatenate([last[7:], n[:7]], 0)
            last = n
            east[slot, span, :] = e
            west[slot, span, :] = w
            north[slot, span, :] = n
            south[slot, span, :] = s
            sums.append(e + w + n + s)
        return sums

    def build(k, _):
        c = place(k)
        await_chunk(3, c)
        sums = [plane_edges(slot, c) for slot in (0, 1)]
        far_copy(0, c).wait_recv()
        for j in range(per):
            span = at(c, j)
            via0 = pick(via_ref[iz, span, :], via_of[0])
            via1 = via_mine[span, :]
            link = harmonic(via0, via1)
            far = harmonic(via1, via_far[span, :])
            cross[span, :] = far
            d0 = sums[0][j] + link + pad_scale * pad_ref[span, :].astype(F32)
            d1 = sums[1][j] + link + far
            i0 = 1.0 / d0
            m = link * i0
            i1 = 1.0 / (d1 - link * m)
            inv0[span, :] = i0
            inv1[span, :] = i1
            mix[span, :] = m
            b0 = is_source * (sink_ref[span, :].astype(F32) * load_ref[span, :])
            src[span, :] = b0
            x1 = m * b0 * i1
            z0[0, inner(c, j), :] = b0 * i0 + m * x1
            z0[1, inner(c, j), :] = x1

        send_chunk(0, c)

        @pl.when(jnp.logical_and(iz == 0, k + AHEAD >= chunks))
        def _():
            far_send_next(1, k + AHEAD - chunks)

        return 0

    lax.fori_loop(0, chunks, build, 0)

    def couple(field, slot, c, j):
        here, right, left, up, down = around(field, slot, c, j)
        span = at(c, j)
        u = (
            east[slot, span, :] * right + west[slot, span, :] * left
            + north[slot, span, :] * up + south[slot, span, :] * down
        )
        return here, u

    zero = jnp.zeros((8, LANES), F32)

    def pass1(k, carry):
        c = place(k)
        mu, t00 = carry
        await_chunk(0, c)

        @pl.when(iz == 1)
        def _():
            far_copy(1, c).wait_recv()

        for j in range(per):
            span = at(c, j)
            h0, u0 = couple(fields[0], 0, c, j)
            h1, u1 = couple(fields[0], 1, c, j)
            b0 = src[span, :]
            a0, a1 = b0 - u0, -(u1 + cross[span, :] * z0_o[span, :])
            s1[0, span, :] = a0
            s1[1, span, :] = a1
            x0, x1 = solve(span, a0, a1)
            y1[0, inner(c, j), :] = x0
            y1[1, inner(c, j), :] = x1
            mu = mu + fold(h0 * b0)
            t00 = t00 + fold(h0 * a0 + h1 * a1)
        send_chunk(1, c)

        @pl.when(iz == 1)
        def _():
            far_copy(2, c).start()

        return mu, t00

    sums = lax.fori_loop(0, chunks, pass1, (zero, zero))

    lane = lax.broadcasted_iota(jnp.int32, (1, LANES), 1)
    axes = (("gx", nx, ix, got_x), ("gy", ny, iy, got_y), ("gz", 2, iz, got_z))
    offset = (0, nx, nx + ny)

    def line_of(values):
        line = jnp.zeros((1, LANES), F32)
        for k, value in enumerate(values):
            line = jnp.where(lane == k, jnp.sum(value), line)
        return line

    def sum_moves(which, stage):
        axis, size, me, got = axes[stage]
        return [
            remote(
                part.at[which, stage], got.at[which, me],
                sum_send.at[which, offset[stage] + k], sum_recv.at[which, offset[stage] + k],
                {axis: lax.rem(me + k, size)},
            )
            for k in range(1, size)
        ]

    def sum_start(which, stage, line):
        part[which, stage] = line
        axes[stage][3][which, axes[stage][2]] = line
        for c in sum_moves(which, stage):
            c.start()

    def sum_finish(which, stage):
        _, size, _, got = axes[stage]
        for c in sum_moves(which, stage):
            c.wait()
        line = got[which, 0]
        for k in range(1, size):
            line = line + got[which, k]
        return line

    def hand_over():
        return remote(
            part.at[0, 2], first_sum, sum_send.at[0, nx + ny], sum_recv.at[0, nx + ny], {"gz": other}
        )

    first_line = line_of(sums)

    @pl.when(iz == 0)
    def _():
        sum_start(0, 0, first_line)

        def send_rest(k, _):
            far_send_next(1, k)
            return 0

        lax.fori_loop(AHEAD, chunks, send_rest, 0)
        sum_start(0, 1, sum_finish(0, 0))

    def pass2(k, _):
        c = place(k)
        await_chunk(1, c)
        far_copy(2, c).wait_recv()
        for j in range(per):
            span = at(c, j)
            _, u0 = couple(fields[1], 0, c, j)
            _, u1 = couple(fields[1], 1, c, j)
            a0 = s1[0, span, :] - u0
            a1 = s1[1, span, :] - (u1 + cross[span, :] * y1_o[span, :])
            s2[0, span, :] = a0
            s2[1, span, :] = a1
            x0, x1 = solve(span, a0, a1)
            h2[0, inner(c, j), :] = x0
            h2[1, inner(c, j), :] = x1
        send_chunk(2, c)

        @pl.when(iz == 1)
        def _():
            far_copy(3, c).start()

        @pl.when(iz == 0)
        def _():
            far_send_next(2, k)

        @pl.when(jnp.logical_and(iz == 0, k == chunks // 2))
        def _():
            line = sum_finish(0, 1)
            part[0, 2] = line
            first_sum[...] = line
            hand_over().start()

        return 0

    lax.fori_loop(0, chunks, pass2, 0)

    @pl.when(iz == 0)
    def _():
        hand_over().wait_send()

    @pl.when(iz == 1)
    def _():
        hand_over().wait_recv()

    def take(line, k):
        return jnp.sum(jnp.where(lane == k, line, 0.0), axis=1, keepdims=True)

    line = first_sum[...]
    mu, t00 = take(line, 0), take(line, 1)
    step, shift = mu / t00, t00 / mu

    def third(a, b, c):
        return (b - step * c) - shift * (a - step * b)

    def blend(c, _):
        for slot in (0, 1):
            for j in range(per):
                span = inner(c, j)
                z2[slot, span, :] = third(z0[slot, span, :], y1[slot, span, :], h2[slot, span, :])
        return 0

    lax.fori_loop(0, chunks, blend, 0)

    def pass3(k, carry):
        c = place(k)
        await_chunk(2, c)

        @pl.when(c == 0)
        def _():
            for slot in (0, 1):
                z2[slot, 0:8, :] = third(z0[slot, 0:8, :], y1[slot, 0:8, :], h2[slot, 0:8, :])

        @pl.when(c == chunks - 1)
        def _():
            top = pl.ds(HALO + rows, 8)
            for slot in (0, 1):
                z2[slot, top, :] = third(z0[slot, top, :], y1[slot, top, :], h2[slot, top, :])

        t01, t11, g1, t02, t12, t22, g2 = carry
        for j in range(per):
            span = at(c, j)
            b0 = src[span, :]
            for slot in (0, 1):
                z2_e[slot, span, :] = third(z0_e[slot, span, :], y1_e[slot, span, :], h2_e[slot, span, :])
                z2_w[slot, span, :] = third(z0_w[slot, span, :], y1_w[slot, span, :], h2_w[slot, span, :])
                h, u = couple((z2, z2_e, z2_w), slot, c, j)
                first = s1[slot, span, :]
                second = first - step * s2[slot, span, :]
                r1 = (b0 - step * first) if slot == 0 else -step * first
                a = (second - shift * r1) - u
                s2[slot, span, :] = second
                s3[slot, span, :] = a
                p = z0[slot, inner(c, j), :]
                q = p - step * y1[slot, inner(c, j), :]
                t01 = t01 + fold(p * second)
                t11 = t11 + fold(q * second)
                t02 = t02 + fold(h * first)
                t12 = t12 + fold(h * second)
                t22 = t22 + fold(h * a)
                if slot == 0:
                    g1 = g1 + fold(q * b0)
                    g2 = g2 + fold(h * b0)
        return t01, t11, g1, t02, t12, t22, g2

    sums = list(lax.fori_loop(0, chunks, pass3, (zero,) * 7))

    def cross_term(k, carry):
        c = place(k)
        far_copy(3, c).wait_recv()
        for j in range(per):
            span = at(c, j)
            far = cross[span, :] * third(z0_o[span, :], y1_o[span, :], h2_o[span, :])
            s3[1, span, :] = s3[1, span, :] - far
            carry = carry + fold(z2[1, inner(c, j), :] * far)

        @pl.when(iz == 0)
        def _():
            far_send_next(3, k)

        return carry

    def far_part():
        return lax.fori_loop(0, chunks, cross_term, zero)

    sums[5] = sums[5] - 2.0 * lax.cond(iz == 0, far_part, lambda: zero)
    line = line_of(sums)
    for stage in range(3):
        sum_start(1, stage, line)
        line = sum_finish(1, stage)

    @pl.when(iz == 1)
    def _():
        far_part()

    t01, t11, g1, t02, t12, t22, g2 = [take(line, k) / mu for k in range(7)]
    l1, l2 = t01 / shift, t02 / shift
    d1, e1 = t11 - l1 * t01, t12 - l1 * t02
    l3 = e1 / d1
    d2 = t22 - l2 * t02 - l3 * e1
    b1 = g1 - l1
    b2 = g2 - l2 - l3 * b1
    c2 = b2 / d2
    c1 = b1 / d1 - l3 * c2
    c0 = step - l1 * c1 - l2 * c2

    def result_copies(c):
        span = at(c, 0, CHUNK)
        return [
            pltpu.make_async_copy(a.at[:, span, :], b.at[:, span, :], out_sem.at[k, c])
            for k, (a, b) in enumerate(((volt_ref, volt_h), (resid_ref, resid_h)))
        ]

    def finish(c, _):
        for slot in (0, 1):
            for j in range(per):
                span, wide = at(c, j), inner(c, j)
                p = z0[slot, wide, :]
                volt_ref[layer[slot], span, :] = (
                    c0 * p + c1 * (p - step * y1[slot, wide, :]) + c2 * z2[slot, wide, :]
                )
                tail = c0 * s1[slot, span, :] + c1 * s2[slot, span, :] + c2 * s3[slot, span, :]
                resid_ref[layer[slot], span, :] = (src[span, :] - tail) if slot == 0 else -tail
        for move in result_copies(c):
            move.start()
        return 0

    lax.fori_loop(0, chunks, finish, 0)

    def drain(c, _):
        for move in result_copies(c):
            move.wait()
        far_copy(0, c).wait_send()

        @pl.when(iz == 1)
        def _():
            far_copy(2, c).wait_send()
            far_copy(3, c).wait_send()

        for stage in range(4):
            for move in side_copies(stage, c):
                move.wait_send()
        return 0

    lax.fori_loop(0, chunks, drain, 0)

    @pl.when(iz == 0)
    def _():
        for k in range(chunks - DEPTH, chunks):
            far_step(3, jnp.int32(k)).wait_send()

    for stage in range(4):
        for way in (0, 1):
            edge_copy(stage, way).wait_send()


def solution(mesh):
    nx, ny = mesh.shape["gx"], mesh.shape["gy"]

    def shards(load_current, sink_mask, pad_mask, plane_class, via_class, plane_table, via_table):
        _, rows, cols = plane_class.shape
        chunks = rows // CHUNK
        flat = pltpu.VMEM((rows, cols), F32)
        flat_i = pltpu.VMEM((rows, cols), jnp.int32)
        both = pltpu.VMEM((2, rows, cols), F32)
        both_i = pltpu.VMEM((2, rows, cols), jnp.int32)
        tall = pltpu.VMEM((2, rows + 2 * HALO, cols), F32)
        side = pltpu.VMEM((2, rows, LANES), F32)
        field = [tall, side, side, flat]
        dma = pltpu.SemaphoreType.DMA
        scratch = [
            flat, flat_i, flat_i, both_i, both_i,
            pltpu.SMEM(plane_table.shape, F32), pltpu.SMEM(via_table.shape, F32), both, both,
            flat, flat,
            tall, side, side,
            both, both, both, both, flat, flat, flat, flat, flat,
            *field, *field, *field, tall, side, side,
            both, both, both,
            pltpu.VMEM((2, 3, 1, LANES), F32),
            pltpu.VMEM((2, nx, 1, LANES), F32),
            pltpu.VMEM((2, ny, 1, LANES), F32),
            pltpu.VMEM((2, 2, 1, LANES), F32),
            pltpu.VMEM((1, LANES), F32),
            dma((7,)), dma((2, chunks)),
            dma((4, chunks)), dma((4, chunks)),
            dma((4, 2, chunks)), dma((4, 2, chunks)),
            dma((4, 2)), dma((4, 2)),
            dma((2, nx + ny + 2)), dma((2, nx + ny + 2)),
        ]
        shape = jax.ShapeDtypeStruct(plane_class.shape, F32)
        hbm = pl.BlockSpec(memory_space=pltpu.HBM)
        free = pl.BlockSpec(memory_space=pl.ANY)
        return pl.pallas_call(
            functools.partial(kernel, (nx, ny, rows, cols)),
            out_shape=(shape, shape),
            in_specs=[hbm] * 7,
            out_specs=(free, free),
            scratch_shapes=scratch,
            compiler_params=pltpu.CompilerParams(
                collective_id=0, has_side_effects=True, vmem_limit_bytes=58 * 1024 * 1024
            ),
        )(load_current, sink_mask, pad_mask, plane_class, via_class, plane_table, via_table)

    layers = P("gz", "gy", "gx")
    plane = P("gy", "gx")
    table = P("gz", None)
    return jax.shard_map(
        shards,
        mesh=mesh,
        in_specs=(plane, plane, plane, layers, layers, table, table),
        out_specs=(layers, layers),
        check_vma=False,
    )
```

```python
import functools

import jax
import jax.numpy as jnp
from jax import lax
from jax.experimental import pallas as pl
from jax.experimental.pallas import tpu as pltpu
from jax.sharding import PartitionSpec as P

PAD_CONDUCTANCE = 20.0
MESH = pl.DeviceIdType.MESH
HALO = 8
LANES = 128
CHUNK = 24
F32 = jnp.float32


def harmonic(first, second):
    return 2.0 * first * second / (first + second)


def pick(classes, table):
    low = (classes & 1) == 1
    mid = (classes & 2) == 2
    high = (classes & 4) == 4
    pairs = [jnp.where(low, table[2 * k + 1], table[2 * k]) for k in range(4)]
    return jnp.where(
        high, jnp.where(mid, pairs[3], pairs[2]), jnp.where(mid, pairs[1], pairs[0])
    )


def fold(value):
    return sum(
        value[:, k : k + LANES] for k in range(LANES, value.shape[1], LANES)
    ) + value[:, :LANES]


def kernel(
    sizes,
    load_h, sink_h, pad_h, plane_h, via_h, plane_tab_h, via_tab_h,
    volt_h, resid_h,
    load_ref, sink_ref, pad_ref, plane_ref, via_ref, plane_tab, via_tab, volt_ref, resid_ref,
    via_mine, via_far,
    g_buf, g_e, g_w,
    east, west, north, south, cross, inv0, inv1, mix, src,
    z0, z0_e, z0_w, z0_o, y1, y1_e, y1_w, y1_o, h2, h2_e, h2_w, h2_o, z2, z2_e, z2_w,
    s1, s2, s3,
    part, got_x, got_y, got_p, first_sum,
    in_sem, out_sem, far_send, far_recv, side_send, side_recv, edge_send, edge_recv,
    sum_send, sum_recv,
):
    nx, ny, rows, cols = sizes
    chunks = rows // CHUNK
    per = CHUNK // 8
    ix, iy, iz = lax.axis_index("gx"), lax.axis_index("gy"), lax.axis_index("gz")
    gx_up, gx_dn = lax.rem(ix + 1, nx), lax.rem(ix + nx - 1, nx)
    gy_up, gy_dn = lax.rem(iy + 1, ny), lax.rem(iy + ny - 1, ny)
    other = 1 - iz
    layer = (iz, other)

    fetch = [
        pltpu.make_async_copy(a, b, in_sem.at[k])
        for k, (a, b) in enumerate(
            (
                (plane_tab_h, plane_tab), (via_tab_h, via_tab), (plane_h, plane_ref),
                (via_h, via_ref), (pad_h, pad_ref), (sink_h, sink_ref), (load_h, load_ref),
            )
        )
    ]
    for c in fetch:
        c.start()

    def plane_peer(k):
        there = lax.rem(iy * 2 + iz + k, 2 * ny)
        return {"gy": there // 2, "gz": lax.rem(there, 2)}

    barrier = pltpu.get_barrier_semaphore()
    peers = [{"gx": lax.rem(ix + k, nx)} for k in range(1, nx)]
    peers += [plane_peer(k) for k in range(1, 2 * ny)]
    for peer in peers:
        pl.semaphore_signal(barrier, inc=1, device_id=peer, device_id_type=MESH)
    def at(c, j=0, n=8):
        return pl.ds(pl.multiple_of(c * CHUNK + 8 * j, 8), n)

    def inner(c, j=0, n=8):
        return pl.ds(pl.multiple_of(c * CHUNK + (8 * j + HALO), 8), n)

    def remote(source, target, send, recv, where_to):
        return pltpu.make_async_remote_copy(
            src_ref=source, dst_ref=target, send_sem=send, recv_sem=recv,
            device_id=where_to, device_id_type=MESH,
        )

    def far_copy(stage, c):
        buf, out = ((via_mine, via_far), (z0, z0_o), (y1, y1_o), (h2, h2_o))[stage]
        source = buf.at[at(c, 0, CHUNK), :] if stage == 0 else buf.at[1, inner(c, 0, CHUNK), :]
        return remote(
            source, out.at[at(c, 0, CHUNK), :],
            far_send.at[stage, c], far_recv.at[stage, c], {"gz": other},
        )

    fields = ((z0, z0_e, z0_w), (y1, y1_e, y1_w), (h2, h2_e, h2_w), (g_buf, g_e, g_w))

    def side_copies(stage, c):
        buf, buf_e, buf_w = fields[stage]
        span = inner(c, 0, CHUNK)
        return [
            remote(
                buf.at[:, span, pl.ds(cols - LANES, LANES)], buf_w.at[:, at(c, 0, CHUNK), :],
                side_send.at[stage, 0, c], side_recv.at[stage, 0, c], {"gx": gx_up},
            ),
            remote(
                buf.at[:, span, pl.ds(0, LANES)], buf_e.at[:, at(c, 0, CHUNK), :],
                side_send.at[stage, 1, c], side_recv.at[stage, 1, c], {"gx": gx_dn},
            ),
        ]

    def edge_copy(stage, way):
        buf = fields[stage][0]
        if way == 0:
            span, out, where_to = pl.ds(rows, 8), pl.ds(0, 8), gy_up
        else:
            span, out, where_to = pl.ds(HALO, 8), pl.ds(HALO + rows, 8), gy_dn
        return remote(
            buf.at[:, span, :], buf.at[:, out, :],
            edge_send.at[stage, way], edge_recv.at[stage, way], {"gy": where_to},
        )

    def send_chunk(stage, c):
        for move in side_copies(stage, c):
            move.start()

        @pl.when(c == chunks - 1)
        def _():
            edge_copy(stage, 0).start()

        @pl.when(c == 0)
        def _():
            edge_copy(stage, 1).start()

    def await_chunk(stage, c):
        for move in side_copies(stage, c):
            move.wait_recv()

        @pl.when(c == 0)
        def _():
            edge_copy(stage, 0).wait_recv()

        @pl.when(c == chunks - 1)
        def _():
            edge_copy(stage, 1).wait_recv()

    def turn(k):
        return lax.rem(k + chunks - 1, chunks)

    def place(k):
        late = jnp.where(k == 3, chunks - 1, jnp.where(k == 4, 0, k - 1))
        return jnp.where(k < 3, k + 1, late)

    for c in fetch[:3]:
        c.wait()
    plane_of = [[plane_tab[layer[slot], k] for k in range(8)] for slot in (0, 1)]
    via_of = [[via_tab[layer[slot], k] for k in range(8)] for slot in (0, 1)]

    def lookup_own(k, _):
        c = place(k)
        for slot in (0, 1):
            for j in range(per):
                g_buf[slot, inner(c, j), :] = pick(
                    plane_ref[layer[slot], at(c, j), :], plane_of[slot]
                )
        return 0

    lax.fori_loop(0, chunks, lookup_own, 0)
    fetch[3].wait()

    def lookup_far(k, _):
        c = turn(k)
        for j in range(per):
            via_mine[at(c, j), :] = pick(via_ref[other, at(c, j), :], via_of[1])
        return 0

    lax.fori_loop(0, chunks, lookup_far, 0)

    pl.semaphore_wait(barrier, len(peers))

    def send_edges(k, _):
        send_chunk(3, turn(k))
        return 0

    lax.fori_loop(0, chunks, send_edges, 0)

    def far_each(n, stages, act):
        for stage in stages:

            @pl.when(n // chunks == stage)
            def _(stage=stage):
                k = n - stage * chunks
                act(far_copy(stage, place(k) if stage else turn(k)))

    def far_left(n, stages):
        far_each(n, stages, lambda move: move.wait_send())

    def far_start(n, stages):
        far_each(n, stages, lambda move: move.start())

    for n in (0, 1):
        far_copy(0, turn(jnp.int32(n))).start()

    def lead(n, _):
        far_left(n - 2, (0,))
        far_start(n, (0,))
        return 0

    lax.fori_loop(2, chunks - 2, lead, 0)
    for n in (chunks - 2, chunks - 1):
        far_copy(0, turn(jnp.int32(n))).start()

    @pl.when(iz == 0)
    def _():
        def clear(c, _):
            z0_o[at(c, 0, CHUNK), :] = jnp.zeros((CHUNK, cols), F32)
            return 0

        lax.fori_loop(0, chunks, clear, 0)

    for c in fetch[4:]:
        c.wait()

    def around(field, slot, c, j):
        buf, buf_e, buf_w = field
        here = buf[slot, inner(c, j), :]
        below = buf[slot, at(c, j), :]
        above = buf[slot, at(c, j + 2), :]
        up = jnp.concatenate([here[1:], above[:1]], 0)
        down = jnp.concatenate([below[7:], here[:7]], 0)
        right = pltpu.roll(
            jnp.concatenate([here, buf_e[slot, at(c, j), :]], 1), cols + LANES - 1, 1
        )[:, :cols]
        left = pltpu.roll(
            jnp.concatenate([buf_w[slot, at(c, j), :], here], 1), 1, 1
        )[:, LANES:]
        return here, right, left, up, down

    is_source = jnp.where(iz == 0, F32(1.0), F32(0.0))
    pad_scale = jnp.where(iz == 0, F32(0.0), F32(PAD_CONDUCTANCE))

    def solve(span, b0, b1):
        m = mix[span, :]
        x1 = (b1 + m * b0) * inv1[span, :]
        return b0 * inv0[span, :] + m * x1, x1

    def plane_edges(slot, c):
        sums = []
        below = g_buf[slot, at(c), :]
        here = g_buf[slot, inner(c), :]
        last = harmonic(below, jnp.concatenate([below[1:], here[:1]], 0))
        for j in range(per):
            span = at(c, j)
            here = g_buf[slot, inner(c, j), :]
            above = g_buf[slot, at(c, j + 2), :]
            wide = jnp.concatenate([g_w[slot, span, :], here, g_e[slot, span, :]], 1)
            edge = harmonic(wide, pltpu.roll(wide, cols + 2 * LANES - 1, 1))[:, : cols + LANES]
            e = edge[:, LANES:]
            w = pltpu.roll(edge, 1, 1)[:, LANES:]
            n = harmonic(here, jnp.concatenate([here[1:], above[:1]], 0))
            s = jnp.concatenate([last[7:], n[:7]], 0)
            last = n
            east[slot, span, :] = e
            west[slot, span, :] = w
            north[slot, span, :] = n
            south[slot, span, :] = s
            sums.append(e + w + n + s)
        return sums

    def build(k, _):
        c = turn(k)
        await_chunk(3, c)
        sums = [plane_edges(slot, c) for slot in (0, 1)]
        far_copy(0, c).wait_recv()
        for j in range(per):
            span = at(c, j)
            via0 = pick(via_ref[iz, span, :], via_of[0])
            via1 = via_mine[span, :]
            link = harmonic(via0, via1)
            far = harmonic(via1, via_far[span, :])
            cross[span, :] = far
            d0 = sums[0][j] + link + pad_scale * pad_ref[span, :].astype(F32)
            d1 = sums[1][j] + link + far
            i0 = 1.0 / d0
            m = link * i0
            i1 = 1.0 / (d1 - link * m)
            inv0[span, :] = i0
            inv1[span, :] = i1
            mix[span, :] = m
            b0 = is_source * (sink_ref[span, :].astype(F32) * load_ref[span, :])
            src[span, :] = b0
            x1 = m * b0 * i1
            z0[0, inner(c, j), :] = b0 * i0 + m * x1
            z0[1, inner(c, j), :] = x1

        send_chunk(0, c)

        @pl.when(jnp.logical_and(iz == 0, k >= 4))
        def _():
            far_left(k, (0,))
            far_start(k + 4, (1,))

        return 0

    lax.fori_loop(0, chunks, build, 0)

    def couple(field, slot, c, j):
        here, right, left, up, down = around(field, slot, c, j)
        span = at(c, j)
        u = (
            east[slot, span, :] * right + west[slot, span, :] * left
            + north[slot, span, :] * up + south[slot, span, :] * down
        )
        return here, u

    zero = jnp.zeros((8, LANES), F32)

    def pass1(k, carry):
        c = place(k)
        mu, t00 = carry

        @pl.when(jnp.logical_and(iz == 0, jnp.logical_or(k == 3, k == 4)))
        def _():
            far_left(chunks - 3 + k, (1,))
            far_start(chunks + 1 + k, (1,))

        await_chunk(0, c)

        @pl.when(iz == 1)
        def _():
            far_copy(1, c).wait_recv()

        for j in range(per):
            span = at(c, j)
            h0, u0 = couple(fields[0], 0, c, j)
            h1, u1 = couple(fields[0], 1, c, j)
            b0 = src[span, :]
            a0, a1 = b0 - u0, -(u1 + cross[span, :] * z0_o[span, :])
            s1[0, span, :] = a0
            s1[1, span, :] = a1
            x0, x1 = solve(span, a0, a1)
            y1[0, inner(c, j), :] = x0
            y1[1, inner(c, j), :] = x1
            mu = mu + fold(h0 * b0)
            t00 = t00 + fold(h0 * a0 + h1 * a1)
        send_chunk(1, c)

        @pl.when(iz == 1)
        def _():
            far_copy(2, c).start()

        return mu, t00

    sums = lax.fori_loop(0, chunks, pass1, (zero, zero))

    lane = lax.broadcasted_iota(jnp.int32, (1, LANES), 1)
    rings = (
        (nx, ix, got_x, lambda k: {"gx": lax.rem(ix + k, nx)}),
        (ny, iy, got_y, lambda k: {"gy": lax.rem(iy + k, ny)}),
        (2 * ny, iy * 2 + iz, got_p, plane_peer),
    )
    offset = (0, nx, nx + ny)

    def line_of(values):
        line = jnp.zeros((1, LANES), F32)
        for k, value in enumerate(values):
            line = jnp.where(lane == k, jnp.sum(value), line)
        return line

    def sum_moves(which, stage):
        size, me, got, peer = rings[stage]
        return [
            remote(
                part.at[which, stage], got.at[which, me],
                sum_send.at[which, offset[stage] + k], sum_recv.at[which, offset[stage] + k],
                peer(k),
            )
            for k in range(1, size)
        ]

    def sum_start(which, stage, line):
        part[which, stage] = line
        rings[stage][2][which, rings[stage][1]] = line
        for c in sum_moves(which, stage):
            c.start()

    def sum_finish(which, stage):
        size, _, got, _ = rings[stage]
        for c in sum_moves(which, stage):
            c.wait()
        line = got[which, 0]
        for k in range(1, size):
            line = line + got[which, k]
        return line

    def hand_over():
        return remote(
            part.at[0, 2], first_sum, sum_send.at[0, nx + ny], sum_recv.at[0, nx + ny], {"gz": other}
        )

    first_line = line_of(sums)

    @pl.when(iz == 0)
    def _():
        sum_start(0, 0, first_line)

        for n in (14, 15, 16):
            far_left(jnp.int32(n - 4), (1,))
            far_start(jnp.int32(n), (1, 2))

    def pass2(k, _):
        c = place(k)
        await_chunk(1, c)
        far_copy(2, c).wait_recv()
        for j in range(per):
            span = at(c, j)
            _, u0 = couple(fields[1], 0, c, j)
            _, u1 = couple(fields[1], 1, c, j)
            a0 = s1[0, span, :] - u0
            a1 = s1[1, span, :] - (u1 + cross[span, :] * y1_o[span, :])
            s2[0, span, :] = a0
            s2[1, span, :] = a1
            x0, x1 = solve(span, a0, a1)
            h2[0, inner(c, j), :] = x0
            h2[1, inner(c, j), :] = x1
        send_chunk(2, c)

        @pl.when(iz == 1)
        def _():
            far_copy(3, c).start()

        @pl.when(iz == 0)
        def _():
            @pl.when(k == 0)
            def _():
                far_left(jnp.int32(13), (1,))

            far_left(14 + k, (1, 2))
            far_start(17 + k, (2, 3))

        @pl.when(jnp.logical_and(iz == 0, k == 3))
        def _():
            sum_start(0, 1, sum_finish(0, 0))

        @pl.when(jnp.logical_and(iz == 0, k == chunks - 1))
        def _():
            line = sum_finish(0, 1)
            part[0, 2] = line
            first_sum[...] = line
            hand_over().start()

        return 0

    lax.fori_loop(0, chunks, pass2, 0)

    @pl.when(iz == 0)
    def _():
        def rest(n, _):
            far_start(n, (3,))
            return 0

        lax.fori_loop(25, 4 * chunks, rest, 0)
        hand_over().wait_send()

    @pl.when(iz == 1)
    def _():
        hand_over().wait_recv()

    def take(line, k):
        return jnp.sum(jnp.where(lane == k, line, 0.0), axis=1, keepdims=True)

    line = first_sum[...]
    mu, t00 = take(line, 0), take(line, 1)
    step, shift = mu / t00, t00 / mu

    def third(a, b, c):
        return (b - step * c) - shift * (a - step * b)

    def blend(c, _):
        for slot in (0, 1):
            for j in range(per):
                span = inner(c, j)
                z2[slot, span, :] = third(z0[slot, span, :], y1[slot, span, :], h2[slot, span, :])
        return 0

    lax.fori_loop(0, chunks, blend, 0)

    def pass3(k, carry):
        c = place(k)
        await_chunk(2, c)

        @pl.when(c == 0)
        def _():
            for slot in (0, 1):
                z2[slot, 0:8, :] = third(z0[slot, 0:8, :], y1[slot, 0:8, :], h2[slot, 0:8, :])

        @pl.when(c == chunks - 1)
        def _():
            top = pl.ds(HALO + rows, 8)
            for slot in (0, 1):
                z2[slot, top, :] = third(z0[slot, top, :], y1[slot, top, :], h2[slot, top, :])

        t01, t11, g1, t02, t12, t22, g2 = carry
        for j in range(per):
            span = at(c, j)
            b0 = src[span, :]
            for slot in (0, 1):
                z2_e[slot, span, :] = third(z0_e[slot, span, :], y1_e[slot, span, :], h2_e[slot, span, :])
                z2_w[slot, span, :] = third(z0_w[slot, span, :], y1_w[slot, span, :], h2_w[slot, span, :])
                h, u = couple((z2, z2_e, z2_w), slot, c, j)
                first = s1[slot, span, :]
                second = first - step * s2[slot, span, :]
                r1 = (b0 - step * first) if slot == 0 else -step * first
                a = (second - shift * r1) - u
                s2[slot, span, :] = second
                s3[slot, span, :] = a
                p = z0[slot, inner(c, j), :]
                q = p - step * y1[slot, inner(c, j), :]
                t01 = t01 + fold(p * second)
                t11 = t11 + fold(q * second)
                t02 = t02 + fold(h * first)
                t12 = t12 + fold(h * second)
                t22 = t22 + fold(h * a)
                if slot == 0:
                    g1 = g1 + fold(q * b0)
                    g2 = g2 + fold(h * b0)
        return t01, t11, g1, t02, t12, t22, g2

    sums = list(lax.fori_loop(0, chunks, pass3, (zero,) * 7))

    def cross_term(k, carry):
        c = place(k)
        far_copy(3, c).wait_recv()
        for j in range(per):
            span = at(c, j)
            far = cross[span, :] * third(z0_o[span, :], y1_o[span, :], h2_o[span, :])
            s3[1, span, :] = s3[1, span, :] - far
            carry = carry + fold(z2[1, inner(c, j), :] * far)

        return carry

    def far_part():
        return lax.fori_loop(0, chunks, cross_term, zero)

    sums[5] = sums[5] - 2.0 * lax.cond(iz == 0, far_part, lambda: zero)
    line = line_of(sums)
    for stage in (0, 2):
        sum_start(1, stage, line)
        line = sum_finish(1, stage)

    @pl.when(iz == 1)
    def _():
        far_part()

    t01, t11, g1, t02, t12, t22, g2 = [take(line, k) / mu for k in range(7)]
    l1, l2 = t01 / shift, t02 / shift
    d1, e1 = t11 - l1 * t01, t12 - l1 * t02
    l3 = e1 / d1
    d2 = t22 - l2 * t02 - l3 * e1
    b1 = g1 - l1
    b2 = g2 - l2 - l3 * b1
    c2 = b2 / d2
    c1 = b1 / d1 - l3 * c2
    c0 = step - l1 * c1 - l2 * c2

    def result_copies(c):
        span = at(c, 0, CHUNK)
        return [
            pltpu.make_async_copy(a.at[:, span, :], b.at[:, span, :], out_sem.at[k, c])
            for k, (a, b) in enumerate(((volt_ref, volt_h), (resid_ref, resid_h)))
        ]

    def finish(c, _):
        for slot in (0, 1):
            for j in range(per):
                span, wide = at(c, j), inner(c, j)
                p = z0[slot, wide, :]
                volt_ref[layer[slot], span, :] = (
                    c0 * p + c1 * (p - step * y1[slot, wide, :]) + c2 * z2[slot, wide, :]
                )
                tail = c0 * s1[slot, span, :] + c1 * s2[slot, span, :] + c2 * s3[slot, span, :]
                resid_ref[layer[slot], span, :] = (src[span, :] - tail) if slot == 0 else -tail
        for move in result_copies(c):
            move.start()
        return 0

    lax.fori_loop(0, chunks, finish, 0)

    def drain(c, _):
        for move in result_copies(c):
            move.wait()
        @pl.when(iz == 1)
        def _():
            far_copy(2, c).wait_send()
            far_copy(3, c).wait_send()

        for stage in range(4):
            for move in side_copies(stage, c):
                move.wait_send()
        return 0

    lax.fori_loop(0, chunks, drain, 0)

    @pl.when(iz == 0)
    def _():
        for n in (22, 23):
            far_left(jnp.int32(n), (2,))
        for k in range(chunks):
            far_copy(3, place(jnp.int32(k))).wait_send()

    @pl.when(iz == 1)
    def _():
        for k in range(4, chunks):
            far_copy(0, turn(jnp.int32(k))).wait_send()

    for stage in range(4):
        for way in (0, 1):
            edge_copy(stage, way).wait_send()


def solution(mesh):
    nx, ny = mesh.shape["gx"], mesh.shape["gy"]

    def shards(load_current, sink_mask, pad_mask, plane_class, via_class, plane_table, via_table):
        _, rows, cols = plane_class.shape
        chunks = rows // CHUNK
        flat = pltpu.VMEM((rows, cols), F32)
        flat_i = pltpu.VMEM((rows, cols), jnp.int32)
        both = pltpu.VMEM((2, rows, cols), F32)
        both_i = pltpu.VMEM((2, rows, cols), jnp.int32)
        tall = pltpu.VMEM((2, rows + 2 * HALO, cols), F32)
        side = pltpu.VMEM((2, rows, LANES), F32)
        field = [tall, side, side, flat]
        dma = pltpu.SemaphoreType.DMA
        scratch = [
            flat, flat_i, flat_i, both_i, both_i,
            pltpu.SMEM(plane_table.shape, F32), pltpu.SMEM(via_table.shape, F32), both, both,
            flat, flat,
            tall, side, side,
            both, both, both, both, flat, flat, flat, flat, flat,
            *field, *field, *field, tall, side, side,
            both, both, both,
            pltpu.VMEM((2, 3, 1, LANES), F32),
            pltpu.VMEM((2, nx, 1, LANES), F32),
            pltpu.VMEM((2, ny, 1, LANES), F32),
            pltpu.VMEM((2, 2 * ny, 1, LANES), F32),
            pltpu.VMEM((1, LANES), F32),
            dma((7,)), dma((2, chunks)),
            dma((4, chunks)), dma((4, chunks)),
            dma((4, 2, chunks)), dma((4, 2, chunks)),
            dma((4, 2)), dma((4, 2)),
            dma((2, nx + 3 * ny)), dma((2, nx + 3 * ny)),
        ]
        shape = jax.ShapeDtypeStruct(plane_class.shape, F32)
        hbm = pl.BlockSpec(memory_space=pltpu.HBM)
        free = pl.BlockSpec(memory_space=pl.ANY)
        return pl.pallas_call(
            functools.partial(kernel, (nx, ny, rows, cols)),
            out_shape=(shape, shape),
            in_specs=[hbm] * 7,
            out_specs=(free, free),
            scratch_shapes=scratch,
            compiler_params=pltpu.CompilerParams(
                collective_id=0, has_side_effects=True, vmem_limit_bytes=58 * 1024 * 1024
            ),
        )(load_current, sink_mask, pad_mask, plane_class, via_class, plane_table, via_table)

    layers = P("gz", "gy", "gx")
    plane = P("gy", "gx")
    table = P("gz", None)
    return jax.shard_map(
        shards,
        mesh=mesh,
        in_specs=(plane, plane, plane, layers, layers, table, table),
        out_specs=(layers, layers),
        check_vma=False,
    )
```

```python
import functools

import jax
import jax.numpy as jnp
from jax import lax
from jax.experimental import pallas as pl
from jax.experimental.pallas import tpu as pltpu
from jax.sharding import PartitionSpec as P

PAD_CONDUCTANCE = 20.0
MESH = pl.DeviceIdType.MESH
HALO = 8
LANES = 128
CHUNK = 24
F32 = jnp.float32


def harmonic(first, second):
    return 2.0 * first * second / (first + second)


def pick(classes, table):
    low = (classes & 1) == 1
    mid = (classes & 2) == 2
    high = (classes & 4) == 4
    pairs = [jnp.where(low, table[2 * k + 1], table[2 * k]) for k in range(4)]
    return jnp.where(
        high, jnp.where(mid, pairs[3], pairs[2]), jnp.where(mid, pairs[1], pairs[0])
    )


def fold(value):
    return sum(
        value[:, k : k + LANES] for k in range(LANES, value.shape[1], LANES)
    ) + value[:, :LANES]


def kernel(
    sizes,
    load_h, sink_h, pad_h, plane_h, via_h, plane_tab_h, via_tab_h,
    volt_ref, resid_ref,
    load_ref, sink_ref, pad_ref, plane_ref, via_ref, plane_tab, via_tab,
    via_mine, via_far,
    g_buf, g_e, g_w,
    east, west, north, south, cross, inv0, inv1, mix, src,
    z0, z0_e, z0_w, z0_o, y1, y1_e, y1_w, y1_o, h2, h2_e, h2_w, h2_o, z2, z2_e, z2_w,
    s1, s2, s3,
    part, got_x, got_y, got_p, first_sum,
    in_sem, far_send, far_recv, side_send, side_recv, edge_send, edge_recv,
    sum_send, sum_recv,
):
    nx, ny, rows, cols = sizes
    chunks = rows // CHUNK
    per = CHUNK // 8
    ix, iy, iz = lax.axis_index("gx"), lax.axis_index("gy"), lax.axis_index("gz")
    gx_up, gx_dn = lax.rem(ix + 1, nx), lax.rem(ix + nx - 1, nx)
    gy_up, gy_dn = lax.rem(iy + 1, ny), lax.rem(iy + ny - 1, ny)
    other = 1 - iz
    layer = (iz, other)

    fetch = [
        pltpu.make_async_copy(a, b, in_sem.at[k])
        for k, (a, b) in enumerate(
            (
                (plane_tab_h, plane_tab), (via_tab_h, via_tab), (plane_h, plane_ref),
                (via_h, via_ref), (pad_h, pad_ref), (sink_h, sink_ref), (load_h, load_ref),
            )
        )
    ]
    for c in fetch:
        c.start()

    def plane_peer(k):
        there = lax.rem(iy * 2 + iz + k, 2 * ny)
        return {"gy": there // 2, "gz": lax.rem(there, 2)}

    barrier = pltpu.get_barrier_semaphore()
    peers = [{"gx": lax.rem(ix + k, nx)} for k in range(1, nx)]
    peers += [plane_peer(k) for k in range(1, 2 * ny)]
    for peer in peers:
        pl.semaphore_signal(barrier, inc=1, device_id=peer, device_id_type=MESH)
    def at(c, j=0, n=8):
        return pl.ds(pl.multiple_of(c * CHUNK + 8 * j, 8), n)

    def inner(c, j=0, n=8):
        return pl.ds(pl.multiple_of(c * CHUNK + (8 * j + HALO), 8), n)

    def remote(source, target, send, recv, where_to):
        return pltpu.make_async_remote_copy(
            src_ref=source, dst_ref=target, send_sem=send, recv_sem=recv,
            device_id=where_to, device_id_type=MESH,
        )

    def far_copy(stage, c):
        buf, out = ((via_mine, via_far), (z0, z0_o), (y1, y1_o), (h2, h2_o))[stage]
        source = buf.at[at(c, 0, CHUNK), :] if stage == 0 else buf.at[1, inner(c, 0, CHUNK), :]
        return remote(
            source, out.at[at(c, 0, CHUNK), :],
            far_send.at[stage, c], far_recv.at[stage, c], {"gz": other},
        )

    fields = ((z0, z0_e, z0_w), (y1, y1_e, y1_w), (h2, h2_e, h2_w), (g_buf, g_e, g_w))

    def side_copies(stage, c):
        buf, buf_e, buf_w = fields[stage]
        span = inner(c, 0, CHUNK)
        return [
            remote(
                buf.at[:, span, pl.ds(cols - LANES, LANES)], buf_w.at[:, at(c, 0, CHUNK), :],
                side_send.at[stage, 0], side_recv.at[stage, c], {"gx": gx_up},
            ),
            remote(
                buf.at[:, span, pl.ds(0, LANES)], buf_e.at[:, at(c, 0, CHUNK), :],
                side_send.at[stage, 1], side_recv.at[stage, c], {"gx": gx_dn},
            ),
        ]

    def edge_copy(stage, way):
        buf = fields[stage][0]
        if way == 0:
            span, out, where_to = pl.ds(rows, 8), pl.ds(0, 8), gy_up
        else:
            span, out, where_to = pl.ds(HALO, 8), pl.ds(HALO + rows, 8), gy_dn
        return remote(
            buf.at[:, span, :], buf.at[:, out, :],
            edge_send.at[stage, way], edge_recv.at[stage, way], {"gy": where_to},
        )

    def send_chunk(stage, c):
        for move in side_copies(stage, c):
            move.start()

        @pl.when(c == chunks - 1)
        def _():
            edge_copy(stage, 0).start()

        @pl.when(c == 0)
        def _():
            edge_copy(stage, 1).start()

    def await_chunk(stage, c):
        both = fields[stage][0].at[:, inner(c, 0, CHUNK), pl.ds(0, 2 * LANES)]
        remote(both, both, side_send.at[stage, 0], side_recv.at[stage, c], {"gx": gx_up}).wait_recv()

        @pl.when(c == 0)
        def _():
            edge_copy(stage, 0).wait_recv()

        @pl.when(c == chunks - 1)
        def _():
            edge_copy(stage, 1).wait_recv()

    def turn(k):
        return lax.rem(k + chunks - 1, chunks)

    def place(k):
        late = jnp.where(k == 3, chunks - 1, jnp.where(k == 4, 0, k - 1))
        return jnp.where(k < 3, k + 1, late)

    for c in fetch[:3]:
        c.wait()
    plane_of = [[plane_tab[layer[slot], k] for k in range(8)] for slot in (0, 1)]
    via_of = [[via_tab[layer[slot], k] for k in range(8)] for slot in (0, 1)]

    def lookup_own(k, _):
        c = place(k)
        for slot in (0, 1):
            for j in range(per):
                g_buf[slot, inner(c, j), :] = pick(
                    plane_ref[layer[slot], at(c, j), :], plane_of[slot]
                )
        return 0

    lax.fori_loop(0, chunks, lookup_own, 0)
    fetch[3].wait()

    def lookup_far(k, _):
        c = turn(k)
        for j in range(per):
            via_mine[at(c, j), :] = pick(via_ref[other, at(c, j), :], via_of[1])
        return 0

    lax.fori_loop(0, chunks, lookup_far, 0)

    pl.semaphore_wait(barrier, len(peers))

    def send_edges(k, _):
        send_chunk(3, turn(k))
        return 0

    lax.fori_loop(0, chunks, send_edges, 0)

    def far_each(n, stages, act):
        for stage in stages:

            @pl.when(n // chunks == stage)
            def _(stage=stage):
                k = n - stage * chunks
                act(far_copy(stage, place(k) if stage else turn(k)))

    def far_left(n, stages):
        far_each(n, stages, lambda move: move.wait_send())

    def far_start(n, stages):
        far_each(n, stages, lambda move: move.start())

    for n in (0, 1):
        far_copy(0, turn(jnp.int32(n))).start()

    def lead(n, _):
        far_left(n - 2, (0,))
        far_start(n, (0,))
        return 0

    lax.fori_loop(2, chunks - 2, lead, 0)
    for n in (chunks - 2, chunks - 1):
        far_copy(0, turn(jnp.int32(n))).start()

    @pl.when(iz == 0)
    def _():
        def clear(c, _):
            z0_o[at(c, 0, CHUNK), :] = jnp.zeros((CHUNK, cols), F32)
            return 0

        lax.fori_loop(0, chunks, clear, 0)

    for c in fetch[4:]:
        c.wait()

    def around(field, slot, c, j):
        buf, buf_e, buf_w = field
        here = buf[slot, inner(c, j), :]
        below = buf[slot, at(c, j), :]
        above = buf[slot, at(c, j + 2), :]
        up = jnp.concatenate([here[1:], above[:1]], 0)
        down = jnp.concatenate([below[7:], here[:7]], 0)
        right = pltpu.roll(
            jnp.concatenate([here, buf_e[slot, at(c, j), :]], 1), cols + LANES - 1, 1
        )[:, :cols]
        left = pltpu.roll(
            jnp.concatenate([buf_w[slot, at(c, j), :], here], 1), 1, 1
        )[:, LANES:]
        return here, right, left, up, down

    is_source = jnp.where(iz == 0, F32(1.0), F32(0.0))
    pad_scale = jnp.where(iz == 0, F32(0.0), F32(PAD_CONDUCTANCE))

    def solve(span, b0, b1):
        m = mix[span, :]
        x1 = (b1 + m * b0) * inv1[span, :]
        return b0 * inv0[span, :] + m * x1, x1

    def plane_edges(slot, c):
        sums = []
        below = g_buf[slot, at(c), :]
        here = g_buf[slot, inner(c), :]
        last = harmonic(below, jnp.concatenate([below[1:], here[:1]], 0))
        for j in range(per):
            span = at(c, j)
            here = g_buf[slot, inner(c, j), :]
            above = g_buf[slot, at(c, j + 2), :]
            wide = jnp.concatenate([g_w[slot, span, :], here, g_e[slot, span, :]], 1)
            edge = harmonic(wide, pltpu.roll(wide, cols + 2 * LANES - 1, 1))[:, : cols + LANES]
            e = edge[:, LANES:]
            w = pltpu.roll(edge, 1, 1)[:, LANES:]
            n = harmonic(here, jnp.concatenate([here[1:], above[:1]], 0))
            s = jnp.concatenate([last[7:], n[:7]], 0)
            last = n
            east[slot, span, :] = e
            west[slot, span, :] = w
            north[slot, span, :] = n
            south[slot, span, :] = s
            sums.append(e + w + n + s)
        return sums

    def build(k, _):
        c = turn(k)
        await_chunk(3, c)
        sums = [plane_edges(slot, c) for slot in (0, 1)]
        far_copy(0, c).wait_recv()
        for j in range(per):
            span = at(c, j)
            via0 = pick(via_ref[iz, span, :], via_of[0])
            via1 = via_mine[span, :]
            link = harmonic(via0, via1)
            far = harmonic(via1, via_far[span, :])
            cross[span, :] = far
            d0 = sums[0][j] + link + pad_scale * pad_ref[span, :].astype(F32)
            d1 = sums[1][j] + link + far
            i0 = 1.0 / d0
            m = link * i0
            i1 = 1.0 / (d1 - link * m)
            inv0[span, :] = i0
            inv1[span, :] = i1
            mix[span, :] = m
            b0 = is_source * (sink_ref[span, :].astype(F32) * load_ref[span, :])
            src[span, :] = b0
            x1 = m * b0 * i1
            z0[0, inner(c, j), :] = b0 * i0 + m * x1
            z0[1, inner(c, j), :] = x1

        send_chunk(0, c)

        @pl.when(jnp.logical_and(iz == 0, k >= 4))
        def _():
            far_left(k, (0,))
            far_start(k + 4, (1,))

        return 0

    lax.fori_loop(0, chunks, build, 0)

    def couple(field, slot, c, j):
        here, right, left, up, down = around(field, slot, c, j)
        span = at(c, j)
        u = (
            east[slot, span, :] * right + west[slot, span, :] * left
            + north[slot, span, :] * up + south[slot, span, :] * down
        )
        return here, u

    zero = jnp.zeros((8, LANES), F32)

    def pass1(k, carry):
        c = place(k)
        mu, t00 = carry

        @pl.when(jnp.logical_and(iz == 0, jnp.logical_or(k == 3, k == 4)))
        def _():
            far_left(chunks - 3 + k, (1,))
            far_start(chunks + 1 + k, (1,))

        await_chunk(0, c)

        @pl.when(iz == 1)
        def _():
            far_copy(1, c).wait_recv()

        for j in range(per):
            span = at(c, j)
            h0, u0 = couple(fields[0], 0, c, j)
            h1, u1 = couple(fields[0], 1, c, j)
            b0 = src[span, :]
            a0, a1 = b0 - u0, -(u1 + cross[span, :] * z0_o[span, :])
            s1[0, span, :] = a0
            s1[1, span, :] = a1
            x0, x1 = solve(span, a0, a1)
            y1[0, inner(c, j), :] = x0
            y1[1, inner(c, j), :] = x1
            mu = mu + fold(h0 * b0)
            t00 = t00 + fold(h0 * a0 + h1 * a1)
        send_chunk(1, c)

        @pl.when(iz == 1)
        def _():
            far_copy(2, c).start()

        return mu, t00

    sums = lax.fori_loop(0, chunks, pass1, (zero, zero))

    lane = lax.broadcasted_iota(jnp.int32, (1, LANES), 1)
    rings = (
        (nx, ix, got_x, lambda k: {"gx": lax.rem(ix + k, nx)}),
        (ny, iy, got_y, lambda k: {"gy": lax.rem(iy + k, ny)}),
        (2 * ny, iy * 2 + iz, got_p, plane_peer),
    )

    def line_of(values):
        line = jnp.zeros((1, LANES), F32)
        for k, value in enumerate(values):
            line = jnp.where(lane == k, jnp.sum(value), line)
        return line

    def sum_moves(which, stage):
        size, me, got, peer = rings[stage]
        return [
            remote(
                part.at[which, stage], got.at[which, me],
                sum_send.at[which, stage], sum_recv.at[which, stage],
                peer(k),
            )
            for k in range(1, size)
        ]

    def sum_start(which, stage, line):
        part[which, stage] = line
        rings[stage][2][which, rings[stage][1]] = line
        for c in sum_moves(which, stage):
            c.start()

    def sum_finish(which, stage):
        size, _, got, peer = rings[stage]
        all_in = got.at[which, pl.ds(0, size - 1)]
        whole = remote(all_in, all_in, sum_send.at[which, stage], sum_recv.at[which, stage], peer(1))
        whole.wait_recv()
        whole.wait_send()
        line = got[which, 0]
        for k in range(1, size):
            line = line + got[which, k]
        return line

    def hand_over():
        return remote(
            part.at[0, 2], first_sum, sum_send.at[0, 2], sum_recv.at[0, 2], {"gz": other}
        )

    first_line = line_of(sums)

    @pl.when(iz == 0)
    def _():
        sum_start(0, 0, first_line)

        for n in (14, 15, 16):
            far_left(jnp.int32(n - 4), (1,))
            far_start(jnp.int32(n), (1, 2))

    def pass2(k, _):
        c = place(k)
        await_chunk(1, c)
        far_copy(2, c).wait_recv()
        for j in range(per):
            span = at(c, j)
            _, u0 = couple(fields[1], 0, c, j)
            _, u1 = couple(fields[1], 1, c, j)
            a0 = s1[0, span, :] - u0
            a1 = s1[1, span, :] - (u1 + cross[span, :] * y1_o[span, :])
            s2[0, span, :] = a0
            s2[1, span, :] = a1
            x0, x1 = solve(span, a0, a1)
            h2[0, inner(c, j), :] = x0
            h2[1, inner(c, j), :] = x1
        send_chunk(2, c)

        @pl.when(iz == 1)
        def _():
            far_copy(3, c).start()

        @pl.when(iz == 0)
        def _():
            @pl.when(k == 0)
            def _():
                far_left(jnp.int32(13), (1,))

            far_left(14 + k, (1, 2))
            far_start(17 + k, (2, 3))

        @pl.when(jnp.logical_and(iz == 0, k == 3))
        def _():
            sum_start(0, 1, sum_finish(0, 0))

        @pl.when(jnp.logical_and(iz == 0, k == chunks - 1))
        def _():
            line = sum_finish(0, 1)
            part[0, 2] = line
            first_sum[...] = line
            hand_over().start()

        return 0

    lax.fori_loop(0, chunks, pass2, 0)

    @pl.when(iz == 0)
    def _():
        def rest(n, _):
            far_start(n, (3,))
            return 0

        lax.fori_loop(25, 4 * chunks, rest, 0)
        hand_over().wait_send()

    @pl.when(iz == 1)
    def _():
        hand_over().wait_recv()

    def take(line, k):
        return jnp.sum(jnp.where(lane == k, line, 0.0), axis=1, keepdims=True)

    line = first_sum[...]
    mu, t00 = take(line, 0), take(line, 1)
    step, shift = mu / t00, t00 / mu

    def third(a, b, c):
        return (b - step * c) - shift * (a - step * b)

    def blend(c, _):
        for slot in (0, 1):
            for j in range(per):
                span = inner(c, j)
                z2[slot, span, :] = third(z0[slot, span, :], y1[slot, span, :], h2[slot, span, :])
        return 0

    lax.fori_loop(0, chunks, blend, 0)

    def pass3(k, carry):
        c = place(k)
        await_chunk(2, c)

        @pl.when(c == 0)
        def _():
            for slot in (0, 1):
                z2[slot, 0:8, :] = third(z0[slot, 0:8, :], y1[slot, 0:8, :], h2[slot, 0:8, :])

        @pl.when(c == chunks - 1)
        def _():
            top = pl.ds(HALO + rows, 8)
            for slot in (0, 1):
                z2[slot, top, :] = third(z0[slot, top, :], y1[slot, top, :], h2[slot, top, :])

        t01, t11, g1, t02, t12, t22, g2 = carry
        for j in range(per):
            span = at(c, j)
            b0 = src[span, :]
            for slot in (0, 1):
                z2_e[slot, span, :] = third(z0_e[slot, span, :], y1_e[slot, span, :], h2_e[slot, span, :])
                z2_w[slot, span, :] = third(z0_w[slot, span, :], y1_w[slot, span, :], h2_w[slot, span, :])
                h, u = couple((z2, z2_e, z2_w), slot, c, j)
                first = s1[slot, span, :]
                second = first - step * s2[slot, span, :]
                r1 = (b0 - step * first) if slot == 0 else -step * first
                a = (second - shift * r1) - u
                s2[slot, span, :] = second
                s3[slot, span, :] = a
                p = z0[slot, inner(c, j), :]
                q = p - step * y1[slot, inner(c, j), :]
                t01 = t01 + fold(p * second)
                t11 = t11 + fold(q * second)
                t02 = t02 + fold(h * first)
                t12 = t12 + fold(h * second)
                t22 = t22 + fold(h * a)
                if slot == 0:
                    g1 = g1 + fold(q * b0)
                    g2 = g2 + fold(h * b0)
        return t01, t11, g1, t02, t12, t22, g2

    sums = list(lax.fori_loop(0, chunks, pass3, (zero,) * 7))

    def cross_term(k, carry):
        c = place(k)
        far_copy(3, c).wait_recv()
        for j in range(per):
            span = at(c, j)
            far = cross[span, :] * third(z0_o[span, :], y1_o[span, :], h2_o[span, :])
            s3[1, span, :] = s3[1, span, :] - far
            carry = carry + fold(z2[1, inner(c, j), :] * far)

        return carry

    def far_part():
        return lax.fori_loop(0, chunks, cross_term, zero)

    sums[5] = sums[5] - 2.0 * lax.cond(iz == 0, far_part, lambda: zero)
    line = line_of(sums)
    for stage in (0, 2):
        sum_start(1, stage, line)
        line = sum_finish(1, stage)

    @pl.when(iz == 1)
    def _():
        far_part()

    t01, t11, g1, t02, t12, t22, g2 = [take(line, k) / mu for k in range(7)]
    l1, l2 = t01 / shift, t02 / shift
    d1, e1 = t11 - l1 * t01, t12 - l1 * t02
    l3 = e1 / d1
    d2 = t22 - l2 * t02 - l3 * e1
    b1 = g1 - l1
    b2 = g2 - l2 - l3 * b1
    c2 = b2 / d2
    c1 = b1 / d1 - l3 * c2
    c0 = step - l1 * c1 - l2 * c2

    def finish(c, _):
        for slot in (0, 1):
            for j in range(per):
                span, wide = at(c, j), inner(c, j)
                p = z0[slot, wide, :]
                volt_ref[layer[slot], span, :] = (
                    c0 * p + c1 * (p - step * y1[slot, wide, :]) + c2 * z2[slot, wide, :]
                )
                tail = c0 * s1[slot, span, :] + c1 * s2[slot, span, :] + c2 * s3[slot, span, :]
                resid_ref[layer[slot], span, :] = (src[span, :] - tail) if slot == 0 else -tail
        return 0

    lax.fori_loop(0, chunks, finish, 0)

    def drain(c, _):
        @pl.when(iz == 1)
        def _():
            far_copy(2, c).wait_send()
            far_copy(3, c).wait_send()

        return 0

    lax.fori_loop(0, chunks, drain, 0)

    @pl.when(iz == 0)
    def _():
        for n in (22, 23):
            far_left(jnp.int32(n), (2,))
        for k in range(chunks):
            far_copy(3, place(jnp.int32(k))).wait_send()

    @pl.when(iz == 1)
    def _():
        for k in range(4, chunks):
            far_copy(0, turn(jnp.int32(k))).wait_send()

    for stage in range(4):
        _, buf_e, buf_w = fields[stage]
        for way in (0, 1):
            edge_copy(stage, way).wait_send()
            remote(
                buf_e, buf_w, side_send.at[stage, way], side_recv.at[stage, 0], {"gx": gx_up}
            ).wait_send()


def solution(mesh):
    nx, ny = mesh.shape["gx"], mesh.shape["gy"]

    def shards(load_current, sink_mask, pad_mask, plane_class, via_class, plane_table, via_table):
        _, rows, cols = plane_class.shape
        chunks = rows // CHUNK
        flat = pltpu.VMEM((rows, cols), F32)
        flat_i = pltpu.VMEM((rows, cols), jnp.int32)
        both = pltpu.VMEM((2, rows, cols), F32)
        both_i = pltpu.VMEM((2, rows, cols), jnp.int32)
        tall = pltpu.VMEM((2, rows + 2 * HALO, cols), F32)
        side = pltpu.VMEM((2, rows, LANES), F32)
        field = [tall, side, side, flat]
        dma = pltpu.SemaphoreType.DMA
        scratch = [
            flat, flat_i, flat_i, both_i, both_i,
            pltpu.SMEM(plane_table.shape, F32), pltpu.SMEM(via_table.shape, F32),
            flat, flat,
            tall, side, side,
            both, both, both, both, flat, flat, flat, flat, flat,
            *field, *field, *field, tall, side, side,
            both, both, both,
            pltpu.VMEM((2, 3, 1, LANES), F32),
            pltpu.VMEM((2, nx, 1, LANES), F32),
            pltpu.VMEM((2, ny, 1, LANES), F32),
            pltpu.VMEM((2, 2 * ny, 1, LANES), F32),
            pltpu.VMEM((1, LANES), F32),
            dma((7,)),
            dma((4, chunks)), dma((4, chunks)),
            dma((4, 2)), dma((4, chunks)),
            dma((4, 2)), dma((4, 2)),
            dma((2, 3)), dma((2, 3)),
        ]
        shape = pltpu.VMEM(plane_class.shape, F32)
        hbm = pl.BlockSpec(memory_space=pltpu.HBM)
        vmem = pl.BlockSpec(memory_space=pltpu.VMEM)
        held = [
            pltpu.with_memory_space_constraint(a, pltpu.HBM)
            for a in (load_current, sink_mask, pad_mask, plane_class, via_class, plane_table, via_table)
        ]
        return pl.pallas_call(
            functools.partial(kernel, (nx, ny, rows, cols)),
            out_shape=(shape, shape),
            in_specs=[hbm] * 7,
            out_specs=(vmem, vmem),
            scratch_shapes=scratch,
            compiler_params=pltpu.CompilerParams(
                collective_id=0, has_side_effects=True, vmem_limit_bytes=48 * 1024 * 1024
            ),
        )(*held)

    layers = P("gz", "gy", "gx")
    plane = P("gy", "gx")
    table = P("gz", None)
    return jax.shard_map(
        shards,
        mesh=mesh,
        in_specs=(plane, plane, plane, layers, layers, table, table),
        out_specs=(layers, layers),
        check_vma=False,
    )
```

```python
import functools

import jax
import jax.numpy as jnp
from jax import lax
from jax.experimental import pallas as pl
from jax.experimental.pallas import tpu as pltpu
from jax.sharding import PartitionSpec as P

PAD_CONDUCTANCE = 20.0
MESH = pl.DeviceIdType.MESH
HALO = 8
LANES = 128
CHUNK = 24
F32 = jnp.float32


def harmonic(first, second):
    return 2.0 * first * second / (first + second)


def pick(classes, table):
    low = (classes & 1) == 1
    mid = (classes & 2) == 2
    high = (classes & 4) == 4
    pairs = [jnp.where(low, table[2 * k + 1], table[2 * k]) for k in range(4)]
    return jnp.where(
        high, jnp.where(mid, pairs[3], pairs[2]), jnp.where(mid, pairs[1], pairs[0])
    )


def fold(value):
    return sum(
        value[:, k : k + LANES] for k in range(LANES, value.shape[1], LANES)
    ) + value[:, :LANES]


def kernel(
    sizes,
    load_h, sink_h, pad_h, plane_h, via_h, plane_tab_h, via_tab_h,
    volt_ref, resid_ref,
    load_ref, sink_ref, pad_ref, plane_ref, via_ref, plane_tab, via_tab,
    via_mine, via_far,
    g_buf, g_e, g_w,
    east, west, north, south, cross, inv0, inv1, mix, src,
    z0, z0_e, z0_w, z0_o, y1, y1_e, y1_w, y1_o, h2, h2_e, h2_w, h2_o, z2, z2_e, z2_w,
    s1, s2, s3,
    edge_out, edge_in, part, got_x, got_p,
    in_sem, far_send, far_recv, side_send, side_recv, edge_send, edge_recv,
    sum_send, sum_recv,
):
    nx, ny, rows, cols = sizes
    chunks = rows // CHUNK
    per = CHUNK // 8
    ix, iy, iz = lax.axis_index("gx"), lax.axis_index("gy"), lax.axis_index("gz")
    gx_up, gx_dn = lax.rem(ix + 1, nx), lax.rem(ix + nx - 1, nx)
    gy_up, gy_dn = lax.rem(iy + 1, ny), lax.rem(iy + ny - 1, ny)
    other = 1 - iz
    layer = (iz, other)

    fetch = [
        pltpu.make_async_copy(a, b, in_sem.at[k])
        for k, (a, b) in enumerate(
            (
                (plane_tab_h, plane_tab), (via_tab_h, via_tab), (plane_h, plane_ref),
                (via_h, via_ref), (pad_h, pad_ref), (sink_h, sink_ref), (load_h, load_ref),
            )
        )
    ]
    for c in fetch:
        c.start()

    def plane_peer(k):
        there = lax.rem(iy * 2 + iz + k, 2 * ny)
        return {"gy": there // 2, "gz": lax.rem(there, 2)}

    barrier = pltpu.get_barrier_semaphore()
    peers = [{"gx": lax.rem(ix + k, nx)} for k in range(1, nx)]
    peers += [plane_peer(k) for k in range(1, 2 * ny)]
    for peer in peers:
        pl.semaphore_signal(barrier, inc=1, device_id=peer, device_id_type=MESH)
    def at(c, j=0, n=8):
        return pl.ds(pl.multiple_of(c * CHUNK + 8 * j, 8), n)

    def inner(c, j=0, n=8):
        return pl.ds(pl.multiple_of(c * CHUNK + (8 * j + HALO), 8), n)

    def remote(source, target, send, recv, where_to):
        return pltpu.make_async_remote_copy(
            src_ref=source, dst_ref=target, send_sem=send, recv_sem=recv,
            device_id=where_to, device_id_type=MESH,
        )

    def far_copy(stage, c):
        buf, out = ((via_mine, via_far), (z0, z0_o), (y1, y1_o), (h2, h2_o))[stage]
        source = buf.at[at(c, 0, CHUNK), :] if stage == 0 else buf.at[1, inner(c, 0, CHUNK), :]
        return remote(
            source, out.at[at(c, 0, CHUNK), :],
            far_send.at[stage, c], far_recv.at[stage, c], {"gz": other},
        )

    fields = ((z0, z0_e, z0_w), (y1, y1_e, y1_w), (h2, h2_e, h2_w), (g_buf, g_e, g_w))

    def side_copies(stage, c):
        buf, buf_e, buf_w = fields[stage]
        span = inner(c, 0, CHUNK)
        return [
            remote(
                buf.at[:, span, pl.ds(cols - LANES, LANES)], buf_w.at[:, at(c, 0, CHUNK), :],
                side_send.at[stage, 0], side_recv.at[stage, c], {"gx": gx_up},
            ),
            remote(
                buf.at[:, span, pl.ds(0, LANES)], buf_e.at[:, at(c, 0, CHUNK), :],
                side_send.at[stage, 1], side_recv.at[stage, c], {"gx": gx_dn},
            ),
        ]

    def edge_copy(stage, way):
        return remote(
            edge_out.at[stage, way], edge_in.at[stage, way],
            edge_send.at[stage, way], edge_recv.at[stage, way], {"gy": (gy_up, gy_dn)[way]},
        )

    parts = [
        (slot, slot * (cols // LANES) + b, slice(b * LANES, (b + 1) * LANES))
        for slot in (0, 1)
        for b in range(cols // LANES)
    ]

    def edge_start(stage, way):
        row = (HALO + rows - 1, HALO)[way]
        for slot, k, lanes in parts:
            edge_out[stage, way, k : k + 1, :] = fields[stage][0][slot, row : row + 1, lanes]
        edge_copy(stage, way).start()

    def edge_finish(stage, way):
        edge_copy(stage, way).wait_recv()
        row = (HALO - 1, HALO + rows)[way]
        for slot, k, lanes in parts:
            fields[stage][0][slot, row : row + 1, lanes] = edge_in[stage, way, k : k + 1, :]

    def send_chunk(stage, c):
        for move in side_copies(stage, c):
            move.start()

        @pl.when(c == chunks - 1)
        def _():
            edge_start(stage, 0)

        @pl.when(c == 0)
        def _():
            edge_start(stage, 1)

    def await_chunk(stage, c):
        both = fields[stage][0].at[:, inner(c, 0, CHUNK), pl.ds(0, 2 * LANES)]
        remote(both, both, side_send.at[stage, 0], side_recv.at[stage, c], {"gx": gx_up}).wait_recv()

        @pl.when(c == 0)
        def _():
            edge_finish(stage, 0)

        @pl.when(c == chunks - 1)
        def _():
            edge_finish(stage, 1)

    def turn(k):
        return lax.rem(k + chunks - 1, chunks)

    def place(k):
        late = jnp.where(k == 3, chunks - 1, jnp.where(k == 4, 0, k - 1))
        return jnp.where(k < 3, k + 1, late)

    for c in fetch[:3]:
        c.wait()
    plane_of = [[plane_tab[layer[slot], k] for k in range(8)] for slot in (0, 1)]
    via_of = [[via_tab[layer[slot], k] for k in range(8)] for slot in (0, 1)]

    def lookup_own(k, _):
        c = place(k)
        for slot in (0, 1):
            for j in range(per):
                g_buf[slot, inner(c, j), :] = pick(
                    plane_ref[layer[slot], at(c, j), :], plane_of[slot]
                )
        return 0

    lax.fori_loop(0, chunks, lookup_own, 0)
    fetch[3].wait()

    def lookup_far(k, _):
        c = turn(k)
        for j in range(per):
            via_mine[at(c, j), :] = pick(via_ref[other, at(c, j), :], via_of[1])
        return 0

    lax.fori_loop(0, chunks, lookup_far, 0)

    pl.semaphore_wait(barrier, len(peers))

    def send_edges(k, _):
        send_chunk(3, turn(k))
        return 0

    lax.fori_loop(0, chunks, send_edges, 0)

    def far_each(n, stages, act):
        for stage in stages:

            @pl.when(n // chunks == stage)
            def _(stage=stage):
                k = n - stage * chunks
                act(far_copy(stage, place(k) if stage else turn(k)))

    def far_left(n, stages):
        far_each(n, stages, lambda move: move.wait_send())

    def far_start(n, stages):
        far_each(n, stages, lambda move: move.start())

    for n in (0, 1):
        far_copy(0, turn(jnp.int32(n))).start()

    def lead(n, _):
        far_left(n - 2, (0,))
        far_start(n, (0,))
        return 0

    lax.fori_loop(2, chunks - 2, lead, 0)
    for n in (chunks - 2, chunks - 1):
        far_copy(0, turn(jnp.int32(n))).start()

    @pl.when(iz == 0)
    def _():
        def clear(c, _):
            z0_o[at(c, 0, CHUNK), :] = jnp.zeros((CHUNK, cols), F32)
            return 0

        lax.fori_loop(0, chunks, clear, 0)

    for c in fetch[4:]:
        c.wait()

    def around(field, slot, c, j):
        buf, buf_e, buf_w = field
        here = buf[slot, inner(c, j), :]
        below = buf[slot, at(c, j), :]
        above = buf[slot, at(c, j + 2), :]
        up = jnp.concatenate([here[1:], above[:1]], 0)
        down = jnp.concatenate([below[7:], here[:7]], 0)
        right = pltpu.roll(
            jnp.concatenate([here, buf_e[slot, at(c, j), :]], 1), cols + LANES - 1, 1
        )[:, :cols]
        left = pltpu.roll(
            jnp.concatenate([buf_w[slot, at(c, j), :], here], 1), 1, 1
        )[:, LANES:]
        return here, right, left, up, down

    is_source = jnp.where(iz == 0, F32(1.0), F32(0.0))
    pad_scale = jnp.where(iz == 0, F32(0.0), F32(PAD_CONDUCTANCE))

    def solve(span, b0, b1):
        m = mix[span, :]
        x1 = (b1 + m * b0) * inv1[span, :]
        return b0 * inv0[span, :] + m * x1, x1

    def plane_edges(slot, c):
        sums = []
        below = g_buf[slot, at(c), :]
        here = g_buf[slot, inner(c), :]
        last = harmonic(below, jnp.concatenate([below[1:], here[:1]], 0))
        for j in range(per):
            span = at(c, j)
            here = g_buf[slot, inner(c, j), :]
            above = g_buf[slot, at(c, j + 2), :]
            wide = jnp.concatenate([g_w[slot, span, :], here, g_e[slot, span, :]], 1)
            edge = harmonic(wide, pltpu.roll(wide, cols + 2 * LANES - 1, 1))[:, : cols + LANES]
            e = edge[:, LANES:]
            w = pltpu.roll(edge, 1, 1)[:, LANES:]
            n = harmonic(here, jnp.concatenate([here[1:], above[:1]], 0))
            s = jnp.concatenate([last[7:], n[:7]], 0)
            last = n
            east[slot, span, :] = e
            west[slot, span, :] = w
            north[slot, span, :] = n
            south[slot, span, :] = s
            sums.append(e + w + n + s)
        return sums

    def build(k, _):
        c = turn(k)
        await_chunk(3, c)
        sums = [plane_edges(slot, c) for slot in (0, 1)]
        far_copy(0, c).wait_recv()
        for j in range(per):
            span = at(c, j)
            via0 = pick(via_ref[iz, span, :], via_of[0])
            via1 = via_mine[span, :]
            link = harmonic(via0, via1)
            far = harmonic(via1, via_far[span, :])
            cross[span, :] = far
            d0 = sums[0][j] + link + pad_scale * pad_ref[span, :].astype(F32)
            d1 = sums[1][j] + link + far
            i0 = 1.0 / d0
            m = link * i0
            i1 = 1.0 / (d1 - link * m)
            inv0[span, :] = i0
            inv1[span, :] = i1
            mix[span, :] = m
            b0 = is_source * (sink_ref[span, :].astype(F32) * load_ref[span, :])
            src[span, :] = b0
            x1 = m * b0 * i1
            z0[0, inner(c, j), :] = b0 * i0 + m * x1
            z0[1, inner(c, j), :] = x1

        send_chunk(0, c)

        @pl.when(jnp.logical_and(iz == 0, k >= 4))
        def _():
            far_left(k, (0,))
            far_start(k + 4, (1,))

        return 0

    lax.fori_loop(0, chunks, build, 0)

    def couple(field, slot, c, j):
        here, right, left, up, down = around(field, slot, c, j)
        span = at(c, j)
        u = (
            east[slot, span, :] * right + west[slot, span, :] * left
            + north[slot, span, :] * up + south[slot, span, :] * down
        )
        return here, u

    zero = jnp.zeros((8, LANES), F32)

    def pass1(k, carry):
        c = place(k)
        mu, t00 = carry

        @pl.when(jnp.logical_and(iz == 0, jnp.logical_or(k == 3, k == 4)))
        def _():
            far_left(chunks - 3 + k, (1,))
            far_start(chunks + 1 + k, (1,))

        await_chunk(0, c)

        @pl.when(iz == 1)
        def _():
            far_copy(1, c).wait_recv()

        for j in range(per):
            span = at(c, j)
            h0, u0 = couple(fields[0], 0, c, j)
            h1, u1 = couple(fields[0], 1, c, j)
            b0 = src[span, :]
            a0, a1 = b0 - u0, -(u1 + cross[span, :] * z0_o[span, :])
            s1[0, span, :] = a0
            s1[1, span, :] = a1
            x0, x1 = solve(span, a0, a1)
            y1[0, inner(c, j), :] = x0
            y1[1, inner(c, j), :] = x1
            mu = mu + fold(h0 * b0)
            t00 = t00 + fold(h0 * a0 + h1 * a1)
        send_chunk(1, c)

        @pl.when(iz == 1)
        def _():
            far_copy(2, c).start()

        return mu, t00

    sums = lax.fori_loop(0, chunks, pass1, (zero, zero))

    lane = lax.broadcasted_iota(jnp.int32, (1, LANES), 1)
    rings = (
        (nx, ix, got_x, lambda k: {"gx": lax.rem(ix + k, nx)}),
        (2 * ny, iy * 2 + iz, got_p, plane_peer),
    )

    def line_of(values):
        line = jnp.zeros((1, LANES), F32)
        for k, value in enumerate(values):
            line = jnp.where(lane == k, jnp.sum(value), line)
        return line

    def sum_moves(which, stage):
        size, me, got, peer = rings[stage]
        return [
            remote(
                part.at[which, stage], got.at[which, me],
                sum_send.at[which, stage], sum_recv.at[which, stage],
                peer(k),
            )
            for k in range(1, size)
        ]

    def sum_start(which, stage, line):
        part[which, stage] = line
        rings[stage][2][which, rings[stage][1]] = line
        for c in sum_moves(which, stage):
            c.start()

    def sum_finish(which, stage):
        size, _, got, peer = rings[stage]
        all_in = got.at[which, pl.ds(0, size - 1)]
        whole = remote(all_in, all_in, sum_send.at[which, stage], sum_recv.at[which, stage], peer(1))
        whole.wait_recv()
        whole.wait_send()
        line = got[which, 0]
        for k in range(1, size):
            line = line + got[which, k]
        return line

    first_line = line_of(sums)

    @pl.when(iz == 0)
    def _():
        sum_start(0, 0, first_line)

        for n in (14, 15, 16):
            far_left(jnp.int32(n - 4), (1,))
            far_start(jnp.int32(n), (1, 2))

    def pass2(k, _):
        c = place(k)
        await_chunk(1, c)
        far_copy(2, c).wait_recv()
        for j in range(per):
            span = at(c, j)
            _, u0 = couple(fields[1], 0, c, j)
            _, u1 = couple(fields[1], 1, c, j)
            a0 = s1[0, span, :] - u0
            a1 = s1[1, span, :] - (u1 + cross[span, :] * y1_o[span, :])
            s2[0, span, :] = a0
            s2[1, span, :] = a1
            x0, x1 = solve(span, a0, a1)
            h2[0, inner(c, j), :] = x0
            h2[1, inner(c, j), :] = x1
        send_chunk(2, c)

        @pl.when(iz == 1)
        def _():
            far_copy(3, c).start()

        @pl.when(iz == 0)
        def _():
            @pl.when(k == 0)
            def _():
                far_left(jnp.int32(13), (1,))

            far_left(14 + k, (1, 2))
            far_start(17 + k, (2, 3))

        @pl.when(jnp.logical_and(iz == 0, k == 2))
        def _():
            sum_start(0, 1, sum_finish(0, 0))

        return 0

    lax.fori_loop(0, chunks, pass2, 0)

    def plane_arrived(count):
        all_in = got_p.at[0, pl.ds(0, count)]
        return remote(all_in, all_in, sum_send.at[0, 1], sum_recv.at[0, 1], plane_peer(1))

    @pl.when(iz == 0)
    def _():
        plane_arrived(ny - 1).wait_recv()
        plane_arrived(2 * ny - 1).wait_send()

        def rest(n, _):
            far_start(n, (3,))
            return 0

        lax.fori_loop(25, 4 * chunks, rest, 0)

    @pl.when(iz == 1)
    def _():
        plane_arrived(ny).wait_recv()

    def take(line, k):
        return jnp.sum(jnp.where(lane == k, line, 0.0), axis=1, keepdims=True)

    line = got_p[0, 0]
    for k in range(1, ny):
        line = line + got_p[0, 2 * k]
    mu, t00 = take(line, 0), take(line, 1)
    step, shift = mu / t00, t00 / mu

    def third(a, b, c):
        return (b - step * c) - shift * (a - step * b)

    def blend(c, _):
        for slot in (0, 1):
            for j in range(per):
                span = inner(c, j)
                z2[slot, span, :] = third(z0[slot, span, :], y1[slot, span, :], h2[slot, span, :])
        return 0

    lax.fori_loop(0, chunks, blend, 0)

    def pass3(k, carry):
        c = lax.rem(k + 1, chunks)
        await_chunk(2, c)

        @pl.when(c == 0)
        def _():
            for slot in (0, 1):
                z2[slot, 0:8, :] = third(z0[slot, 0:8, :], y1[slot, 0:8, :], h2[slot, 0:8, :])

        @pl.when(c == chunks - 1)
        def _():
            top = pl.ds(HALO + rows, 8)
            for slot in (0, 1):
                z2[slot, top, :] = third(z0[slot, top, :], y1[slot, top, :], h2[slot, top, :])

        t01, t11, g1, t02, t12, t22, g2 = carry
        for j in range(per):
            span = at(c, j)
            b0 = src[span, :]
            for slot in (0, 1):
                z2_e[slot, span, :] = third(z0_e[slot, span, :], y1_e[slot, span, :], h2_e[slot, span, :])
                z2_w[slot, span, :] = third(z0_w[slot, span, :], y1_w[slot, span, :], h2_w[slot, span, :])
                h, u = couple((z2, z2_e, z2_w), slot, c, j)
                first = s1[slot, span, :]
                second = first - step * s2[slot, span, :]
                r1 = (b0 - step * first) if slot == 0 else -step * first
                a = (second - shift * r1) - u
                s2[slot, span, :] = second
                s3[slot, span, :] = a
                p = z0[slot, inner(c, j), :]
                q = p - step * y1[slot, inner(c, j), :]
                t01 = t01 + fold(p * second)
                t11 = t11 + fold(q * second)
                t02 = t02 + fold(h * first)
                t12 = t12 + fold(h * second)
                t22 = t22 + fold(h * a)
                if slot == 0:
                    g1 = g1 + fold(q * b0)
                    g2 = g2 + fold(h * b0)
        return t01, t11, g1, t02, t12, t22, g2

    sums = list(lax.fori_loop(0, chunks, pass3, (zero,) * 7))

    def cross_term(k, carry):
        c = place(k)
        far_copy(3, c).wait_recv()
        for j in range(per):
            span = at(c, j)
            far = cross[span, :] * third(z0_o[span, :], y1_o[span, :], h2_o[span, :])
            s3[1, span, :] = s3[1, span, :] - far
            carry = carry + fold(z2[1, inner(c, j), :] * far)

        return carry

    def far_part():
        return lax.fori_loop(0, chunks, cross_term, zero)

    sums[5] = sums[5] - 2.0 * lax.cond(iz == 0, far_part, lambda: zero)
    line = line_of(sums)
    for stage in (0, 1):
        sum_start(1, stage, line)
        line = sum_finish(1, stage)

    @pl.when(iz == 1)
    def _():
        far_part()

    t01, t11, g1, t02, t12, t22, g2 = [take(line, k) / mu for k in range(7)]
    l1, l2 = t01 / shift, t02 / shift
    d1, e1 = t11 - l1 * t01, t12 - l1 * t02
    l3 = e1 / d1
    d2 = t22 - l2 * t02 - l3 * e1
    b1 = g1 - l1
    b2 = g2 - l2 - l3 * b1
    c2 = b2 / d2
    c1 = b1 / d1 - l3 * c2
    c0 = step - l1 * c1 - l2 * c2

    def finish(c, _):
        for slot in (0, 1):
            for j in range(per):
                span, wide = at(c, j), inner(c, j)
                p = z0[slot, wide, :]
                volt_ref[layer[slot], span, :] = (
                    c0 * p + c1 * (p - step * y1[slot, wide, :]) + c2 * z2[slot, wide, :]
                )
                tail = c0 * s1[slot, span, :] + c1 * s2[slot, span, :] + c2 * s3[slot, span, :]
                resid_ref[layer[slot], span, :] = (src[span, :] - tail) if slot == 0 else -tail
        return 0

    lax.fori_loop(0, chunks, finish, 0)

    def drain(c, _):
        @pl.when(iz == 1)
        def _():
            far_copy(2, c).wait_send()
            far_copy(3, c).wait_send()

        return 0

    lax.fori_loop(0, chunks, drain, 0)

    @pl.when(iz == 0)
    def _():
        for n in (22, 23):
            far_left(jnp.int32(n), (2,))
        for k in range(chunks):
            far_copy(3, place(jnp.int32(k))).wait_send()

    @pl.when(iz == 1)
    def _():
        for k in range(4, chunks):
            far_copy(0, turn(jnp.int32(k))).wait_send()

    for stage in range(4):
        _, buf_e, buf_w = fields[stage]
        for way in (0, 1):
            edge_copy(stage, way).wait_send()
            remote(
                buf_e, buf_w, side_send.at[stage, way], side_recv.at[stage, 0], {"gx": gx_up}
            ).wait_send()


def solution(mesh):
    nx, ny = mesh.shape["gx"], mesh.shape["gy"]

    def shards(load_current, sink_mask, pad_mask, plane_class, via_class, plane_table, via_table):
        _, rows, cols = plane_class.shape
        chunks = rows // CHUNK
        flat = pltpu.VMEM((rows, cols), F32)
        flat_i = pltpu.VMEM((rows, cols), jnp.int32)
        both = pltpu.VMEM((2, rows, cols), F32)
        both_i = pltpu.VMEM((2, rows, cols), jnp.int32)
        tall = pltpu.VMEM((2, rows + 2 * HALO, cols), F32)
        side = pltpu.VMEM((2, rows, LANES), F32)
        field = [tall, side, side, flat]
        dma = pltpu.SemaphoreType.DMA
        scratch = [
            flat, flat_i, flat_i, both_i, both_i,
            pltpu.SMEM(plane_table.shape, F32), pltpu.SMEM(via_table.shape, F32),
            flat, flat,
            tall, side, side,
            both, both, both, both, flat, flat, flat, flat, flat,
            *field, *field, *field, tall, side, side,
            both, both, both,
            pltpu.VMEM((4, 2, 2 * cols // LANES, LANES), F32),
            pltpu.VMEM((4, 2, 2 * cols // LANES, LANES), F32),
            pltpu.VMEM((2, 2, 1, LANES), F32),
            pltpu.VMEM((2, nx, 1, LANES), F32),
            pltpu.VMEM((2, 2 * ny, 1, LANES), F32),
            dma((7,)),
            dma((4, chunks)), dma((4, chunks)),
            dma((4, 2)), dma((4, chunks)),
            dma((4, 2)), dma((4, 2)),
            dma((2, 2)), dma((2, 2)),
        ]
        shape = pltpu.VMEM(plane_class.shape, F32)
        hbm = pl.BlockSpec(memory_space=pltpu.HBM)
        vmem = pl.BlockSpec(memory_space=pltpu.VMEM)
        held = [
            pltpu.with_memory_space_constraint(a, pltpu.HBM)
            for a in (load_current, sink_mask, pad_mask, plane_class, via_class, plane_table, via_table)
        ]
        return pl.pallas_call(
            functools.partial(kernel, (nx, ny, rows, cols)),
            out_shape=(shape, shape),
            in_specs=[hbm] * 7,
            out_specs=(vmem, vmem),
            scratch_shapes=scratch,
            compiler_params=pltpu.CompilerParams(
                collective_id=0, has_side_effects=True, vmem_limit_bytes=48 * 1024 * 1024
            ),
        )(*held)

    layers = P("gz", "gy", "gx")
    plane = P("gy", "gx")
    table = P("gz", None)
    return jax.shard_map(
        shards,
        mesh=mesh,
        in_specs=(plane, plane, plane, layers, layers, table, table),
        out_specs=(layers, layers),
        check_vma=False,
    )
```

```python
import functools

import jax
import jax.numpy as jnp
from jax import lax
from jax.experimental import pallas as pl
from jax.experimental.pallas import tpu as pltpu
from jax.sharding import PartitionSpec as P

PAD_CONDUCTANCE = 20.0
MESH = pl.DeviceIdType.MESH
HALO = 8
LANES = 128
CHUNK = 24
F32 = jnp.float32


def harmonic(first, second):
    return 2.0 * first * second / (first + second)


def pick(classes, table):
    low = (classes & 1) == 1
    mid = (classes & 2) == 2
    high = (classes & 4) == 4
    pairs = [jnp.where(low, table[2 * k + 1], table[2 * k]) for k in range(4)]
    return jnp.where(
        high, jnp.where(mid, pairs[3], pairs[2]), jnp.where(mid, pairs[1], pairs[0])
    )


def fold(value):
    return sum(
        value[:, k : k + LANES] for k in range(LANES, value.shape[1], LANES)
    ) + value[:, :LANES]


def kernel(
    sizes,
    load_h, sink_h, pad_h, plane_h, via_h, plane_tab_h, via_tab_h,
    volt_ref, resid_ref,
    load_ref, sink_ref, pad_ref, plane_ref, via_ref, plane_tab, via_tab,
    via_mine, via_far,
    g_buf, g_e, g_w,
    east, west, north, south, cross, inv0, inv1, mix, src,
    z0, z0_e, z0_w, z0_o, y1, y1_e, y1_w, y1_o, h2, h2_e, h2_w, h2_o, z2, z2_e, z2_w,
    s1, s2, s3,
    edge_out, edge_in, part, got_x, got_p,
    in_sem, far_send, far_recv, side_send, side_recv, edge_send, edge_recv,
    sum_send, sum_recv,
):
    nx, ny, rows, cols = sizes
    chunks = rows // CHUNK
    per = CHUNK // 8
    ix, iy, iz = lax.axis_index("gx"), lax.axis_index("gy"), lax.axis_index("gz")
    gx_up, gx_dn = lax.rem(ix + 1, nx), lax.rem(ix + nx - 1, nx)
    gy_up, gy_dn = lax.rem(iy + 1, ny), lax.rem(iy + ny - 1, ny)
    other = 1 - iz
    layer = (iz, other)

    fetch = [
        pltpu.make_async_copy(a, b, in_sem.at[k])
        for k, (a, b) in enumerate(
            (
                (via_tab_h, via_tab), (via_h.at[other], via_ref.at[other]), (plane_tab_h, plane_tab),
                (plane_h, plane_ref), (via_h.at[iz], via_ref.at[iz]), (pad_h, pad_ref), (sink_h, sink_ref), (load_h, load_ref),
            )
        )
    ]
    for c in fetch:
        c.start()

    def plane_peer(k):
        there = lax.rem(iy * 2 + iz + k, 2 * ny)
        return {"gy": there // 2, "gz": lax.rem(there, 2)}

    barrier = pltpu.get_barrier_semaphore()
    peers = [{"gx": lax.rem(ix + k, nx)} for k in range(1, nx)]
    peers += [plane_peer(k) for k in range(1, 2 * ny)]
    for peer in peers:
        pl.semaphore_signal(barrier, inc=1, device_id=peer, device_id_type=MESH)
    def at(c, j=0, n=8):
        return pl.ds(pl.multiple_of(c * CHUNK + 8 * j, 8), n)

    def inner(c, j=0, n=8):
        return pl.ds(pl.multiple_of(c * CHUNK + (8 * j + HALO), 8), n)

    def remote(source, target, send, recv, where_to):
        return pltpu.make_async_remote_copy(
            src_ref=source, dst_ref=target, send_sem=send, recv_sem=recv,
            device_id=where_to, device_id_type=MESH,
        )

    def far_copy(stage, c):
        buf, out = ((via_mine, via_far), (z0, z0_o), (y1, y1_o), (h2, h2_o))[stage]
        source = buf.at[at(c, 0, CHUNK), :] if stage == 0 else buf.at[1, inner(c, 0, CHUNK), :]
        return remote(
            source, out.at[at(c, 0, CHUNK), :],
            far_send.at[stage, c], far_recv.at[stage, c], {"gz": other},
        )

    fields = ((z0, z0_e, z0_w), (y1, y1_e, y1_w), (h2, h2_e, h2_w), (g_buf, g_e, g_w))

    def side_copies(stage, c):
        buf, buf_e, buf_w = fields[stage]
        span = inner(c, 0, CHUNK)
        return [
            remote(
                buf.at[:, span, pl.ds(cols - LANES, LANES)], buf_w.at[:, at(c, 0, CHUNK), :],
                side_send.at[stage, 0], side_recv.at[stage, c], {"gx": gx_up},
            ),
            remote(
                buf.at[:, span, pl.ds(0, LANES)], buf_e.at[:, at(c, 0, CHUNK), :],
                side_send.at[stage, 1], side_recv.at[stage, c], {"gx": gx_dn},
            ),
        ]

    def edge_copy(stage, way):
        return remote(
            edge_out.at[stage, way], edge_in.at[stage, way],
            edge_send.at[stage, way], edge_recv.at[stage, way], {"gy": (gy_up, gy_dn)[way]},
        )

    parts = [
        (slot, slot * (cols // LANES) + b, slice(b * LANES, (b + 1) * LANES))
        for slot in (0, 1)
        for b in range(cols // LANES)
    ]

    def edge_start(stage, way):
        row = (HALO + rows - 1, HALO)[way]
        for slot, k, lanes in parts:
            edge_out[stage, way, k : k + 1, :] = fields[stage][0][slot, row : row + 1, lanes]
        edge_copy(stage, way).start()

    def edge_finish(stage, way):
        edge_copy(stage, way).wait_recv()
        row = (HALO - 1, HALO + rows)[way]
        for slot, k, lanes in parts:
            fields[stage][0][slot, row : row + 1, lanes] = edge_in[stage, way, k : k + 1, :]

    def send_chunk(stage, c):
        for move in side_copies(stage, c):
            move.start()

        @pl.when(c == chunks - 1)
        def _():
            edge_start(stage, 0)

        @pl.when(c == 0)
        def _():
            edge_start(stage, 1)

    def await_chunk(stage, c):
        both = fields[stage][0].at[:, inner(c, 0, CHUNK), pl.ds(0, 2 * LANES)]
        remote(both, both, side_send.at[stage, 0], side_recv.at[stage, c], {"gx": gx_up}).wait_recv()

        @pl.when(c == 0)
        def _():
            edge_finish(stage, 0)

        @pl.when(c == chunks - 1)
        def _():
            edge_finish(stage, 1)

    def turn(k):
        return lax.rem(k + chunks - 1, chunks)

    def place(k):
        late = jnp.where(k == 3, chunks - 1, jnp.where(k == 4, 0, k - 1))
        return jnp.where(k < 3, k + 1, late)

    for c in fetch[:2]:
        c.wait()
    via_of = [[via_tab[layer[slot], k] for k in range(8)] for slot in (0, 1)]

    def lookup_far(k, _):
        c = turn(k)
        for j in range(per):
            via_mine[at(c, j), :] = pick(via_ref[other, at(c, j), :], via_of[1])
        return 0

    lax.fori_loop(0, chunks, lookup_far, 0)
    pl.semaphore_wait(barrier, len(peers))
    for n in (0, 1):
        far_copy(0, turn(jnp.int32(n))).start()

    for c in fetch[2:4]:
        c.wait()
    plane_of = [[plane_tab[layer[slot], k] for k in range(8)] for slot in (0, 1)]

    def lookup_own(k, _):
        c = turn(k)
        for slot in (0, 1):
            for j in range(per):
                g_buf[slot, inner(c, j), :] = pick(
                    plane_ref[layer[slot], at(c, j), :], plane_of[slot]
                )
        send_chunk(3, c)
        return 0

    lax.fori_loop(0, chunks, lookup_own, 0)

    def far_each(n, stages, act):
        for stage in stages:

            @pl.when(n // chunks == stage)
            def _(stage=stage):
                k = n - stage * chunks
                act(far_copy(stage, place(k) if stage else turn(k)))

    def far_left(n, stages):
        far_each(n, stages, lambda move: move.wait_send())

    def far_start(n, stages):
        far_each(n, stages, lambda move: move.start())

    def lead(n, _):
        far_left(n - 2, (0,))
        far_start(n, (0,))
        return 0

    lax.fori_loop(2, chunks - 2, lead, 0)
    for n in (chunks - 2, chunks - 1):
        far_copy(0, turn(jnp.int32(n))).start()

    @pl.when(iz == 0)
    def _():
        def clear(c, _):
            z0_o[at(c, 0, CHUNK), :] = jnp.zeros((CHUNK, cols), F32)
            return 0

        lax.fori_loop(0, chunks, clear, 0)

    for c in fetch[4:]:
        c.wait()

    def around(field, slot, c, j):
        buf, buf_e, buf_w = field
        here = buf[slot, inner(c, j), :]
        below = buf[slot, at(c, j), :]
        above = buf[slot, at(c, j + 2), :]
        up = jnp.concatenate([here[1:], above[:1]], 0)
        down = jnp.concatenate([below[7:], here[:7]], 0)
        right = pltpu.roll(
            jnp.concatenate([here, buf_e[slot, at(c, j), :]], 1), cols + LANES - 1, 1
        )[:, :cols]
        left = pltpu.roll(
            jnp.concatenate([buf_w[slot, at(c, j), :], here], 1), 1, 1
        )[:, LANES:]
        return here, right, left, up, down

    is_source = jnp.where(iz == 0, F32(1.0), F32(0.0))
    pad_scale = jnp.where(iz == 0, F32(0.0), F32(PAD_CONDUCTANCE))

    def solve(span, b0, b1):
        m = mix[span, :]
        x1 = (b1 + m * b0) * inv1[span, :]
        return b0 * inv0[span, :] + m * x1, x1

    def plane_edges(slot, c):
        sums = []
        below = g_buf[slot, at(c), :]
        here = g_buf[slot, inner(c), :]
        last = harmonic(below, jnp.concatenate([below[1:], here[:1]], 0))
        for j in range(per):
            span = at(c, j)
            here = g_buf[slot, inner(c, j), :]
            above = g_buf[slot, at(c, j + 2), :]
            wide = jnp.concatenate([g_w[slot, span, :], here, g_e[slot, span, :]], 1)
            edge = harmonic(wide, pltpu.roll(wide, cols + 2 * LANES - 1, 1))[:, : cols + LANES]
            e = edge[:, LANES:]
            w = pltpu.roll(edge, 1, 1)[:, LANES:]
            n = harmonic(here, jnp.concatenate([here[1:], above[:1]], 0))
            s = jnp.concatenate([last[7:], n[:7]], 0)
            last = n
            east[slot, span, :] = e
            west[slot, span, :] = w
            north[slot, span, :] = n
            south[slot, span, :] = s
            sums.append(e + w + n + s)
        return sums

    def build(k, _):
        c = turn(k)
        await_chunk(3, c)
        sums = [plane_edges(slot, c) for slot in (0, 1)]
        far_copy(0, c).wait_recv()
        for j in range(per):
            span = at(c, j)
            via0 = pick(via_ref[iz, span, :], via_of[0])
            via1 = via_mine[span, :]
            link = harmonic(via0, via1)
            far = harmonic(via1, via_far[span, :])
            cross[span, :] = far
            d0 = sums[0][j] + link + pad_scale * pad_ref[span, :].astype(F32)
            d1 = sums[1][j] + link + far
            i0 = 1.0 / d0
            m = link * i0
            i1 = 1.0 / (d1 - link * m)
            inv0[span, :] = i0
            inv1[span, :] = i1
            mix[span, :] = m
            b0 = is_source * (sink_ref[span, :].astype(F32) * load_ref[span, :])
            src[span, :] = b0
            x1 = m * b0 * i1
            z0[0, inner(c, j), :] = b0 * i0 + m * x1
            z0[1, inner(c, j), :] = x1

        send_chunk(0, c)

        @pl.when(jnp.logical_and(iz == 0, k >= 4))
        def _():
            far_left(k, (0,))
            far_start(k + 4, (1,))

        return 0

    lax.fori_loop(0, chunks, build, 0)

    def couple(field, slot, c, j):
        here, right, left, up, down = around(field, slot, c, j)
        span = at(c, j)
        u = (
            east[slot, span, :] * right + west[slot, span, :] * left
            + north[slot, span, :] * up + south[slot, span, :] * down
        )
        return here, u

    zero = jnp.zeros((8, LANES), F32)

    def pass1(k, carry):
        c = place(k)
        mu, t00 = carry

        @pl.when(jnp.logical_and(iz == 0, jnp.logical_or(k == 3, k == 4)))
        def _():
            far_left(chunks - 3 + k, (1,))
            far_start(chunks + 1 + k, (1,))

        await_chunk(0, c)

        @pl.when(iz == 1)
        def _():
            far_copy(1, c).wait_recv()

        for j in range(per):
            span = at(c, j)
            h0, u0 = couple(fields[0], 0, c, j)
            h1, u1 = couple(fields[0], 1, c, j)
            b0 = src[span, :]
            a0, a1 = b0 - u0, -(u1 + cross[span, :] * z0_o[span, :])
            s1[0, span, :] = a0
            s1[1, span, :] = a1
            x0, x1 = solve(span, a0, a1)
            y1[0, inner(c, j), :] = x0
            y1[1, inner(c, j), :] = x1
            mu = mu + fold(h0 * b0)
            t00 = t00 + fold(h0 * a0 + h1 * a1)
        send_chunk(1, c)

        @pl.when(iz == 1)
        def _():
            far_copy(2, c).start()

        return mu, t00

    sums = lax.fori_loop(0, chunks, pass1, (zero, zero))

    lane = lax.broadcasted_iota(jnp.int32, (1, LANES), 1)
    rings = (
        (nx, ix, got_x, lambda k: {"gx": lax.rem(ix + k, nx)}),
        (2 * ny, iy * 2 + iz, got_p, plane_peer),
    )

    def line_of(values):
        line = jnp.zeros((1, LANES), F32)
        for k, value in enumerate(values):
            line = jnp.where(lane == k, jnp.sum(value), line)
        return line

    def sum_moves(which, stage):
        size, me, got, peer = rings[stage]
        return [
            remote(
                part.at[which, stage], got.at[which, me],
                sum_send.at[which, stage], sum_recv.at[which, stage],
                peer(k),
            )
            for k in range(1, size)
        ]

    def sum_start(which, stage, line):
        part[which, stage] = line
        rings[stage][2][which, rings[stage][1]] = line
        for c in sum_moves(which, stage):
            c.start()

    def sum_finish(which, stage):
        size, _, got, peer = rings[stage]
        all_in = got.at[which, pl.ds(0, size - 1)]
        whole = remote(all_in, all_in, sum_send.at[which, stage], sum_recv.at[which, stage], peer(1))
        whole.wait_recv()
        whole.wait_send()
        line = got[which, 0]
        for k in range(1, size):
            line = line + got[which, k]
        return line

    first_line = line_of(sums)

    @pl.when(iz == 0)
    def _():
        sum_start(0, 0, first_line)

        for n in (14, 15, 16):
            far_left(jnp.int32(n - 4), (1,))
            far_start(jnp.int32(n), (1, 2))

    def pass2(k, _):
        c = place(k)
        await_chunk(1, c)
        far_copy(2, c).wait_recv()
        for j in range(per):
            span = at(c, j)
            _, u0 = couple(fields[1], 0, c, j)
            _, u1 = couple(fields[1], 1, c, j)
            a0 = s1[0, span, :] - u0
            a1 = s1[1, span, :] - (u1 + cross[span, :] * y1_o[span, :])
            s2[0, span, :] = a0
            s2[1, span, :] = a1
            x0, x1 = solve(span, a0, a1)
            h2[0, inner(c, j), :] = x0
            h2[1, inner(c, j), :] = x1
        send_chunk(2, c)

        @pl.when(iz == 1)
        def _():
            far_copy(3, c).start()

        @pl.when(jnp.logical_and(iz == 0, k < chunks - 1))
        def _():
            @pl.when(k == 0)
            def _():
                far_left(jnp.int32(13), (1,))

            far_left(14 + k, (1, 2))
            far_start(17 + k, (2,))

        @pl.when(jnp.logical_and(iz == 0, k == 2))
        def _():
            sum_start(0, 1, sum_finish(0, 0))

        return 0

    lax.fori_loop(0, chunks, pass2, 0)

    def send_rest(first, last):
        def rest(n, _):
            far_start(n, (3,))
            return 0

        lax.fori_loop(first, last, rest, 0)

    def plane_arrived(count):
        all_in = got_p.at[0, pl.ds(0, count)]
        return remote(all_in, all_in, sum_send.at[0, 1], sum_recv.at[0, 1], plane_peer(1))

    @pl.when(iz == 0)
    def _():
        plane_arrived(ny - 1).wait_recv()
        plane_arrived(2 * ny - 1).wait_send()

    @pl.when(iz == 1)
    def _():
        plane_arrived(ny).wait_recv()

    def take(line, k):
        return jnp.sum(jnp.where(lane == k, line, 0.0), axis=1, keepdims=True)

    line = got_p[0, 0]
    for k in range(1, ny):
        line = line + got_p[0, 2 * k]
    mu, t00 = take(line, 0), take(line, 1)
    step, shift = mu / t00, t00 / mu

    def third(a, b, c):
        return (b - step * c) - shift * (a - step * b)

    def blend(c, _):
        for slot in (0, 1):
            for j in range(per):
                span = inner(c, j)
                z2[slot, span, :] = third(z0[slot, span, :], y1[slot, span, :], h2[slot, span, :])
        return 0

    lax.fori_loop(0, chunks, blend, 0)

    def pass3(k, carry):
        c = lax.rem(k + 1, chunks)
        await_chunk(2, c)

        @pl.when(c == 0)
        def _():
            for slot in (0, 1):
                z2[slot, 0:8, :] = third(z0[slot, 0:8, :], y1[slot, 0:8, :], h2[slot, 0:8, :])

        @pl.when(c == chunks - 1)
        def _():
            top = pl.ds(HALO + rows, 8)
            for slot in (0, 1):
                z2[slot, top, :] = third(z0[slot, top, :], y1[slot, top, :], h2[slot, top, :])

        t01, t11, g1, t02, t12, t22, g2 = carry
        for j in range(per):
            span = at(c, j)
            b0 = src[span, :]
            for slot in (0, 1):
                z2_e[slot, span, :] = third(z0_e[slot, span, :], y1_e[slot, span, :], h2_e[slot, span, :])
                z2_w[slot, span, :] = third(z0_w[slot, span, :], y1_w[slot, span, :], h2_w[slot, span, :])
                h, u = couple((z2, z2_e, z2_w), slot, c, j)
                first = s1[slot, span, :]
                second = first - step * s2[slot, span, :]
                r1 = (b0 - step * first) if slot == 0 else -step * first
                a = (second - shift * r1) - u
                s2[slot, span, :] = second
                s3[slot, span, :] = a
                p = z0[slot, inner(c, j), :]
                q = p - step * y1[slot, inner(c, j), :]
                t01 = t01 + fold(p * second)
                t11 = t11 + fold(q * second)
                t02 = t02 + fold(h * first)
                t12 = t12 + fold(h * second)
                t22 = t22 + fold(h * a)
                if slot == 0:
                    g1 = g1 + fold(q * b0)
                    g2 = g2 + fold(h * b0)
        return t01, t11, g1, t02, t12, t22, g2

    sums = list(lax.fori_loop(0, chunks, pass3, (zero,) * 7))

    @pl.when(iz == 0)
    def _():
        send_rest(24, 32)

    def cross_term(k, carry):
        c = place(k)
        far_copy(3, c).wait_recv()
        for j in range(per):
            span = at(c, j)
            far = cross[span, :] * third(z0_o[span, :], y1_o[span, :], h2_o[span, :])
            s3[1, span, :] = s3[1, span, :] - far
            carry = carry + fold(z2[1, inner(c, j), :] * far)

        return carry

    def far_part():
        return lax.fori_loop(0, chunks, cross_term, zero)

    sums[5] = sums[5] - 2.0 * lax.cond(iz == 0, far_part, lambda: zero)

    line = line_of(sums)
    for stage in (0, 1):
        sum_start(1, stage, line)
        line = sum_finish(1, stage)

    @pl.when(iz == 1)
    def _():
        far_part()

    t01, t11, g1, t02, t12, t22, g2 = [take(line, k) / mu for k in range(7)]
    l1, l2 = t01 / shift, t02 / shift
    d1, e1 = t11 - l1 * t01, t12 - l1 * t02
    l3 = e1 / d1
    d2 = t22 - l2 * t02 - l3 * e1
    b1 = g1 - l1
    b2 = g2 - l2 - l3 * b1
    c2 = b2 / d2
    c1 = b1 / d1 - l3 * c2
    c0 = step - l1 * c1 - l2 * c2

    def finish(c, _):
        for slot in (0, 1):
            for j in range(per):
                span, wide = at(c, j), inner(c, j)
                p = z0[slot, wide, :]
                volt_ref[layer[slot], span, :] = (
                    c0 * p + c1 * (p - step * y1[slot, wide, :]) + c2 * z2[slot, wide, :]
                )
                tail = c0 * s1[slot, span, :] + c1 * s2[slot, span, :] + c2 * s3[slot, span, :]
                resid_ref[layer[slot], span, :] = (src[span, :] - tail) if slot == 0 else -tail
        return 0

    lax.fori_loop(0, chunks, finish, 0)

    def drain(c, _):
        @pl.when(iz == 1)
        def _():
            far_copy(2, c).wait_send()
            far_copy(3, c).wait_send()

        return 0

    lax.fori_loop(0, chunks, drain, 0)

    @pl.when(iz == 0)
    def _():
        for n in (21, 22, 23):
            far_left(jnp.int32(n), (2,))
        for k in range(chunks):
            far_copy(3, place(jnp.int32(k))).wait_send()

    @pl.when(iz == 1)
    def _():
        for k in range(4, chunks):
            far_copy(0, turn(jnp.int32(k))).wait_send()

    for stage in range(4):
        _, buf_e, buf_w = fields[stage]
        for way in (0, 1):
            edge_copy(stage, way).wait_send()
            remote(
                buf_e, buf_w, side_send.at[stage, way], side_recv.at[stage, 0], {"gx": gx_up}
            ).wait_send()


def solution(mesh):
    nx, ny = mesh.shape["gx"], mesh.shape["gy"]

    def shards(load_current, sink_mask, pad_mask, plane_class, via_class, plane_table, via_table):
        _, rows, cols = plane_class.shape
        chunks = rows // CHUNK
        flat = pltpu.VMEM((rows, cols), F32)
        flat_i = pltpu.VMEM((rows, cols), jnp.int32)
        both = pltpu.VMEM((2, rows, cols), F32)
        both_i = pltpu.VMEM((2, rows, cols), jnp.int32)
        tall = pltpu.VMEM((2, rows + 2 * HALO, cols), F32)
        side = pltpu.VMEM((2, rows, LANES), F32)
        field = [tall, side, side, flat]
        dma = pltpu.SemaphoreType.DMA
        scratch = [
            flat, flat_i, flat_i, both_i, both_i,
            pltpu.SMEM(plane_table.shape, F32), pltpu.SMEM(via_table.shape, F32),
            flat, flat,
            tall, side, side,
            both, both, both, both, flat, flat, flat, flat, flat,
            *field, *field, *field, tall, side, side,
            both, both, both,
            pltpu.VMEM((4, 2, 2 * cols // LANES, LANES), F32),
            pltpu.VMEM((4, 2, 2 * cols // LANES, LANES), F32),
            pltpu.VMEM((2, 2, 1, LANES), F32),
            pltpu.VMEM((2, nx, 1, LANES), F32),
            pltpu.VMEM((2, 2 * ny, 1, LANES), F32),
            dma((8,)),
            dma((4, chunks)), dma((4, chunks)),
            dma((4, 2)), dma((4, chunks)),
            dma((4, 2)), dma((4, 2)),
            dma((2, 2)), dma((2, 2)),
        ]
        shape = pltpu.VMEM(plane_class.shape, F32)
        hbm = pl.BlockSpec(memory_space=pltpu.HBM)
        vmem = pl.BlockSpec(memory_space=pltpu.VMEM)
        held = [
            pltpu.with_memory_space_constraint(a, pltpu.HBM)
            for a in (load_current, sink_mask, pad_mask, plane_class, via_class, plane_table, via_table)
        ]
        return pl.pallas_call(
            functools.partial(kernel, (nx, ny, rows, cols)),
            out_shape=(shape, shape),
            in_specs=[hbm] * 7,
            out_specs=(vmem, vmem),
            scratch_shapes=scratch,
            compiler_params=pltpu.CompilerParams(
                collective_id=0, has_side_effects=True, vmem_limit_bytes=48 * 1024 * 1024
            ),
        )(*held)

    layers = P("gz", "gy", "gx")
    plane = P("gy", "gx")
    table = P("gz", None)
    return jax.shard_map(
        shards,
        mesh=mesh,
        in_specs=(plane, plane, plane, layers, layers, table, table),
        out_specs=(layers, layers),
        check_vma=False,
    )
```

```python
import functools

import jax
import jax.numpy as jnp
from jax import lax
from jax.experimental import pallas as pl
from jax.experimental.pallas import tpu as pltpu
from jax.sharding import PartitionSpec as P

PAD_CONDUCTANCE = 20.0
MESH = pl.DeviceIdType.MESH
HALO = 8
LANES = 128
CHUNK = 24
F32 = jnp.float32


def harmonic(first, second):
    return 2.0 * first * second / (first + second)


def pick(classes, table):
    low = (classes & 1) == 1
    mid = (classes & 2) == 2
    high = (classes & 4) == 4
    pairs = [jnp.where(low, table[2 * k + 1], table[2 * k]) for k in range(4)]
    return jnp.where(
        high, jnp.where(mid, pairs[3], pairs[2]), jnp.where(mid, pairs[1], pairs[0])
    )


def fold(value):
    return sum(
        value[:, k : k + LANES] for k in range(LANES, value.shape[1], LANES)
    ) + value[:, :LANES]


def kernel(
    sizes,
    load_h, sink_h, pad_h, plane_h, via_h, plane_tab_h, via_tab_h,
    volt_ref, resid_ref, step_ref,
    load_ref, sink_ref, pad_ref, plane_ref, via_ref, plane_tab, via_tab,
    via_mine, via_far,
    g_buf, g_e, g_w,
    east, west, north, south, cross, inv0, inv1, mix, src,
    z0, z0_e, z0_w, z0_o, y1, y1_e, y1_w, y1_o, h2, h2_e, h2_w, h2_o, z2, z2_e, z2_w,
    s1, s2, s3,
    edge_out, edge_in, part, got_x, got_p,
    in_sem, far_send, far_recv, side_send, side_recv, edge_send, edge_recv,
    sum_send, sum_recv,
):
    nx, ny, rows, cols = sizes
    chunks = rows // CHUNK
    per = CHUNK // 8
    ix, iy, iz = lax.axis_index("gx"), lax.axis_index("gy"), lax.axis_index("gz")
    gx_up, gx_dn = lax.rem(ix + 1, nx), lax.rem(ix + nx - 1, nx)
    gy_up, gy_dn = lax.rem(iy + 1, ny), lax.rem(iy + ny - 1, ny)
    other = 1 - iz
    layer = (iz, other)

    fetch = [
        pltpu.make_async_copy(a, b, in_sem.at[k])
        for k, (a, b) in enumerate(
            (
                (via_tab_h, via_tab), (via_h.at[other], via_ref.at[other]), (plane_tab_h, plane_tab),
                (plane_h, plane_ref), (via_h.at[iz], via_ref.at[iz]), (pad_h, pad_ref), (sink_h, sink_ref), (load_h, load_ref),
            )
        )
    ]
    for c in fetch:
        c.start()

    def plane_peer(k):
        there = lax.rem(iy * 2 + iz + k, 2 * ny)
        return {"gy": there // 2, "gz": lax.rem(there, 2)}

    barrier = pltpu.get_barrier_semaphore()
    peers = [{"gx": lax.rem(ix + k, nx)} for k in range(1, nx)]
    peers += [plane_peer(k) for k in range(1, 2 * ny)]
    for peer in peers:
        pl.semaphore_signal(barrier, inc=1, device_id=peer, device_id_type=MESH)
    def at(c, j=0, n=8):
        return pl.ds(pl.multiple_of(c * CHUNK + 8 * j, 8), n)

    def inner(c, j=0, n=8):
        return pl.ds(pl.multiple_of(c * CHUNK + (8 * j + HALO), 8), n)

    def remote(source, target, send, recv, where_to):
        return pltpu.make_async_remote_copy(
            src_ref=source, dst_ref=target, send_sem=send, recv_sem=recv,
            device_id=where_to, device_id_type=MESH,
        )

    def far_copy(stage, c):
        buf, out = ((via_mine, via_far), (z0, z0_o), (y1, y1_o), (h2, h2_o))[stage]
        source = buf.at[at(c, 0, CHUNK), :] if stage == 0 else buf.at[1, inner(c, 0, CHUNK), :]
        return remote(
            source, out.at[at(c, 0, CHUNK), :],
            far_send.at[stage, c], far_recv.at[stage, c], {"gz": other},
        )

    fields = ((z0, z0_e, z0_w), (y1, y1_e, y1_w), (h2, h2_e, h2_w), (g_buf, g_e, g_w))

    def side_copies(stage, c):
        buf, buf_e, buf_w = fields[stage]
        span = inner(c, 0, CHUNK)
        return [
            remote(
                buf.at[:, span, pl.ds(cols - LANES, LANES)], buf_w.at[:, at(c, 0, CHUNK), :],
                side_send.at[stage, 0], side_recv.at[stage, c], {"gx": gx_up},
            ),
            remote(
                buf.at[:, span, pl.ds(0, LANES)], buf_e.at[:, at(c, 0, CHUNK), :],
                side_send.at[stage, 1], side_recv.at[stage, c], {"gx": gx_dn},
            ),
        ]

    def edge_copy(stage, way):
        return remote(
            edge_out.at[stage, way], edge_in.at[stage, way],
            edge_send.at[stage, way], edge_recv.at[stage, way], {"gy": (gy_up, gy_dn)[way]},
        )

    parts = [
        (slot, slot * (cols // LANES) + b, slice(b * LANES, (b + 1) * LANES))
        for slot in (0, 1)
        for b in range(cols // LANES)
    ]

    def edge_start(stage, way):
        row = (HALO + rows - 1, HALO)[way]
        for slot, k, lanes in parts:
            edge_out[stage, way, k : k + 1, :] = fields[stage][0][slot, row : row + 1, lanes]
        edge_copy(stage, way).start()

    def edge_finish(stage, way):
        edge_copy(stage, way).wait_recv()
        row = (HALO - 1, HALO + rows)[way]
        for slot, k, lanes in parts:
            fields[stage][0][slot, row : row + 1, lanes] = edge_in[stage, way, k : k + 1, :]

    def send_chunk(stage, c):
        for move in side_copies(stage, c):
            move.start()

        @pl.when(c == chunks - 1)
        def _():
            edge_start(stage, 0)

        @pl.when(c == 0)
        def _():
            edge_start(stage, 1)

    def await_chunk(stage, c):
        both = fields[stage][0].at[:, inner(c, 0, CHUNK), pl.ds(0, 2 * LANES)]
        remote(both, both, side_send.at[stage, 0], side_recv.at[stage, c], {"gx": gx_up}).wait_recv()

        @pl.when(c == 0)
        def _():
            edge_finish(stage, 0)

        @pl.when(c == chunks - 1)
        def _():
            edge_finish(stage, 1)

    def turn(k):
        return lax.rem(k + chunks - 1, chunks)

    def place(k):
        late = jnp.where(k == 3, chunks - 1, jnp.where(k == 4, 0, k - 1))
        return jnp.where(k < 3, k + 1, late)

    for c in fetch[:2]:
        c.wait()
    via_of = [[via_tab[layer[slot], k] for k in range(8)] for slot in (0, 1)]

    def lookup_far(k, _):
        c = turn(k)
        for j in range(per):
            via_mine[at(c, j), :] = pick(via_ref[other, at(c, j), :], via_of[1])
        return 0

    lax.fori_loop(0, chunks, lookup_far, 0)
    pl.semaphore_wait(barrier, len(peers))
    for n in (0, 1):
        far_copy(0, turn(jnp.int32(n))).start()

    for c in fetch[2:4]:
        c.wait()
    plane_of = [[plane_tab[layer[slot], k] for k in range(8)] for slot in (0, 1)]

    def lookup_own(k, _):
        c = turn(k)
        for slot in (0, 1):
            for j in range(per):
                g_buf[slot, inner(c, j), :] = pick(
                    plane_ref[layer[slot], at(c, j), :], plane_of[slot]
                )
        send_chunk(3, c)
        return 0

    lax.fori_loop(0, chunks, lookup_own, 0)

    def far_each(n, stages, act):
        for stage in stages:

            @pl.when(n // chunks == stage)
            def _(stage=stage):
                k = n - stage * chunks
                act(far_copy(stage, place(k) if stage else turn(k)))

    def far_left(n, stages):
        far_each(n, stages, lambda move: move.wait_send())

    def far_start(n, stages):
        far_each(n, stages, lambda move: move.start())

    def lead(n, _):
        far_left(n - 2, (0,))
        far_start(n, (0,))
        return 0

    lax.fori_loop(2, chunks - 2, lead, 0)
    for n in (chunks - 2, chunks - 1):
        far_copy(0, turn(jnp.int32(n))).start()

    @pl.when(iz == 0)
    def _():
        def clear(c, _):
            z0_o[at(c, 0, CHUNK), :] = jnp.zeros((CHUNK, cols), F32)
            return 0

        lax.fori_loop(0, chunks, clear, 0)

    for c in fetch[4:]:
        c.wait()

    def around(field, slot, c, j):
        buf, buf_e, buf_w = field
        here = buf[slot, inner(c, j), :]
        below = buf[slot, at(c, j), :]
        above = buf[slot, at(c, j + 2), :]
        up = jnp.concatenate([here[1:], above[:1]], 0)
        down = jnp.concatenate([below[7:], here[:7]], 0)
        right = pltpu.roll(
            jnp.concatenate([here, buf_e[slot, at(c, j), :]], 1), cols + LANES - 1, 1
        )[:, :cols]
        left = pltpu.roll(
            jnp.concatenate([buf_w[slot, at(c, j), :], here], 1), 1, 1
        )[:, LANES:]
        return here, right, left, up, down

    is_source = jnp.where(iz == 0, F32(1.0), F32(0.0))
    pad_scale = jnp.where(iz == 0, F32(0.0), F32(PAD_CONDUCTANCE))

    def solve(span, b0, b1):
        m = mix[span, :]
        x1 = (b1 + m * b0) * inv1[span, :]
        return b0 * inv0[span, :] + m * x1, x1

    def plane_edges(slot, c):
        sums = []
        below = g_buf[slot, at(c), :]
        here = g_buf[slot, inner(c), :]
        last = harmonic(below, jnp.concatenate([below[1:], here[:1]], 0))
        for j in range(per):
            span = at(c, j)
            here = g_buf[slot, inner(c, j), :]
            above = g_buf[slot, at(c, j + 2), :]
            wide = jnp.concatenate([g_w[slot, span, :], here, g_e[slot, span, :]], 1)
            edge = harmonic(wide, pltpu.roll(wide, cols + 2 * LANES - 1, 1))[:, : cols + LANES]
            e = edge[:, LANES:]
            w = pltpu.roll(edge, 1, 1)[:, LANES:]
            n = harmonic(here, jnp.concatenate([here[1:], above[:1]], 0))
            s = jnp.concatenate([last[7:], n[:7]], 0)
            last = n
            east[slot, span, :] = e
            west[slot, span, :] = w
            north[slot, span, :] = n
            south[slot, span, :] = s
            sums.append(e + w + n + s)
        return sums

    def build(k, _):
        c = turn(k)
        await_chunk(3, c)
        sums = [plane_edges(slot, c) for slot in (0, 1)]
        far_copy(0, c).wait_recv()
        for j in range(per):
            span = at(c, j)
            via0 = pick(via_ref[iz, span, :], via_of[0])
            via1 = via_mine[span, :]
            link = harmonic(via0, via1)
            far = harmonic(via1, via_far[span, :])
            cross[span, :] = far
            d0 = sums[0][j] + link + pad_scale * pad_ref[span, :].astype(F32)
            d1 = sums[1][j] + link + far
            i0 = 1.0 / d0
            m = link * i0
            i1 = 1.0 / (d1 - link * m)
            inv0[span, :] = i0
            inv1[span, :] = i1
            mix[span, :] = m
            b0 = is_source * (sink_ref[span, :].astype(F32) * load_ref[span, :])
            src[span, :] = b0
            x1 = m * b0 * i1
            z0[0, inner(c, j), :] = b0 * i0 + m * x1
            z0[1, inner(c, j), :] = x1

        send_chunk(0, c)

        @pl.when(jnp.logical_and(iz == 0, k >= 4))
        def _():
            far_left(k, (0,))
            far_start(k + 4, (1,))

        return 0

    lax.fori_loop(0, chunks, build, 0)

    def couple(field, slot, c, j):
        here, right, left, up, down = around(field, slot, c, j)
        span = at(c, j)
        u = (
            east[slot, span, :] * right + west[slot, span, :] * left
            + north[slot, span, :] * up + south[slot, span, :] * down
        )
        return here, u

    zero = jnp.zeros((8, LANES), F32)

    def pass1(k, carry):
        c = place(k)
        mu, t00 = carry

        @pl.when(jnp.logical_and(iz == 0, jnp.logical_or(k == 3, k == 4)))
        def _():
            far_left(chunks - 3 + k, (1,))
            far_start(chunks + 1 + k, (1,))

        await_chunk(0, c)

        @pl.when(iz == 1)
        def _():
            far_copy(1, c).wait_recv()

        for j in range(per):
            span = at(c, j)
            h0, u0 = couple(fields[0], 0, c, j)
            h1, u1 = couple(fields[0], 1, c, j)
            b0 = src[span, :]
            a0, a1 = b0 - u0, -(u1 + cross[span, :] * z0_o[span, :])
            s1[0, span, :] = a0
            s1[1, span, :] = a1
            x0, x1 = solve(span, a0, a1)
            y1[0, inner(c, j), :] = x0
            y1[1, inner(c, j), :] = x1
            mu = mu + fold(h0 * b0)
            t00 = t00 + fold(h0 * a0 + h1 * a1)
        send_chunk(1, c)

        @pl.when(iz == 1)
        def _():
            far_copy(2, c).start()

        return mu, t00

    sums = lax.fori_loop(0, chunks, pass1, (zero, zero))

    lane = lax.broadcasted_iota(jnp.int32, (1, LANES), 1)
    rings = (
        (nx, ix, got_x, lambda k: {"gx": lax.rem(ix + k, nx)}),
        (2 * ny, iy * 2 + iz, got_p, plane_peer),
    )

    def line_of(values):
        line = jnp.zeros((1, LANES), F32)
        for k, value in enumerate(values):
            line = jnp.where(lane == k, jnp.sum(value), line)
        return line

    def sum_moves(which, stage):
        size, me, got, peer = rings[stage]
        return [
            remote(
                part.at[which, stage], got.at[which, me],
                sum_send.at[which, stage], sum_recv.at[which, stage],
                peer(k),
            )
            for k in range(1, size)
        ]

    def sum_start(which, stage, line):
        part[which, stage] = line
        rings[stage][2][which, rings[stage][1]] = line
        for c in sum_moves(which, stage):
            c.start()

    def sum_finish(which, stage):
        size, _, got, peer = rings[stage]
        all_in = got.at[which, pl.ds(0, size - 1)]
        whole = remote(all_in, all_in, sum_send.at[which, stage], sum_recv.at[which, stage], peer(1))
        whole.wait_recv()
        whole.wait_send()
        line = got[which, 0]
        for k in range(1, size):
            line = line + got[which, k]
        return line

    first_line = line_of(sums)

    @pl.when(iz == 0)
    def _():
        sum_start(0, 0, first_line)

        for n in (14, 15, 16):
            far_left(jnp.int32(n - 4), (1,))
            far_start(jnp.int32(n), (1, 2))

    def pass2(k, _):
        c = place(k)
        await_chunk(1, c)
        far_copy(2, c).wait_recv()
        for j in range(per):
            span = at(c, j)
            _, u0 = couple(fields[1], 0, c, j)
            _, u1 = couple(fields[1], 1, c, j)
            a0 = s1[0, span, :] - u0
            a1 = s1[1, span, :] - (u1 + cross[span, :] * y1_o[span, :])
            s2[0, span, :] = a0
            s2[1, span, :] = a1
            x0, x1 = solve(span, a0, a1)
            h2[0, inner(c, j), :] = x0
            h2[1, inner(c, j), :] = x1
        send_chunk(2, c)

        @pl.when(iz == 1)
        def _():
            far_copy(3, c).start()

        @pl.when(jnp.logical_and(iz == 0, k < chunks - 1))
        def _():
            @pl.when(k == 0)
            def _():
                far_left(jnp.int32(13), (1,))

            far_left(14 + k, (1, 2))
            far_start(17 + k, (2,))

        @pl.when(jnp.logical_and(iz == 0, k == 2))
        def _():
            sum_start(0, 1, sum_finish(0, 0))

        return 0

    lax.fori_loop(0, chunks, pass2, 0)

    def send_rest(first, last):
        def rest(n, _):
            far_start(n, (3,))
            return 0

        lax.fori_loop(first, last, rest, 0)

    def plane_arrived(count):
        all_in = got_p.at[0, pl.ds(0, count)]
        return remote(all_in, all_in, sum_send.at[0, 1], sum_recv.at[0, 1], plane_peer(1))

    @pl.when(iz == 0)
    def _():
        plane_arrived(ny - 1).wait_recv()
        plane_arrived(2 * ny - 1).wait_send()

    @pl.when(iz == 1)
    def _():
        plane_arrived(ny).wait_recv()

    def take(line, k):
        return jnp.sum(jnp.where(lane == k, line, 0.0), axis=1, keepdims=True)

    line = got_p[0, 0]
    for k in range(1, ny):
        line = line + got_p[0, 2 * k]
    mu, t00 = take(line, 0), take(line, 1)
    step, shift = mu / t00, t00 / mu
    step_ref[...] = jnp.broadcast_to(step, (1, LANES))

    def third(a, b, c):
        return (b - step * c) - shift * (a - step * b)

    def blend(c, _):
        for slot in (0, 1):
            for j in range(per):
                span = inner(c, j)
                z2[slot, span, :] = third(z0[slot, span, :], y1[slot, span, :], h2[slot, span, :])
        return 0

    lax.fori_loop(0, chunks, blend, 0)

    def pass3(k, carry):
        c = lax.rem(k + 1, chunks)
        await_chunk(2, c)

        @pl.when(c == 0)
        def _():
            for slot in (0, 1):
                z2[slot, 0:8, :] = third(z0[slot, 0:8, :], y1[slot, 0:8, :], h2[slot, 0:8, :])

        @pl.when(c == chunks - 1)
        def _():
            top = pl.ds(HALO + rows, 8)
            for slot in (0, 1):
                z2[slot, top, :] = third(z0[slot, top, :], y1[slot, top, :], h2[slot, top, :])

        t01, t11, g1, t02, t12, t22, g2 = carry
        for j in range(per):
            span = at(c, j)
            b0 = src[span, :]
            for slot in (0, 1):
                z2_e[slot, span, :] = third(z0_e[slot, span, :], y1_e[slot, span, :], h2_e[slot, span, :])
                z2_w[slot, span, :] = third(z0_w[slot, span, :], y1_w[slot, span, :], h2_w[slot, span, :])
                h, u = couple((z2, z2_e, z2_w), slot, c, j)
                first = s1[slot, span, :]
                second = first - step * s2[slot, span, :]
                r1 = (b0 - step * first) if slot == 0 else -step * first
                a = (second - shift * r1) - u
                s2[slot, span, :] = second
                s3[slot, span, :] = a
                p = z0[slot, inner(c, j), :]
                q = p - step * y1[slot, inner(c, j), :]
                t01 = t01 + fold(p * second)
                t11 = t11 + fold(q * second)
                t02 = t02 + fold(h * first)
                t12 = t12 + fold(h * second)
                t22 = t22 + fold(h * a)
                if slot == 0:
                    g1 = g1 + fold(q * b0)
                    g2 = g2 + fold(h * b0)
        return t01, t11, g1, t02, t12, t22, g2

    sums = list(lax.fori_loop(0, chunks, pass3, (zero,) * 7))

    @pl.when(iz == 0)
    def _():
        send_rest(24, 32)

    def cross_term(k, carry):
        c = place(k)
        far_copy(3, c).wait_recv()
        for j in range(per):
            span = at(c, j)
            far = cross[span, :] * third(z0_o[span, :], y1_o[span, :], h2_o[span, :])
            s3[1, span, :] = s3[1, span, :] - far
            carry = carry + fold(z2[1, inner(c, j), :] * far)

        return carry

    def far_part():
        return lax.fori_loop(0, chunks, cross_term, zero)

    sums[5] = sums[5] - 2.0 * lax.cond(iz == 0, far_part, lambda: zero)

    line = line_of(sums)
    for stage in (0, 1):
        sum_start(1, stage, line)
        line = sum_finish(1, stage)

    @pl.when(iz == 1)
    def _():
        far_part()

    t01, t11, g1, t02, t12, t22, g2 = [take(line, k) / mu for k in range(7)]
    l1, l2 = t01 / shift, t02 / shift
    d1, e1 = t11 - l1 * t01, t12 - l1 * t02
    l3 = e1 / d1
    d2 = t22 - l2 * t02 - l3 * e1
    b1 = g1 - l1
    b2 = g2 - l2 - l3 * b1
    c2 = b2 / d2
    c1 = b1 / d1 - l3 * c2
    c0 = 1.0 - shift * (l1 * c1 + l2 * c2)
    c1, c2 = shift * c1, shift * c2

    def finish(c, _):
        for slot in (0, 1):
            for j in range(per):
                span, wide = at(c, j), inner(c, j)
                p = z0[slot, wide, :]
                volt_ref[layer[slot], span, :] = (
                    c0 * p + c1 * (p - step * y1[slot, wide, :]) + c2 * z2[slot, wide, :]
                )
                tail = c0 * s1[slot, span, :] + c1 * s2[slot, span, :] + c2 * s3[slot, span, :]
                resid_ref[layer[slot], span, :] = (shift * src[span, :] - tail) if slot == 0 else -tail
        return 0

    lax.fori_loop(0, chunks, finish, 0)

    def drain(c, _):
        @pl.when(iz == 1)
        def _():
            far_copy(2, c).wait_send()
            far_copy(3, c).wait_send()

        return 0

    lax.fori_loop(0, chunks, drain, 0)

    @pl.when(iz == 0)
    def _():
        for n in (21, 22, 23):
            far_left(jnp.int32(n), (2,))
        for k in range(chunks):
            far_copy(3, place(jnp.int32(k))).wait_send()

    @pl.when(iz == 1)
    def _():
        for k in range(4, chunks):
            far_copy(0, turn(jnp.int32(k))).wait_send()

    for stage in range(4):
        _, buf_e, buf_w = fields[stage]
        for way in (0, 1):
            edge_copy(stage, way).wait_send()
            remote(
                buf_e, buf_w, side_send.at[stage, way], side_recv.at[stage, 0], {"gx": gx_up}
            ).wait_send()


def solution(mesh):
    nx, ny = mesh.shape["gx"], mesh.shape["gy"]

    def shards(load_current, sink_mask, pad_mask, plane_class, via_class, plane_table, via_table):
        _, rows, cols = plane_class.shape
        chunks = rows // CHUNK
        flat = pltpu.VMEM((rows, cols), F32)
        flat_i = pltpu.VMEM((rows, cols), jnp.int32)
        both = pltpu.VMEM((2, rows, cols), F32)
        both_i = pltpu.VMEM((2, rows, cols), jnp.int32)
        tall = pltpu.VMEM((2, rows + 2 * HALO, cols), F32)
        side = pltpu.VMEM((2, rows, LANES), F32)
        field = [tall, side, side, flat]
        dma = pltpu.SemaphoreType.DMA
        scratch = [
            flat, flat_i, flat_i, both_i, both_i,
            pltpu.SMEM(plane_table.shape, F32), pltpu.SMEM(via_table.shape, F32),
            flat, flat,
            tall, side, side,
            both, both, both, both, flat, flat, flat, flat, flat,
            *field, *field, *field, tall, side, side,
            both, both, both,
            pltpu.VMEM((4, 2, 2 * cols // LANES, LANES), F32),
            pltpu.VMEM((4, 2, 2 * cols // LANES, LANES), F32),
            pltpu.VMEM((2, 2, 1, LANES), F32),
            pltpu.VMEM((2, nx, 1, LANES), F32),
            pltpu.VMEM((2, 2 * ny, 1, LANES), F32),
            dma((8,)),
            dma((4, chunks)), dma((4, chunks)),
            dma((4, 2)), dma((4, chunks)),
            dma((4, 2)), dma((4, 2)),
            dma((2, 2)), dma((2, 2)),
        ]
        shape = pltpu.VMEM(plane_class.shape, F32)
        hbm = pl.BlockSpec(memory_space=pltpu.HBM)
        vmem = pl.BlockSpec(memory_space=pltpu.VMEM)
        held = [
            pltpu.with_memory_space_constraint(a, pltpu.HBM)
            for a in (load_current, sink_mask, pad_mask, plane_class, via_class, plane_table, via_table)
        ]
        voltage, residual, step = pl.pallas_call(
            functools.partial(kernel, (nx, ny, rows, cols)),
            out_shape=(shape, shape, pltpu.VMEM((1, LANES), F32)),
            in_specs=[hbm] * 7,
            out_specs=(vmem, vmem, vmem),
            scratch_shapes=scratch,
            compiler_params=pltpu.CompilerParams(
                collective_id=0, has_side_effects=True, vmem_limit_bytes=48 * 1024 * 1024
            ),
        )(*held)
        return voltage * step[0, 0], residual * step[0, 0]

    layers = P("gz", "gy", "gx")
    plane = P("gy", "gx")
    table = P("gz", None)
    return jax.shard_map(
        shards,
        mesh=mesh,
        in_specs=(plane, plane, plane, layers, layers, table, table),
        out_specs=(layers, layers),
        check_vma=False,
    )
```

```python
import functools

import jax
import jax.numpy as jnp
from jax import lax
from jax.experimental import pallas as pl
from jax.experimental.pallas import tpu as pltpu
from jax.sharding import PartitionSpec as P

PAD_CONDUCTANCE = 20.0
MESH = pl.DeviceIdType.MESH
HALO = 8
LANES = 128
CHUNK = 24
F32 = jnp.float32


def harmonic(first, second):
    return 2.0 * first * second / (first + second)


def pick(classes, table):
    low = (classes & 1) == 1
    mid = (classes & 2) == 2
    high = (classes & 4) == 4
    pairs = [jnp.where(low, table[2 * k + 1], table[2 * k]) for k in range(4)]
    return jnp.where(
        high, jnp.where(mid, pairs[3], pairs[2]), jnp.where(mid, pairs[1], pairs[0])
    )


def fold(value):
    return sum(
        value[:, k : k + LANES] for k in range(LANES, value.shape[1], LANES)
    ) + value[:, :LANES]


def kernel(
    sizes,
    load_h, sink_h, pad_h, plane_h, via_h, plane_tab_h, via_tab_h,
    volt_ref, resid_ref, step_ref,
    load_ref, sink_ref, pad_ref, plane_ref, via_ref, plane_tab, via_tab,
    via_mine, via_far,
    g_buf, g_e, g_w,
    east, west, north, south, cross, inv0, inv1, mix, src,
    z0, z0_e, z0_w, z0_o, y1, y1_e, y1_w, y1_o, h2, h2_e, h2_w, h2_o, z2, z2_e, z2_w,
    s1, s2, s3,
    edge_out, edge_in, part, got_x, got_p,
    in_sem, far_send, far_recv, side_send, side_recv, edge_send, edge_recv,
    sum_send, sum_recv,
):
    nx, ny, rows, cols = sizes
    chunks = rows // CHUNK
    per = CHUNK // 8
    ix, iy, iz = lax.axis_index("gx"), lax.axis_index("gy"), lax.axis_index("gz")
    gx_up, gx_dn = lax.rem(ix + 1, nx), lax.rem(ix + nx - 1, nx)
    gy_up, gy_dn = lax.rem(iy + 1, ny), lax.rem(iy + ny - 1, ny)
    other = 1 - iz
    layer = (iz, other)

    fetch = [
        pltpu.make_async_copy(a, b, in_sem.at[k])
        for k, (a, b) in enumerate(
            (
                (via_tab_h, via_tab), (via_h.at[other], via_ref.at[other]), (plane_tab_h, plane_tab),
                (plane_h, plane_ref), (via_h.at[iz], via_ref.at[iz]), (pad_h, pad_ref), (sink_h, sink_ref), (load_h, load_ref),
            )
        )
    ]
    for c in fetch:
        c.start()

    def plane_peer(k):
        there = lax.rem(iy * 2 + iz + k, 2 * ny)
        return {"gy": there // 2, "gz": lax.rem(there, 2)}

    barrier = pltpu.get_barrier_semaphore()
    peers = [{"gx": lax.rem(ix + k, nx)} for k in range(1, nx)]
    peers += [plane_peer(k) for k in range(1, 2 * ny)]
    for peer in peers:
        pl.semaphore_signal(barrier, inc=1, device_id=peer, device_id_type=MESH)
    def at(c, j=0, n=8):
        return pl.ds(pl.multiple_of(c * CHUNK + 8 * j, 8), n)

    def inner(c, j=0, n=8):
        return pl.ds(pl.multiple_of(c * CHUNK + (8 * j + HALO), 8), n)

    def remote(source, target, send, recv, where_to):
        return pltpu.make_async_remote_copy(
            src_ref=source, dst_ref=target, send_sem=send, recv_sem=recv,
            device_id=where_to, device_id_type=MESH,
        )

    def far_copy(stage, c):
        buf, out = ((via_mine, via_far), (z0, z0_o), (y1, y1_o), (h2, h2_o))[stage]
        source = buf.at[at(c, 0, CHUNK), :] if stage == 0 else buf.at[1, inner(c, 0, CHUNK), :]
        return remote(
            source, out.at[at(c, 0, CHUNK), :],
            far_send.at[stage, c], far_recv.at[stage, c], {"gz": other},
        )

    fields = ((z0, z0_e, z0_w), (y1, y1_e, y1_w), (h2, h2_e, h2_w), (g_buf, g_e, g_w))

    def side_copies(stage, c):
        buf, buf_e, buf_w = fields[stage]
        span = inner(c, 0, CHUNK)
        return [
            remote(
                buf.at[:, span, pl.ds(cols - LANES, LANES)], buf_w.at[:, at(c, 0, CHUNK), :],
                side_send.at[stage, 0], side_recv.at[stage, c], {"gx": gx_up},
            ),
            remote(
                buf.at[:, span, pl.ds(0, LANES)], buf_e.at[:, at(c, 0, CHUNK), :],
                side_send.at[stage, 1], side_recv.at[stage, c], {"gx": gx_dn},
            ),
        ]

    def edge_copy(stage, way):
        return remote(
            edge_out.at[stage, way], edge_in.at[stage, way],
            edge_send.at[stage, way], edge_recv.at[stage, way], {"gy": (gy_up, gy_dn)[way]},
        )

    parts = [
        (slot, slot * (cols // LANES) + b, slice(b * LANES, (b + 1) * LANES))
        for slot in (0, 1)
        for b in range(cols // LANES)
    ]

    def edge_start(stage, way):
        row = (HALO + rows - 1, HALO)[way]
        for slot, k, lanes in parts:
            edge_out[stage, way, k : k + 1, :] = fields[stage][0][slot, row : row + 1, lanes]
        edge_copy(stage, way).start()

    def edge_finish(stage, way):
        edge_copy(stage, way).wait_recv()
        row = (HALO - 1, HALO + rows)[way]
        for slot, k, lanes in parts:
            fields[stage][0][slot, row : row + 1, lanes] = edge_in[stage, way, k : k + 1, :]

    def send_chunk(stage, c):
        for move in side_copies(stage, c):
            move.start()

        @pl.when(c == chunks - 1)
        def _():
            edge_start(stage, 0)

        @pl.when(c == 0)
        def _():
            edge_start(stage, 1)

    def await_chunk(stage, c):
        both = fields[stage][0].at[:, inner(c, 0, CHUNK), pl.ds(0, 2 * LANES)]
        remote(both, both, side_send.at[stage, 0], side_recv.at[stage, c], {"gx": gx_up}).wait_recv()

        @pl.when(c == 0)
        def _():
            edge_finish(stage, 0)

        @pl.when(c == chunks - 1)
        def _():
            edge_finish(stage, 1)

    def turn(k):
        return lax.rem(k + chunks - 1, chunks)

    def place(k):
        late = jnp.where(k == 3, chunks - 1, jnp.where(k == 4, 0, k - 1))
        return jnp.where(k < 3, k + 1, late)

    for c in fetch[:2]:
        c.wait()
    via_of = [[via_tab[layer[slot], k] for k in range(8)] for slot in (0, 1)]

    def lookup_far(k, _):
        c = turn(k)
        for j in range(per):
            via_mine[at(c, j), :] = pick(via_ref[other, at(c, j), :], via_of[1])
        return 0

    lax.fori_loop(0, chunks, lookup_far, 0)
    pl.semaphore_wait(barrier, len(peers))
    for n in (0, 1):
        far_copy(0, turn(jnp.int32(n))).start()

    for c in fetch[2:4]:
        c.wait()
    plane_of = [[plane_tab[layer[slot], k] for k in range(8)] for slot in (0, 1)]

    def lookup_own(k, _):
        c = turn(k)
        for slot in (0, 1):
            for j in range(per):
                g_buf[slot, inner(c, j), :] = pick(
                    plane_ref[layer[slot], at(c, j), :], plane_of[slot]
                )
        send_chunk(3, c)
        return 0

    lax.fori_loop(0, chunks, lookup_own, 0)

    def far_each(n, stages, act):
        for stage in stages:

            @pl.when(n // chunks == stage)
            def _(stage=stage):
                k = n - stage * chunks
                act(far_copy(stage, place(k) if stage else turn(k)))

    def far_left(n, stages):
        far_each(n, stages, lambda move: move.wait_send())

    def far_start(n, stages):
        far_each(n, stages, lambda move: move.start())

    def lead(n, _):
        far_left(n - 2, (0,))
        far_start(n, (0,))
        return 0

    lax.fori_loop(2, chunks - 2, lead, 0)
    for n in (chunks - 2, chunks - 1):
        far_copy(0, turn(jnp.int32(n))).start()

    @pl.when(iz == 0)
    def _():
        def clear(c, _):
            z0_o[at(c, 0, CHUNK), :] = jnp.zeros((CHUNK, cols), F32)
            return 0

        lax.fori_loop(0, chunks, clear, 0)

    for c in fetch[4:]:
        c.wait()

    def around(field, slot, c, j):
        buf, buf_e, buf_w = field
        here = buf[slot, inner(c, j), :]
        below = buf[slot, at(c, j), :]
        above = buf[slot, at(c, j + 2), :]
        up = jnp.concatenate([here[1:], above[:1]], 0)
        down = jnp.concatenate([below[7:], here[:7]], 0)
        right = pltpu.roll(
            jnp.concatenate([here, buf_e[slot, at(c, j), :]], 1), cols + LANES - 1, 1
        )[:, :cols]
        left = pltpu.roll(
            jnp.concatenate([buf_w[slot, at(c, j), :], here], 1), 1, 1
        )[:, LANES:]
        return here, right, left, up, down

    is_source = jnp.where(iz == 0, F32(1.0), F32(0.0))
    pad_scale = jnp.where(iz == 0, F32(0.0), F32(PAD_CONDUCTANCE))

    def solve(span, b0, b1):
        m = mix[span, :]
        x1 = (b1 + m * b0) * inv1[span, :]
        return b0 * inv0[span, :] + m * x1, x1

    def plane_edges(slot, c):
        sums = []
        below = g_buf[slot, at(c), :]
        here = g_buf[slot, inner(c), :]
        last = harmonic(below, jnp.concatenate([below[1:], here[:1]], 0))
        for j in range(per):
            span = at(c, j)
            here = g_buf[slot, inner(c, j), :]
            above = g_buf[slot, at(c, j + 2), :]
            wide = jnp.concatenate([g_w[slot, span, :], here, g_e[slot, span, :]], 1)
            edge = harmonic(wide, pltpu.roll(wide, cols + 2 * LANES - 1, 1))[:, : cols + LANES]
            e = edge[:, LANES:]
            w = pltpu.roll(edge, 1, 1)[:, LANES:]
            n = harmonic(here, jnp.concatenate([here[1:], above[:1]], 0))
            s = jnp.concatenate([last[7:], n[:7]], 0)
            last = n
            east[slot, span, :] = e
            west[slot, span, :] = w
            north[slot, span, :] = n
            south[slot, span, :] = s
            sums.append(e + w + n + s)
        return sums

    def build(k, _):
        c = turn(k)
        await_chunk(3, c)
        sums = [plane_edges(slot, c) for slot in (0, 1)]
        far_copy(0, c).wait_recv()
        for j in range(per):
            span = at(c, j)
            via0 = pick(via_ref[iz, span, :], via_of[0])
            via1 = via_mine[span, :]
            link = harmonic(via0, via1)
            far = harmonic(via1, via_far[span, :])
            cross[span, :] = far
            d0 = sums[0][j] + link + pad_scale * pad_ref[span, :].astype(F32)
            d1 = sums[1][j] + link + far
            i0 = 1.0 / d0
            m = link * i0
            i1 = 1.0 / (d1 - link * m)
            inv0[span, :] = i0
            inv1[span, :] = i1
            mix[span, :] = m
            b0 = is_source * (sink_ref[span, :].astype(F32) * load_ref[span, :])
            src[span, :] = b0
            x1 = m * b0 * i1
            z0[0, inner(c, j), :] = b0 * i0 + m * x1
            z0[1, inner(c, j), :] = x1

        send_chunk(0, c)

        @pl.when(jnp.logical_and(iz == 0, k >= 4))
        def _():
            far_left(k, (0,))
            far_start(k + 4, (1,))

        return 0

    lax.fori_loop(0, chunks, build, 0)

    def couple(field, slot, c, j):
        here, right, left, up, down = around(field, slot, c, j)
        span = at(c, j)
        u = (
            east[slot, span, :] * right + west[slot, span, :] * left
            + north[slot, span, :] * up + south[slot, span, :] * down
        )
        return here, u

    zero = jnp.zeros((8, LANES), F32)

    def pass1(k, carry):
        c = place(k)
        mu, t00 = carry

        @pl.when(jnp.logical_and(iz == 0, jnp.logical_or(k == 3, k == 4)))
        def _():
            far_left(chunks - 3 + k, (1,))
            far_start(chunks + 1 + k, (1,))

        await_chunk(0, c)

        @pl.when(iz == 1)
        def _():
            far_copy(1, c).wait_recv()

        for j in range(per):
            span = at(c, j)
            h0, u0 = couple(fields[0], 0, c, j)
            h1, u1 = couple(fields[0], 1, c, j)
            b0 = src[span, :]
            a0, a1 = b0 - u0, -(u1 + cross[span, :] * z0_o[span, :])
            s1[0, span, :] = a0
            s1[1, span, :] = a1
            x0, x1 = solve(span, a0, a1)
            y1[0, inner(c, j), :] = x0
            y1[1, inner(c, j), :] = x1
            mu = mu + fold(h0 * b0)
            t00 = t00 + fold(h0 * a0 + h1 * a1)
        send_chunk(1, c)

        @pl.when(iz == 1)
        def _():
            far_copy(2, c).start()

        return mu, t00

    sums = lax.fori_loop(0, chunks, pass1, (zero, zero))

    lane = lax.broadcasted_iota(jnp.int32, (1, LANES), 1)
    rings = (
        (nx, ix, got_x, lambda k: {"gx": lax.rem(ix + k, nx)}),
        (2 * ny, iy * 2 + iz, got_p, plane_peer),
    )

    def line_of(values):
        line = jnp.zeros((1, LANES), F32)
        for k, value in enumerate(values):
            line = jnp.where(lane == k, jnp.sum(value), line)
        return line

    def sum_moves(which, stage):
        size, me, got, peer = rings[stage]
        return [
            remote(
                part.at[which, stage], got.at[which, me],
                sum_send.at[which, stage], sum_recv.at[which, stage],
                peer(k),
            )
            for k in range(1, size)
        ]

    def sum_start(which, stage, line):
        part[which, stage] = line
        rings[stage][2][which, rings[stage][1]] = line
        for c in sum_moves(which, stage):
            c.start()

    def sum_finish(which, stage):
        size, _, got, peer = rings[stage]
        all_in = got.at[which, pl.ds(0, size - 1)]
        whole = remote(all_in, all_in, sum_send.at[which, stage], sum_recv.at[which, stage], peer(1))
        whole.wait_recv()
        whole.wait_send()
        line = got[which, 0]
        for k in range(1, size):
            line = line + got[which, k]
        return line

    first_line = line_of(sums)

    @pl.when(iz == 0)
    def _():
        sum_start(0, 0, first_line)

        for n in (14, 15, 16):
            far_left(jnp.int32(n - 4), (1,))
            far_start(jnp.int32(n), (1, 2))

    def pass2(k, _):
        c = place(k)
        await_chunk(1, c)
        far_copy(2, c).wait_recv()
        for j in range(per):
            span = at(c, j)
            _, u0 = couple(fields[1], 0, c, j)
            _, u1 = couple(fields[1], 1, c, j)
            a0 = s1[0, span, :] - u0
            a1 = s1[1, span, :] - (u1 + cross[span, :] * y1_o[span, :])
            s2[0, span, :] = a0
            s2[1, span, :] = a1
            x0, x1 = solve(span, a0, a1)
            h2[0, inner(c, j), :] = x0
            h2[1, inner(c, j), :] = x1
        send_chunk(2, c)

        @pl.when(iz == 1)
        def _():
            far_copy(3, c).start()

        @pl.when(jnp.logical_and(iz == 0, k < chunks - 1))
        def _():
            @pl.when(k == 0)
            def _():
                far_left(jnp.int32(13), (1,))

            far_left(14 + k, (1, 2))
            far_start(17 + k, (2,))

        @pl.when(jnp.logical_and(iz == 0, k == 2))
        def _():
            sum_start(0, 1, sum_finish(0, 0))

        return 0

    lax.fori_loop(0, chunks, pass2, 0)

    def send_rest(first, last):
        def rest(n, _):
            far_start(n, (3,))
            return 0

        lax.fori_loop(first, last, rest, 0)

    def plane_arrived(count):
        all_in = got_p.at[0, pl.ds(0, count)]
        return remote(all_in, all_in, sum_send.at[0, 1], sum_recv.at[0, 1], plane_peer(1))

    @pl.when(iz == 0)
    def _():
        plane_arrived(ny - 1).wait_recv()
        plane_arrived(2 * ny - 1).wait_send()

    @pl.when(iz == 1)
    def _():
        plane_arrived(ny).wait_recv()

    def take(line, k):
        return jnp.sum(jnp.where(lane == k, line, 0.0), axis=1, keepdims=True)

    line = got_p[0, 0]
    for k in range(1, ny):
        line = line + got_p[0, 2 * k]
    mu, t00 = take(line, 0), take(line, 1)
    step, shift = mu / t00, t00 / mu
    step_ref[...] = jnp.broadcast_to(step, (1, LANES))

    def third(a, b, c):
        return (b - step * c) - shift * (a - step * b)

    def blend(c, _):
        for slot in (0, 1):
            for j in range(per):
                span = inner(c, j)
                z2[slot, span, :] = third(z0[slot, span, :], y1[slot, span, :], h2[slot, span, :])
        return 0

    lax.fori_loop(0, chunks, blend, 0)

    def pass3(k, carry):
        c = lax.rem(k + 1, chunks)
        await_chunk(2, c)

        @pl.when(c == 0)
        def _():
            for slot in (0, 1):
                z2[slot, 0:8, :] = third(z0[slot, 0:8, :], y1[slot, 0:8, :], h2[slot, 0:8, :])

        @pl.when(c == chunks - 1)
        def _():
            top = pl.ds(HALO + rows, 8)
            for slot in (0, 1):
                z2[slot, top, :] = third(z0[slot, top, :], y1[slot, top, :], h2[slot, top, :])

        t01, t11, g1, t02, t12, t22, g2 = carry
        for j in range(per):
            span = at(c, j)
            b0 = src[span, :]
            for slot in (0, 1):
                z2_e[slot, span, :] = third(z0_e[slot, span, :], y1_e[slot, span, :], h2_e[slot, span, :])
                z2_w[slot, span, :] = third(z0_w[slot, span, :], y1_w[slot, span, :], h2_w[slot, span, :])
                h, u = couple((z2, z2_e, z2_w), slot, c, j)
                first = s1[slot, span, :]
                second = first - step * s2[slot, span, :]
                r1 = (b0 - step * first) if slot == 0 else -step * first
                a = (second - shift * r1) - u
                s2[slot, span, :] = second
                s3[slot, span, :] = a
                p = z0[slot, inner(c, j), :]
                q = p - step * y1[slot, inner(c, j), :]
                t01 = t01 + fold(p * second)
                t11 = t11 + fold(q * second)
                t02 = t02 + fold(h * first)
                t12 = t12 + fold(h * second)
                t22 = t22 + fold(h * a)
                if slot == 0:
                    g1 = g1 + fold(q * b0)
                    g2 = g2 + fold(h * b0)
        return t01, t11, g1, t02, t12, t22, g2

    sums = list(lax.fori_loop(0, chunks, pass3, (zero,) * 7))

    @pl.when(iz == 0)
    def _():
        send_rest(24, 32)

    def cross_term(k, carry):
        c = place(k)
        far_copy(3, c).wait_recv()
        for j in range(per):
            span = at(c, j)
            far = cross[span, :] * third(z0_o[span, :], y1_o[span, :], h2_o[span, :])
            s3[1, span, :] = s3[1, span, :] - far
            carry = carry + fold(z2[1, inner(c, j), :] * far)

        return carry

    def far_part():
        return lax.fori_loop(0, chunks, cross_term, zero)

    sums[5] = sums[5] - 2.0 * lax.cond(iz == 0, far_part, lambda: zero)

    line = line_of(sums)
    sum_start(1, 0, line)
    sum_start(1, 1, sum_finish(1, 0))

    @pl.when(iz == 1)
    def _():
        far_part()

    line = sum_finish(1, 1)

    t01, t11, g1, t02, t12, t22, g2 = [take(line, k) / mu for k in range(7)]
    l1, l2 = t01 / shift, t02 / shift
    d1, e1 = t11 - l1 * t01, t12 - l1 * t02
    l3 = e1 / d1
    d2 = t22 - l2 * t02 - l3 * e1
    b1 = g1 - l1
    b2 = g2 - l2 - l3 * b1
    c2 = b2 / d2
    c1 = b1 / d1 - l3 * c2
    c0 = 1.0 - shift * (l1 * c1 + l2 * c2)
    c1, c2 = shift * c1, shift * c2

    def finish(c, _):
        for slot in (0, 1):
            for j in range(per):
                span, wide = at(c, j), inner(c, j)
                p = z0[slot, wide, :]
                volt_ref[layer[slot], span, :] = (
                    c0 * p + c1 * (p - step * y1[slot, wide, :]) + c2 * z2[slot, wide, :]
                )
                tail = c0 * s1[slot, span, :] + c1 * s2[slot, span, :] + c2 * s3[slot, span, :]
                resid_ref[layer[slot], span, :] = (shift * src[span, :] - tail) if slot == 0 else -tail
        return 0

    lax.fori_loop(0, chunks, finish, 0)

    def drain(c, _):
        @pl.when(iz == 1)
        def _():
            far_copy(2, c).wait_send()
            far_copy(3, c).wait_send()

        return 0

    lax.fori_loop(0, chunks, drain, 0)

    @pl.when(iz == 0)
    def _():
        for n in (21, 22, 23):
            far_left(jnp.int32(n), (2,))
        for k in range(chunks):
            far_copy(3, place(jnp.int32(k))).wait_send()

    @pl.when(iz == 1)
    def _():
        for k in range(4, chunks):
            far_copy(0, turn(jnp.int32(k))).wait_send()

    for stage in range(4):
        _, buf_e, buf_w = fields[stage]
        for way in (0, 1):
            edge_copy(stage, way).wait_send()
            remote(
                buf_e, buf_w, side_send.at[stage, way], side_recv.at[stage, 0], {"gx": gx_up}
            ).wait_send()


def solution(mesh):
    nx, ny = mesh.shape["gx"], mesh.shape["gy"]

    def shards(load_current, sink_mask, pad_mask, plane_class, via_class, plane_table, via_table):
        _, rows, cols = plane_class.shape
        chunks = rows // CHUNK
        flat = pltpu.VMEM((rows, cols), F32)
        flat_i = pltpu.VMEM((rows, cols), jnp.int32)
        both = pltpu.VMEM((2, rows, cols), F32)
        both_i = pltpu.VMEM((2, rows, cols), jnp.int32)
        tall = pltpu.VMEM((2, rows + 2 * HALO, cols), F32)
        side = pltpu.VMEM((2, rows, LANES), F32)
        field = [tall, side, side, flat]
        dma = pltpu.SemaphoreType.DMA
        scratch = [
            flat, flat_i, flat_i, both_i, both_i,
            pltpu.SMEM(plane_table.shape, F32), pltpu.SMEM(via_table.shape, F32),
            flat, flat,
            tall, side, side,
            both, both, both, both, flat, flat, flat, flat, flat,
            *field, *field, *field, tall, side, side,
            both, both, both,
            pltpu.VMEM((4, 2, 2 * cols // LANES, LANES), F32),
            pltpu.VMEM((4, 2, 2 * cols // LANES, LANES), F32),
            pltpu.VMEM((2, 2, 1, LANES), F32),
            pltpu.VMEM((2, nx, 1, LANES), F32),
            pltpu.VMEM((2, 2 * ny, 1, LANES), F32),
            dma((8,)),
            dma((4, chunks)), dma((4, chunks)),
            dma((4, 2)), dma((4, chunks)),
            dma((4, 2)), dma((4, 2)),
            dma((2, 2)), dma((2, 2)),
        ]
        shape = pltpu.VMEM(plane_class.shape, F32)
        hbm = pl.BlockSpec(memory_space=pltpu.HBM)
        vmem = pl.BlockSpec(memory_space=pltpu.VMEM)
        held = [
            pltpu.with_memory_space_constraint(a, pltpu.HBM)
            for a in (load_current, sink_mask, pad_mask, plane_class, via_class, plane_table, via_table)
        ]
        voltage, residual, step = pl.pallas_call(
            functools.partial(kernel, (nx, ny, rows, cols)),
            out_shape=(shape, shape, pltpu.VMEM((1, LANES), F32)),
            in_specs=[hbm] * 7,
            out_specs=(vmem, vmem, vmem),
            scratch_shapes=scratch,
            compiler_params=pltpu.CompilerParams(
                collective_id=0, has_side_effects=True, vmem_limit_bytes=48 * 1024 * 1024
            ),
        )(*held)
        return voltage * step[0, 0], residual * step[0, 0]

    layers = P("gz", "gy", "gx")
    plane = P("gy", "gx")
    table = P("gz", None)
    return jax.shard_map(
        shards,
        mesh=mesh,
        in_specs=(plane, plane, plane, layers, layers, table, table),
        out_specs=(layers, layers),
        check_vma=False,
    )
```
